8 devices in a mesh: dp: 1 (over z), tp: 2 (over y), ep: 4 (over x, core).
Axes of the slice: x: 2, y: 2, z: 1, core: 2. Of those that a mesh axis runs over, the one named last changes fastest.
Arguments:
- normed: bfloat16 [2048, 2048], P(('dp', 'ep'))
- residual: bfloat16 [2048, 2048], P(('dp', 'ep'))
- w_router: float32 [2048, 60], replicated
- ws_gate: bfloat16 [2048, 5632], P(None, 'tp')
- ws_up: bfloat16 [2048, 5632], P(None, 'tp')
- ws_down: bfloat16 [5632, 2048], P('tp')
- we_gate: bfloat16 [60, 2048, 1408], P('ep', None, 'tp')
- we_up: bfloat16 [60, 2048, 1408], P('ep', None, 'tp')
- we_down: bfloat16 [60, 1408, 2048], P('ep', 'tp')
- first_id: int32 [2048], P(('dp', 'ep'))
- alt_id: int32 [2048], P(('dp', 'ep'))
Outputs:
- output: bfloat16 [2048, 2048], P(('dp', 'ep'))
All inputs are finite; a program needn't handle non-finite values.
Results may differ from the reference program's by a relative error of at most 0.00530088.
Values are sent between devices in bfloat16 or wider.
A program may use at most 1 GiB of HBM per device.

```python
import jax
import jax.numpy as jnp
from jax import lax

TOK_DEV = 512
EP_RANKS = 4
EXPERTS = 60
D_MODEL = 2048
FF_EXPERT = 1408
FF_SHARED = 5632
HOT_COUNT = 4
HOT_WEIGHT = 3

TOKENS = TOK_DEV * EP_RANKS
LOCAL_EXPERTS = EXPERTS // EP_RANKS
CAPACITY = (5 * TOKENS + 4 * EXPERTS - 1) // (4 * EXPERTS)


def draw_routing(route_key):
    key_list = jax.random.split(route_key, 6)
    hot_flag = (jax.random.permutation(key_list[0], EXPERTS) < HOT_COUNT).astype(jnp.int32)
    cum_weight = jnp.cumsum((1 + (HOT_WEIGHT - 1) * hot_flag).reshape(EP_RANKS, LOCAL_EXPERTS), axis=1)
    owner_quota = jnp.arange(TOK_DEV, dtype=jnp.int32) % EP_RANKS
    owner_first = jax.vmap(lambda key_one: jax.random.permutation(key_one, owner_quota))(jax.random.split(key_list[1], EP_RANKS))
    owner_alt = jax.vmap(lambda key_one: jax.random.permutation(key_one, owner_quota))(jax.random.split(key_list[2], EP_RANKS))
    row_cum = cum_weight[owner_first]
    draw_value = jax.random.randint(key_list[3], (EP_RANKS, TOK_DEV), 0, row_cum[:, :, -1])
    local_first = jnp.sum((row_cum <= draw_value[:, :, None]).astype(jnp.int32), axis=2)
    alt_shift = jax.random.randint(key_list[4], (EP_RANKS, TOK_DEV), 1, LOCAL_EXPERTS)
    free_pick = jax.random.randint(key_list[5], (EP_RANKS, TOK_DEV), 0, LOCAL_EXPERTS)
    local_alt = jnp.where(owner_alt == owner_first, (local_first + alt_shift) % LOCAL_EXPERTS, free_pick)
    first_id = (owner_first * LOCAL_EXPERTS + local_first).reshape(TOKENS).astype(jnp.int32)
    alt_id = (owner_alt * LOCAL_EXPERTS + local_alt).reshape(TOKENS).astype(jnp.int32)
    return first_id, alt_id


def setup_inputs(seed: int = 0, part: int = 0) -> dict:
    root_key = jax.random.key(seed)
    part_keys = jax.random.split(jax.random.fold_in(root_key, part), 3)
    weight_keys = jax.random.split(root_key, 7)
    normed = jax.random.normal(part_keys[0], (TOKENS, D_MODEL), jnp.float32).astype(jnp.bfloat16)
    residual = jax.random.normal(part_keys[1], (TOKENS, D_MODEL), jnp.float32).astype(jnp.bfloat16)
    first_id, alt_id = draw_routing(part_keys[2])
    w_router = jax.random.normal(weight_keys[0], (D_MODEL, EXPERTS), jnp.float32) * D_MODEL ** -0.5
    ws_gate = (jax.random.normal(weight_keys[1], (D_MODEL, FF_SHARED), jnp.float32) * D_MODEL ** -0.5).astype(jnp.bfloat16)
    ws_up = (jax.random.normal(weight_keys[2], (D_MODEL, FF_SHARED), jnp.float32) * D_MODEL ** -0.5).astype(jnp.bfloat16)
    ws_down = (jax.random.normal(weight_keys[3], (FF_SHARED, D_MODEL), jnp.float32) * FF_SHARED ** -0.5).astype(jnp.bfloat16)
    we_gate = (jax.random.normal(weight_keys[4], (EXPERTS, D_MODEL, FF_EXPERT), jnp.float32) * D_MODEL ** -0.5).astype(jnp.bfloat16)
    we_up = (jax.random.normal(weight_keys[5], (EXPERTS, D_MODEL, FF_EXPERT), jnp.float32) * D_MODEL ** -0.5).astype(jnp.bfloat16)
    we_down = (jax.random.normal(weight_keys[6], (EXPERTS, FF_EXPERT, D_MODEL), jnp.float32) * (EXPERTS * FF_EXPERT ** -0.5)).astype(jnp.bfloat16)
    return {'normed': normed, 'residual': residual, 'w_router': w_router, 'ws_gate': ws_gate, 'ws_up': ws_up, 'ws_down': ws_down, 'we_gate': we_gate, 'we_up': we_up, 'we_down': we_down, 'first_id': first_id, 'alt_id': alt_id}


def expert_mlp(token_rows, w_gate, w_up, w_down):
    gate_pre = jnp.dot(token_rows, w_gate, preferred_element_type=jnp.float32)
    up_pre = jnp.dot(token_rows, w_up, preferred_element_type=jnp.float32)
    hidden_act = (jax.nn.silu(gate_pre) * up_pre).astype(jnp.bfloat16)
    return jnp.dot(hidden_act, w_down, preferred_element_type=jnp.float32)


def rank_in_column(onehot):
    return jnp.sum(jnp.cumsum(onehot, axis=0) * onehot, axis=1) - 1


def reference(normed, residual, w_router, ws_gate, ws_up, ws_down, we_gate, we_up, we_down, first_id, alt_id):
    expert_ids = jnp.arange(EXPERTS, dtype=jnp.int32)
    onehot_first = (first_id[:, None] == expert_ids[None, :]).astype(jnp.int32)
    rank_first = rank_in_column(onehot_first)
    kept_mask = rank_first < CAPACITY
    slot_load = jnp.minimum(jnp.sum(onehot_first, axis=0), CAPACITY)
    overflow = jnp.logical_not(kept_mask)
    onehot_alt = ((alt_id[:, None] == expert_ids[None, :]) & overflow[:, None]).astype(jnp.int32)
    rank_alt = rank_in_column(onehot_alt)
    recycled = overflow & (rank_alt < (CAPACITY - slot_load)[alt_id])
    active = kept_mask | recycled
    chosen = jnp.where(kept_mask, first_id, alt_id)
    slot_index = jnp.where(kept_mask, rank_first, slot_load[alt_id] + rank_alt)
    table_size = EXPERTS * CAPACITY
    slot_code = jnp.where(active, chosen * CAPACITY + slot_index, table_size)
    slot_token = jnp.full((table_size,), TOKENS, jnp.int32).at[slot_code].set(jnp.arange(TOKENS, dtype=jnp.int32), mode='drop')
    slot_rows = jnp.take(normed, slot_token, axis=0, mode='fill', fill_value=0).reshape(EXPERTS, CAPACITY, D_MODEL)
    routed_slots = lax.map(lambda bundle: expert_mlp(bundle[0], bundle[1], bundle[2], bundle[3]).astype(jnp.bfloat16), (slot_rows, we_gate, we_up, we_down))
    routed = jnp.take(routed_slots.reshape(table_size, D_MODEL), jnp.minimum(slot_code, table_size - 1), axis=0)
    router_prob = jax.nn.softmax(jnp.dot(normed, w_router, preferred_element_type=jnp.float32), axis=-1)
    gate_weight = jnp.take_along_axis(router_prob, chosen[:, None], axis=1)[:, 0] * active.astype(jnp.float32)
    shared = lax.map(lambda block_rows: expert_mlp(block_rows, ws_gate, ws_up, ws_down), normed.reshape(EP_RANKS, TOK_DEV, D_MODEL)).reshape(TOKENS, D_MODEL)
    combined = residual.astype(jnp.float32) + shared + gate_weight[:, None] * routed.astype(jnp.float32)
    return combined.astype(jnp.bfloat16)
```

```python
import functools

import jax
import jax.numpy as jnp
from jax import lax
from jax.experimental import pallas as pl
from jax.experimental.pallas import tpu as pltpu
from jax.sharding import PartitionSpec as P

MESH = pl.DeviceIdType.MESH
F32 = jnp.float32
BF16 = jnp.bfloat16
LANES = 128
RANK_BLOCK = 256
X_CHUNKS = 4
OUT_CHUNKS = 4


def dot(a, b):
    return jnp.dot(a, b, preferred_element_type=F32)


def dot_bt(a, b):
    return lax.dot_general(a, b, (((1,), (1,)), ((), ())), preferred_element_type=F32)


def dot_at(a, b):
    return lax.dot_general(a, b, (((0,), (0,)), ((), ())), preferred_element_type=F32)


def moe_kernel(dims, x_hbm, res_hbm, wr_hbm, wsg_hbm, wsu_hbm, wsd_hbm, weg_hbm, weu_hbm, wed_hbm, first_ref, alt_ref, o_hbm,
               x_all, ids_all, code_rows, code_col, gate_col, slot_x, sh_own, sh_send, sh_recv, ex_own, ex_send, ex_recv, ret, out_half, res_half, wr,
               ld_sem, id_send, id_recv, sib_send, sib_recv, xp_send, xp_recv, fw_send, fw_recv,
               ysh_send, ysh_recv, yex_send, yex_recv, rs_send, rs_recv, rx_send, rx_recv, rf_send, rf_recv, yo_send, yo_recv, lo_sem):
    experts, capacity, pad_cap, local_experts, ep_size = dims
    tok, d_model = x_hbm.shape
    half = d_model // 2
    slots = local_experts * pad_cap
    ff_shared = wsg_hbm.shape[1]
    ff_expert = weg_hbm.shape[1]
    dp = lax.axis_index("dp")
    t = lax.axis_index("tp")
    me = lax.axis_index("ep")
    core = lax.rem(me, 2)
    sib = me + 1 - 2 * core
    xp = lax.rem(me + 2, ep_size)
    diag = lax.rem(sib + 2, ep_size)
    y_peer = (dp, 1 - t, me)
    sib_dev = (dp, t, sib)
    xp_dev = (dp, t, xp)
    diag_dev = (dp, t, diag)

    own_x = pltpu.make_async_copy(x_hbm, x_all.at[me], ld_sem.at[0])
    own_x.start()
    own_off = pl.multiple_of(t * half, half)
    peer_off = pl.multiple_of((1 - t) * half, half)
    res_load = pltpu.make_async_copy(res_hbm.at[:, pl.ds(own_off, half)], res_half, ld_sem.at[1])
    res_load.start()
    wr_load = pltpu.make_async_copy(wr_hbm, wr, ld_sem.at[2])
    wr_load.start()

    barrier = pltpu.get_barrier_semaphore()
    for dev in (y_peer, sib_dev, xp_dev, diag_dev):
        pl.semaphore_signal(barrier, inc=1, device_id=dev, device_id_type=MESH)

    ids_all[pl.ds(me, 1), 0:1, :] = first_ref[...].reshape(1, 1, tok)
    ids_all[pl.ds(me, 1), 1:2, :] = alt_ref[...].reshape(1, 1, tok)
    own_x.wait()
    pl.semaphore_wait(barrier, 4)

    def remote(src, dst, s_sem, r_sem, dev):
        return pltpu.make_async_remote_copy(src_ref=src, dst_ref=dst, send_sem=s_sem, recv_sem=r_sem, device_id=dev, device_id_type=MESH)

    id_copies = [remote(ids_all.at[me], ids_all.at[me], id_send.at[i], id_recv.at[i], dev) for i, dev in enumerate((sib_dev, xp_dev, diag_dev))]
    for copy in id_copies:
        copy.start()
    x_rows = tok // X_CHUNKS
    xp_copies = [remote(x_all.at[me, pl.ds(c * x_rows, x_rows)], x_all.at[me, pl.ds(c * x_rows, x_rows)], xp_send.at[c], xp_recv.at[c], xp_dev) for c in range(X_CHUNKS)]
    for copy in xp_copies:
        copy.start()
    sib_copy = remote(x_all.at[me], x_all.at[me], sib_send.at[0], sib_recv.at[0], sib_dev)
    sib_copy.start()
    fw_copies = [remote(x_all.at[xp, pl.ds(c * x_rows, x_rows)], x_all.at[xp, pl.ds(c * x_rows, x_rows)], fw_send.at[c], fw_recv.at[c], sib_dev) for c in range(X_CHUNKS)]

    hc = 256
    n_hidden = ff_shared // hc
    n_half = half // hc

    def ysh_copy(j):
        return remote(sh_send.at[j], sh_recv.at[j], ysh_send.at[j], ysh_recv.at[j], y_peer)

    def shared_phase(act, wg, wu, wd, g_sem, u_sem, d_sem):
        def gate_copy(c, slot):
            return pltpu.make_async_copy(wsg_hbm.at[:, pl.ds(pl.multiple_of(c * hc, hc), hc)], wg.at[slot], g_sem.at[slot])

        def up_copy(c, slot):
            return pltpu.make_async_copy(wsu_hbm.at[:, pl.ds(pl.multiple_of(c * hc, hc), hc)], wu.at[slot], u_sem.at[slot])

        def down_copy(j, slot):
            col = jnp.where(j < n_half, peer_off + j * hc, own_off + (j - n_half) * hc)
            return pltpu.make_async_copy(wsd_hbm.at[:, pl.ds(pl.multiple_of(col, hc), hc)], wd.at[slot], d_sem.at[slot])

        for slot in range(2):
            gate_copy(slot, slot).start()
            up_copy(slot, slot).start()
        for slot in range(2):
            down_copy(slot, slot).start()

        @pl.loop(0, n_hidden)
        def _(c):
            slot = lax.rem(c, 2)
            gate_copy(c, slot).wait()
            up_copy(c, slot).wait()
            x = x_all[me]
            g = dot(x, wg[slot])
            u = dot(x, wu[slot])
            act[:, pl.ds(pl.multiple_of(c * hc, hc), hc)] = (jax.nn.silu(g) * u).astype(BF16)

            @pl.when(c + 2 < n_hidden)
            def _():
                gate_copy(c + 2, slot).start()
                up_copy(c + 2, slot).start()

        @pl.loop(0, n_half)
        def _(j):
            slot = lax.rem(j, 2)
            down_copy(j, slot).wait()
            sh_send[j] = dot(act[...], wd[slot])
            ysh_copy(j).start()
            down_copy(j + 2, slot).start()

        @pl.loop(0, n_half)
        def _(j):
            slot = lax.rem(j, 2)
            down_copy(j + n_half, slot).wait()
            sh_own[j] = dot(act[...], wd[slot])

            @pl.when(j + 2 < n_half)
            def _():
                down_copy(j + n_half + 2, slot).start()

    pl.run_scoped(shared_phase, pltpu.VMEM((tok, ff_shared), BF16), pltpu.VMEM((2, d_model, hc), BF16), pltpu.VMEM((2, d_model, hc), BF16),
                  pltpu.VMEM((2, ff_shared, hc), BF16), pltpu.SemaphoreType.DMA((2,)), pltpu.SemaphoreType.DMA((2,)), pltpu.SemaphoreType.DMA((2,)))

    def yex_copy(e):
        return remote(ex_send.at[e], ex_recv.at[e], yex_send.at[e], yex_recv.at[e], y_peer)

    def routed_phase(sel, wg, wu, wd, g_sem, u_sem, d_sem):
        def gate_copy(e, slot):
            return pltpu.make_async_copy(weg_hbm.at[e], wg.at[slot], g_sem.at[slot])

        def up_copy(e, slot):
            return pltpu.make_async_copy(weu_hbm.at[e], wu.at[slot], u_sem.at[slot])

        def down_copy(e, slot):
            return pltpu.make_async_copy(wed_hbm.at[e], wd.at[slot], d_sem.at[slot])

        for slot in range(2):
            gate_copy(slot, slot).start()
            up_copy(slot, slot).start()
            down_copy(slot, slot).start()

        for copy in id_copies:
            copy.wait()
        e_pad = -(-experts // 8) * 8
        e_iota = lax.broadcasted_iota(jnp.int32, (e_pad, RANK_BLOCK), 0)
        row_i = lax.broadcasted_iota(jnp.int32, (RANK_BLOCK, RANK_BLOCK), 0)
        col_i = lax.broadcasted_iota(jnp.int32, (RANK_BLOCK, RANK_BLOCK), 1)
        upper = (row_i <= col_i).astype(F32).astype(BF16)
        blocks = [(q, b * RANK_BLOCK) for q in range(ep_size) for b in range(tok // RANK_BLOCK)]
        cap = jnp.float32(capacity)
        total = jnp.zeros((e_pad, 1), F32)
        rank_first = []
        for q, lo in blocks:
            first = ids_all[q, 0:1, lo:lo + RANK_BLOCK]
            hot = (e_iota == first).astype(F32)
            cum = dot(hot.astype(BF16), upper) + total
            rank_first.append(jnp.sum(cum * hot, axis=0, keepdims=True) - 1.0)
            total = total + jnp.sum(hot, axis=1, keepdims=True)
        load = jnp.minimum(total, cap)
        room = cap - load
        total = jnp.zeros((e_pad, 1), F32)
        slot_iota = lax.broadcasted_iota(jnp.int32, (slots, RANK_BLOCK), 0).astype(F32)
        base = (me * slots).astype(F32)
        for i, (q, lo) in enumerate(blocks):
            first = ids_all[q, 0:1, lo:lo + RANK_BLOCK]
            alt = ids_all[q, 1:2, lo:lo + RANK_BLOCK]
            kept = rank_first[i] < cap
            over = jnp.where(kept, 0.0, 1.0)
            hot = (e_iota == alt).astype(F32) * over
            cum = dot(hot.astype(BF16), upper) + total
            rank_alt = jnp.sum(cum * hot, axis=0, keepdims=True) - 1.0
            total = total + jnp.sum(hot, axis=1, keepdims=True)
            room_tok = jnp.sum(hot * room, axis=0, keepdims=True)
            load_tok = jnp.sum(hot * load, axis=0, keepdims=True)
            code_first = first.astype(F32) * pad_cap + rank_first[i]
            code_alt = jnp.where(rank_alt < room_tok, alt.astype(F32) * pad_cap + load_tok + rank_alt, -1.0)
            code = jnp.where(kept, code_first, code_alt)
            code_rows[q, :, lo:lo + RANK_BLOCK] = jnp.broadcast_to(code, (8, RANK_BLOCK))
            tok_off = q * tok + lo
            sel[:, tok_off:tok_off + RANK_BLOCK] = (slot_iota == code - base).astype(F32).astype(BF16)

        own_code = jnp.broadcast_to(code_rows[me][0:1, :], (LANES, tok))
        code_t = own_code.T
        code_col[...] = code_t

        wr_load.wait()
        x = x_all[me]
        w = wr[...]
        w_hi = w.astype(BF16)
        w_rest = w - w_hi.astype(F32)
        w_mid = w_rest.astype(BF16)
        w_lo = (w_rest - w_mid.astype(F32)).astype(BF16)
        logits = dot_bt(x, w_hi) + (dot_bt(x, w_mid) + dot_bt(x, w_lo))
        top = jnp.max(logits, axis=1, keepdims=True)
        prob = jnp.exp(logits - top)
        denom = jnp.sum(prob, axis=1, keepdims=True)
        lane_lo = lax.broadcasted_iota(jnp.int32, (tok, experts), 1).astype(F32) * pad_cap
        code_e = code_t[:, 0:experts]
        picked = (code_e >= lane_lo) & (code_e < lane_lo + pad_cap)
        gate = jnp.sum(jnp.where(picked, prob, 0.0), axis=1, keepdims=True) / denom
        gate_col[...] = jnp.broadcast_to(gate, (tok, LANES))

        for c in range(X_CHUNKS):
            xp_copies[c].wait_recv()
            fw_copies[c].start()
        sib_copy.wait()
        for c in range(X_CHUNKS):
            fw_copies[c].wait()
            xp_copies[c].wait_send()

        nc = 256

        @pl.loop(0, d_model // nc)
        def _(n):
            cols = pl.ds(pl.multiple_of(n * nc, nc), nc)
            acc = dot(sel[:, 0:tok], x_all[0, :, cols])
            for q in range(1, ep_size):
                acc = acc + dot(sel[:, q * tok:(q + 1) * tok], x_all[q, :, cols])
            slot_x[:, cols] = acc.astype(BF16)

        @pl.loop(0, local_experts)
        def _(e):
            slot = lax.rem(e, 2)
            gate_copy(e, slot).wait()
            up_copy(e, slot).wait()
            rows = slot_x[pl.ds(pl.multiple_of(e * pad_cap, pad_cap), pad_cap), :]
            g = dot_bt(wg[slot], rows)
            u = dot_bt(wu[slot], rows)
            hidden = (jax.nn.silu(g) * u).astype(BF16)

            @pl.when(e + 2 < local_experts)
            def _():
                gate_copy(e + 2, slot).start()
                up_copy(e + 2, slot).start()

            down_copy(e, slot).wait()
            ex_send[e] = dot_at(hidden, wd[slot, :, pl.ds(peer_off, half)])
            yex_copy(e).start()
            ex_own[e] = dot_at(hidden, wd[slot, :, pl.ds(own_off, half)])

            @pl.when(e + 2 < local_experts)
            def _():
                down_copy(e + 2, slot).start()

    pl.run_scoped(routed_phase, pltpu.VMEM((slots, ep_size * tok), BF16), pltpu.VMEM((2, ff_expert, d_model), BF16), pltpu.VMEM((2, ff_expert, d_model), BF16),
                  pltpu.VMEM((2, ff_expert, d_model), BF16), pltpu.SemaphoreType.DMA((2,)), pltpu.SemaphoreType.DMA((2,)), pltpu.SemaphoreType.DMA((2,)))

    res_load.wait()

    @pl.loop(0, n_half)
    def _(j):
        ysh_copy(j).wait()
        cols = pl.ds(pl.multiple_of(j * hc, hc), hc)
        sh_own[j] = res_half[:, cols].astype(F32) + (sh_own[j] + sh_recv[j])

    def ret_copy(e, who, s_sem, r_sem, dev):
        return remote(ret.at[e, who], ret.at[e, who], s_sem.at[e], r_sem.at[e], dev)

    @pl.loop(0, local_experts)
    def _(e):
        yex_copy(e).wait()
        ret[e, pl.ds(me, 1)] = (ex_own[e] + ex_recv[e]).astype(BF16).reshape(1, pad_cap, half)
        ret_copy(e, me, rx_send, rx_recv, xp_dev).start()
        ret_copy(e, me, rs_send, rs_recv, sib_dev).start()

        def finish(p):
            ret_copy(p, me, rx_send, rx_recv, xp_dev).wait()
            ret_copy(p, xp, rf_send, rf_recv, sib_dev).start()

        @pl.when(e > 0)
        def _():
            finish(e - 1)

        @pl.when(e == local_experts - 1)
        def _():
            finish(e)

    k_lanes = ep_size * pad_cap
    lane = lax.broadcasted_iota(jnp.int32, (tok, k_lanes), 1)
    owner = sum((lane >= q * pad_cap).astype(jnp.int32) for q in range(1, ep_size))
    lane_code = (lane + owner * (slots - pad_cap)).astype(F32)
    code_k = jnp.concatenate([code_col[...]] * 2, axis=1)[:, 0:k_lanes]

    @pl.loop(0, local_experts)
    def _(e):
        ret_copy(e, me, rs_send, rs_recv, sib_dev).wait()
        ret_copy(e, xp, rf_send, rf_recv, sib_dev).wait()
        pick = (code_k == lane_code + (e * pad_cap).astype(F32)).astype(F32).astype(BF16)
        rows = ret[e].reshape(k_lanes, half)
        gate = gate_col[:, 0:1]
        for j in range(n_half):
            sh_own[j] = sh_own[j] + gate * dot(pick, rows[:, j * hc:(j + 1) * hc])

    o_rows = tok // OUT_CHUNKS
    local_outs, y_outs = [], []
    for c in range(OUT_CHUNKS):
        rows = pl.ds(c * o_rows, o_rows)
        for j in range(n_half):
            out_half[rows, j * hc:(j + 1) * hc] = sh_own[j, rows, :].astype(BF16)
        dst = o_hbm.at[rows, pl.ds(own_off, half)]
        copy = remote(out_half.at[rows], dst, yo_send.at[c], yo_recv.at[c], y_peer)
        copy.start()
        y_outs.append(copy)
        copy = pltpu.make_async_copy(out_half.at[rows], dst, lo_sem.at[c])
        copy.start()
        local_outs.append(copy)
    for copy in y_outs + local_outs:
        copy.wait()


def solution(mesh):
    ep_size = mesh.shape["ep"]
    tok_spec = P(("dp", "ep"), None)
    id_spec = P(("dp", "ep"))

    def device_step(normed, residual, w_router, ws_gate, ws_up, ws_down, we_gate, we_up, we_down, first_id, alt_id):
        tok, d_model = normed.shape
        local_experts, _, ff_expert = we_gate.shape
        experts = local_experts * ep_size
        capacity = (5 * tok * ep_size + 4 * experts - 1) // (4 * experts)
        pad_cap = -(-capacity // 16) * 16
        half = d_model // 2
        hc = 256
        slots = local_experts * pad_cap
        dma = pltpu.SemaphoreType.DMA
        any_spec = pl.BlockSpec(memory_space=pl.ANY)
        vmem_spec = pl.BlockSpec(memory_space=pltpu.VMEM)
        return pl.pallas_call(
            functools.partial(moe_kernel, (experts, capacity, pad_cap, local_experts, ep_size)),
            out_shape=jax.ShapeDtypeStruct((tok, d_model), BF16),
            in_specs=[any_spec] * 9 + [vmem_spec] * 2,
            out_specs=any_spec,
            scratch_shapes=[
                pltpu.VMEM((ep_size, tok, d_model), BF16),
                pltpu.VMEM((ep_size, 8, tok), jnp.int32),
                pltpu.VMEM((ep_size, 8, tok), F32),
                pltpu.VMEM((tok, LANES), F32),
                pltpu.VMEM((tok, LANES), F32),
                pltpu.VMEM((slots, d_model), BF16),
                pltpu.VMEM((half // hc, tok, hc), F32),
                pltpu.VMEM((half // hc, tok, hc), F32),
                pltpu.VMEM((half // hc, tok, hc), F32),
                pltpu.VMEM((local_experts, pad_cap, half), F32),
                pltpu.VMEM((local_experts, pad_cap, half), F32),
                pltpu.VMEM((local_experts, pad_cap, half), F32),
                pltpu.VMEM((local_experts, ep_size, pad_cap, half), BF16),
                pltpu.VMEM((tok, half), BF16),
                pltpu.VMEM((tok, half), BF16),
                pltpu.VMEM((experts, d_model), F32),
                dma((3,)), dma((3,)), dma((3,)), dma((1,)), dma((1,)), dma((X_CHUNKS,)), dma((X_CHUNKS,)), dma((X_CHUNKS,)), dma((X_CHUNKS,)),
                dma((half // hc,)), dma((half // hc,)), dma((local_experts,)), dma((local_experts,)),
                dma((local_experts,)), dma((local_experts,)), dma((local_experts,)), dma((local_experts,)), dma((local_experts,)), dma((local_experts,)),
                dma((OUT_CHUNKS,)), dma((OUT_CHUNKS,)), dma((OUT_CHUNKS,)),
            ],
            compiler_params=pltpu.CompilerParams(collective_id=0, has_side_effects=True, vmem_limit_bytes=67043328),
        )(normed, residual, w_router.T, ws_gate, ws_up, ws_down, jnp.swapaxes(we_gate, 1, 2), jnp.swapaxes(we_up, 1, 2), we_down, first_id.reshape(1, tok), alt_id.reshape(1, tok))

    return jax.shard_map(device_step, mesh=mesh, in_specs=(tok_spec, tok_spec, P(None, None), P(None, 'tp'), P(None, 'tp'), P('tp', None), P('ep', None, 'tp'), P('ep', None, 'tp'), P('ep', 'tp', None), id_spec, id_spec), out_specs=tok_spec, check_vma=False)
```

```python
import functools

import jax
import jax.numpy as jnp
from jax import lax
from jax.experimental import pallas as pl
from jax.experimental.pallas import tpu as pltpu
from jax.sharding import PartitionSpec as P

MESH = pl.DeviceIdType.MESH
F32 = jnp.float32
BF16 = jnp.bfloat16
LANES = 128
RANK_BLOCK = 256
X_CHUNKS = 4
ROW_BLOCKS = 2
OUT_CHUNKS = 2
COL = 256
SUBS = 2
EARLY = 7


def dot(a, b):
    return jnp.dot(a, b, preferred_element_type=F32)


def dot_bt(a, b):
    return lax.dot_general(a, b, (((1,), (1,)), ((), ())), preferred_element_type=F32)


def dot_at(a, b):
    return lax.dot_general(a, b, (((0,), (0,)), ((), ())), preferred_element_type=F32)


def moe_kernel(dims, x_hbm, res_hbm, wr_hbm, wsg_hbm, wsu_hbm, wsd_hbm, weg_hbm, weu_hbm, wed_hbm, first_ref, alt_ref, o_hbm,
               x_near, x_far, ids_all, code_rows, code_col, gate_col, slot_x, sh_own, sh_send, sh_recv, ex_out, ex_recv, ret, out_half, res_half, wr,
               ld_sem, id_send, id_recv, sib_send, sib_recv, xp_send, xp_recv, fw_send, fw_recv,
               ysh_send, ysh_recv, yex_send, yex_recv, rs_send, rs_recv, rx_send, rx_recv, rf_send, rf_recv, yo_send, yo_recv, lo_sem):
    experts, capacity, pad_cap, local_experts, ep_size = dims
    tok, d_model = x_hbm.shape
    half = d_model // 2
    slots = local_experts * pad_cap
    ff_shared = wsg_hbm.shape[1]
    ff_expert = weg_hbm.shape[1]
    dp = lax.axis_index("dp")
    t = lax.axis_index("tp")
    me = lax.axis_index("ep")
    core = lax.rem(me, 2)
    sib = me + 1 - 2 * core
    xp = lax.rem(me + 2, ep_size)
    diag = lax.rem(sib + 2, ep_size)
    y_peer = (dp, 1 - t, me)
    sib_dev = (dp, t, sib)
    xp_dev = (dp, t, xp)
    diag_dev = (dp, t, diag)
    own_off = pl.multiple_of(t * half, half)
    peer_off = pl.multiple_of((1 - t) * half, half)
    x_rows = tok // X_CHUNKS
    r_rows = tok // ROW_BLOCKS
    n_hidden = ff_shared // COL
    n_half = half // COL
    sub_cols = half // SUBS
    sub_blocks = sub_cols // COL

    barrier = pltpu.get_barrier_semaphore()
    for dev in (y_peer, sib_dev, xp_dev, diag_dev):
        pl.semaphore_signal(barrier, inc=1, device_id=dev, device_id_type=MESH)

    def remote(src, dst, s_sem, r_sem, dev):
        return pltpu.make_async_remote_copy(src_ref=src, dst_ref=dst, send_sem=s_sem, recv_sem=r_sem, device_id=dev, device_id_type=MESH)

    id_copies = [remote(ids_all.at[me], ids_all.at[me], id_send.at[i], id_recv.at[i], dev) for i, dev in enumerate((sib_dev, xp_dev, diag_dev))]
    xp_copies = [remote(x_hbm.at[pl.ds(c * x_rows, x_rows)], x_far.at[c, 0], xp_send.at[c], xp_recv.at[c], xp_dev) for c in range(X_CHUNKS)]
    sib_copy = remote(x_hbm, x_near.at[1], sib_send.at[0], sib_recv.at[0], sib_dev)
    fw_copies = [remote(x_far.at[c, 0], x_far.at[c, 1], fw_send.at[c], fw_recv.at[c], sib_dev) for c in range(X_CHUNKS)]
    own_x = [pltpu.make_async_copy(x_hbm.at[pl.ds(r * r_rows, r_rows)], x_near.at[0, pl.ds(r * r_rows, r_rows)], ld_sem.at[r]) for r in range(ROW_BLOCKS)]
    res_load = pltpu.make_async_copy(res_hbm.at[:, pl.ds(own_off, half)], res_half, ld_sem.at[ROW_BLOCKS])
    wr_load = pltpu.make_async_copy(wr_hbm, wr, ld_sem.at[ROW_BLOCKS + 1])

    def ysh_copy(r, j):
        return remote(sh_send.at[r, j], sh_recv.at[r, j], ysh_send.at[r, j], ysh_recv.at[r, j], y_peer)

    def shared_phase(act, wg, wu, wd, g_sem, u_sem, d_sem):
        def gate_copy(c, slot):
            return pltpu.make_async_copy(wsg_hbm.at[:, pl.ds(pl.multiple_of(lax.rem(c, n_hidden) * COL, COL), COL)], wg.at[slot], g_sem.at[slot])

        def up_copy(c, slot):
            return pltpu.make_async_copy(wsu_hbm.at[:, pl.ds(pl.multiple_of(lax.rem(c, n_hidden) * COL, COL), COL)], wu.at[slot], u_sem.at[slot])

        def down_copy(k, slot):
            j = lax.rem(k, 2 * n_half)
            col = jnp.where(j < n_half, peer_off + j * COL, own_off + (j - n_half) * COL)
            return pltpu.make_async_copy(wsd_hbm.at[:, pl.ds(pl.multiple_of(col, COL), COL)], wd.at[slot], d_sem.at[slot])

        own_x[0].start()
        for slot in range(2):
            gate_copy(jnp.int32(slot), slot).start()
            up_copy(jnp.int32(slot), slot).start()
        for copy in own_x[1:]:
            copy.start()
        for slot in range(2):
            down_copy(jnp.int32(slot), slot).start()
        res_load.start()
        wr_load.start()
        ids_all[pl.ds(me, 1), 0:1, :] = first_ref[...].reshape(1, 1, tok)
        ids_all[pl.ds(me, 1), 1:2, :] = alt_ref[...].reshape(1, 1, tok)
        pl.semaphore_wait(barrier, 4)
        for copy in xp_copies:
            copy.start()
        sib_copy.start()
        for copy in id_copies:
            copy.start()

        for r in range(ROW_BLOCKS):
            own_x[r].wait()

            @pl.loop(0, n_hidden)
            def _(c):
                k = c + r * n_hidden
                slot = lax.rem(k, 2)
                gate_copy(k, slot).wait()
                up_copy(k, slot).wait()
                x = x_near[0, r * r_rows:(r + 1) * r_rows, :]
                g = dot(x, wg[slot])
                u = dot(x, wu[slot])
                act[:, pl.ds(pl.multiple_of(c * COL, COL), COL)] = (jax.nn.silu(g) * u).astype(BF16)

                @pl.when(k + 2 < ROW_BLOCKS * n_hidden)
                def _():
                    gate_copy(k + 2, slot).start()
                    up_copy(k + 2, slot).start()

            @pl.loop(0, n_half)
            def _(j):
                k = j + r * 2 * n_half
                slot = lax.rem(k, 2)
                down_copy(k, slot).wait()
                sh_send[r, j] = dot(act[...], wd[slot])
                ysh_copy(r, j).start()
                down_copy(k + 2, slot).start()

            @pl.loop(0, n_half)
            def _(j):
                k = j + r * 2 * n_half + n_half
                slot = lax.rem(k, 2)
                down_copy(k, slot).wait()
                sh_own[j, r * r_rows:(r + 1) * r_rows, :] = dot(act[...], wd[slot])

                @pl.when(k + 2 < ROW_BLOCKS * 2 * n_half)
                def _():
                    down_copy(k + 2, slot).start()

    pl.run_scoped(shared_phase, pltpu.VMEM((r_rows, ff_shared), BF16), pltpu.VMEM((2, d_model, COL), BF16), pltpu.VMEM((2, d_model, COL), BF16),
                  pltpu.VMEM((2, ff_shared, COL), BF16), pltpu.SemaphoreType.DMA((2,)), pltpu.SemaphoreType.DMA((2,)), pltpu.SemaphoreType.DMA((2,)))

    def yex_copy(sub, e):
        cols = pl.ds(pl.multiple_of(peer_off + sub * sub_cols, sub_cols), sub_cols)
        return remote(ex_out.at[e, pl.ds(0, pad_cap), cols], ex_recv.at[sub, e, pl.ds(0, pad_cap)], yex_send.at[sub, e], yex_recv.at[sub, e], y_peer)

    def routed_phase(sel_near, sel_far, wg, wu, wd, g_sem, u_sem, d_sem):
        def gate_copy(e, slot):
            return pltpu.make_async_copy(weg_hbm.at[e], wg.at[slot], g_sem.at[slot])

        def up_copy(e, slot):
            return pltpu.make_async_copy(weu_hbm.at[e], wu.at[slot], u_sem.at[slot])

        def down_copy(e, slot):
            return pltpu.make_async_copy(wed_hbm.at[e], wd.at[slot], d_sem.at[slot])

        for slot in range(2):
            gate_copy(slot, slot).start()
            up_copy(slot, slot).start()
            down_copy(slot, slot).start()

        with jax.named_scope("routing"):
            for copy in id_copies:
                copy.wait()
            e_pad = -(-experts // 8) * 8
            e_iota = lax.broadcasted_iota(jnp.int32, (e_pad, RANK_BLOCK), 0)
            row_i = lax.broadcasted_iota(jnp.int32, (RANK_BLOCK, RANK_BLOCK), 0)
            col_i = lax.broadcasted_iota(jnp.int32, (RANK_BLOCK, RANK_BLOCK), 1)
            upper = (row_i <= col_i).astype(F32).astype(BF16)
            blocks = [(q, b * RANK_BLOCK) for q in range(ep_size) for b in range(tok // RANK_BLOCK)]
            cap = jnp.float32(capacity)
            total = jnp.zeros((e_pad, 1), F32)
            rank_first = []
            for q, lo in blocks:
                first = ids_all[q, 0:1, lo:lo + RANK_BLOCK]
                hot = (e_iota == first).astype(F32)
                cum = dot(hot.astype(BF16), upper) + total
                rank_first.append(jnp.sum(cum * hot, axis=0, keepdims=True) - 1.0)
                total = total + jnp.sum(hot, axis=1, keepdims=True)
            load = jnp.minimum(total, cap)
            room = cap - load
            total = jnp.zeros((e_pad, 1), F32)
            for i, (q, lo) in enumerate(blocks):
                first = ids_all[q, 0:1, lo:lo + RANK_BLOCK]
                alt = ids_all[q, 1:2, lo:lo + RANK_BLOCK]
                kept = rank_first[i] < cap
                over = jnp.where(kept, 0.0, 1.0)
                hot = (e_iota == alt).astype(F32) * over
                cum = dot(hot.astype(BF16), upper) + total
                rank_alt = jnp.sum(cum * hot, axis=0, keepdims=True) - 1.0
                total = total + jnp.sum(hot, axis=1, keepdims=True)
                room_tok = jnp.sum(hot * room, axis=0, keepdims=True)
                load_tok = jnp.sum(hot * load, axis=0, keepdims=True)
                code_first = first.astype(F32) * pad_cap + rank_first[i]
                code_alt = jnp.where(rank_alt < room_tok, alt.astype(F32) * pad_cap + load_tok + rank_alt, -1.0)
                code = jnp.where(kept, code_first, code_alt)
                code_rows[q, :, lo:lo + RANK_BLOCK] = jnp.broadcast_to(code, (8, RANK_BLOCK))

            base = (me * slots).astype(F32)
            slot_iota = lax.broadcasted_iota(jnp.int32, (slots, x_rows), 0).astype(F32) + base
            for i, q in enumerate((me, sib)):
                codes = code_rows[q]
                for lo in range(0, tok, x_rows):
                    sel_near[:, i * tok + lo:i * tok + lo + x_rows] = (slot_iota == codes[0:1, lo:lo + x_rows]).astype(F32).astype(BF16)
            for i, q in enumerate((xp, diag)):
                codes = code_rows[q]
                for c in range(X_CHUNKS):
                    sel_far[c, :, i * x_rows:(i + 1) * x_rows] = (slot_iota == codes[0:1, c * x_rows:(c + 1) * x_rows]).astype(F32).astype(BF16)

            code_t = jnp.broadcast_to(code_rows[me][0:1, :], (LANES, tok)).T
            code_col[...] = code_t

        with jax.named_scope("router"):
            wr_load.wait()
            x = x_near[0]
            w = wr[...]
            w_hi = w.astype(BF16)
            w_rest = w - w_hi.astype(F32)
            w_mid = w_rest.astype(BF16)
            w_lo = (w_rest - w_mid.astype(F32)).astype(BF16)
            logits = dot_bt(x, w_hi) + (dot_bt(x, w_mid) + dot_bt(x, w_lo))
            top = jnp.max(logits, axis=1, keepdims=True)
            prob = jnp.exp(logits - top)
            denom = jnp.sum(prob, axis=1, keepdims=True)
            lane_lo = lax.broadcasted_iota(jnp.int32, (tok, experts), 1).astype(F32) * pad_cap
            code_e = code_t[:, 0:experts]
            picked = (code_e >= lane_lo) & (code_e < lane_lo + pad_cap)
            gate = jnp.sum(jnp.where(picked, prob, 0.0), axis=1, keepdims=True) / denom
            gate_col[...] = jnp.broadcast_to(gate, (tok, LANES))

        nc = 256
        with jax.named_scope("near"):
            sib_copy.wait()

            @pl.loop(0, d_model // nc)
            def _(n):
                cols = pl.ds(pl.multiple_of(n * nc, nc), nc)
                acc = dot(sel_near[:, 0:tok], x_near[0, :, cols]) + dot(sel_near[:, tok:2 * tok], x_near[1, :, cols])
                slot_x[:, cols] = acc.astype(BF16)

        with jax.named_scope("far"):
            xp_copies[0].wait_recv()
            fw_copies[0].start()
            for c in range(X_CHUNKS):
                if c + 1 < X_CHUNKS:
                    xp_copies[c + 1].wait_recv()
                    fw_copies[c + 1].start()
                fw_copies[c].wait_recv()

                @pl.loop(0, d_model // nc)
                def _(n):
                    cols = pl.ds(pl.multiple_of(n * nc, nc), nc)
                    rows = x_far[c, :, :, cols].reshape(2 * x_rows, nc)
                    slot_x[:, cols] += dot(sel_far[c], rows).astype(BF16)

        with jax.named_scope("experts"):
            @pl.loop(0, local_experts)
            def _(e):
                slot = lax.rem(e, 2)
                gate_copy(e, slot).wait()
                up_copy(e, slot).wait()
                rows = slot_x[pl.ds(pl.multiple_of(e * pad_cap, pad_cap), pad_cap), :]
                g = dot_bt(wg[slot], rows)
                u = dot_bt(wu[slot], rows)
                hidden = (jax.nn.silu(g) * u).astype(BF16)

                @pl.when(e + 2 < local_experts)
                def _():
                    gate_copy(e + 2, slot).start()
                    up_copy(e + 2, slot).start()

                down_copy(e, slot).wait()
                ex_out[e] = dot_at(hidden, wd[slot])
                yex_copy(0, e).start()

                @pl.when(e < EARLY)
                def _():
                    yex_copy(1, e).start()

                @pl.when(e + 2 < local_experts)
                def _():
                    down_copy(e + 2, slot).start()

            @pl.loop(EARLY, local_experts)
            def _(e):
                yex_copy(1, e).start()

    pl.run_scoped(routed_phase, pltpu.VMEM((slots, 2 * tok), BF16), pltpu.VMEM((X_CHUNKS, slots, 2 * x_rows), BF16),
                  pltpu.VMEM((2, ff_expert, d_model), BF16), pltpu.VMEM((2, ff_expert, d_model), BF16),
                  pltpu.VMEM((2, ff_expert, d_model), BF16), pltpu.SemaphoreType.DMA((2,)), pltpu.SemaphoreType.DMA((2,)), pltpu.SemaphoreType.DMA((2,)))

    with jax.named_scope("fin_shared"):
        for copy in xp_copies + fw_copies:
            copy.wait_send()
        res_load.wait()
        for r in range(ROW_BLOCKS):
            @pl.loop(0, n_half)
            def _(j):
                ysh_copy(r, j).wait()
                cols = pl.ds(pl.multiple_of(j * COL, COL), COL)
                rows = slice(r * r_rows, (r + 1) * r_rows)
                sh_own[j, rows, :] = res_half[rows, cols].astype(F32) + (sh_own[j, rows, :] + sh_recv[r, j])

    def ret_copy(sub, e, who, s_sem, r_sem, dev):
        return remote(ret.at[sub, e, who], ret.at[sub, e, who], s_sem.at[sub, e], r_sem.at[sub, e], dev)

    k_lanes = ep_size * pad_cap
    lane = lax.broadcasted_iota(jnp.int32, (tok, k_lanes), 1)
    owner = sum((lane >= q * pad_cap).astype(jnp.int32) for q in range(1, ep_size))
    lane_code = (lane + owner * (slots - pad_cap)).astype(F32)

    def forward(sub, e):
        ret_copy(sub, e, me, rx_send, rx_recv, xp_dev).wait()
        ret_copy(sub, e, xp, rf_send, rf_recv, sib_dev).start()

    def combine(sub, e):
        ret_copy(sub, e, me, rs_send, rs_recv, sib_dev).wait()
        ret_copy(sub, e, xp, rf_send, rf_recv, sib_dev).wait()
        code_k = jnp.concatenate([code_col[...]] * 2, axis=1)[:, 0:k_lanes]
        pick = (code_k == lane_code + jnp.asarray(e * pad_cap, jnp.int32).astype(F32)).astype(F32).astype(BF16)
        rows = ret[sub, e].reshape(k_lanes, sub_cols)
        gate = gate_col[:, 0:1]
        for j in range(sub_blocks):
            jj = sub * sub_blocks + j
            sh_own[jj] = sh_own[jj] + gate * dot(pick, rows[:, j * COL:(j + 1) * COL])

    o_rows = tok // OUT_CHUNKS

    def out_copies(sub, c):
        rows = pl.ds(c * o_rows, o_rows)
        src = out_half.at[sub, rows]
        dst = o_hbm.at[rows, pl.ds(pl.multiple_of(own_off + sub * sub_cols, sub_cols), sub_cols)]
        return remote(src, dst, yo_send.at[sub, c], yo_recv.at[sub, c], y_peer), pltpu.make_async_copy(src, dst, lo_sem.at[sub, c])

    def emit(sub):
        for c in range(OUT_CHUNKS):
            rows = slice(c * o_rows, (c + 1) * o_rows)
            for j in range(sub_blocks):
                out_half[sub, rows, j * COL:(j + 1) * COL] = sh_own[sub * sub_blocks + j, rows, :].astype(BF16)
            if sub > 0:
                for copy in out_copies(sub, c):
                    copy.start()

    lag = 3
    for sub in range(SUBS):
        with jax.named_scope(f"ret{sub}"):
            @pl.loop(0, local_experts)
            def _(e):
                yex_copy(sub, e).wait()
                own_cols = pl.ds(pl.multiple_of(own_off + sub * sub_cols, sub_cols), sub_cols)
                ret[sub, e, pl.ds(me, 1)] = (ex_out[e, :, own_cols] + ex_recv[sub, e]).astype(BF16).reshape(1, pad_cap, sub_cols)
                ret_copy(sub, e, me, rx_send, rx_recv, xp_dev).start()
                ret_copy(sub, e, me, rs_send, rs_recv, sib_dev).start()

                @pl.when(e >= 1)
                def _():
                    forward(sub, e - 1)

                @pl.when(e >= lag)
                def _():
                    combine(sub, e - lag)

            if sub > 0:
                for c in range(OUT_CHUNKS):
                    for copy in out_copies(0, c):
                        copy.start()
            forward(sub, local_experts - 1)

        with jax.named_scope(f"drain{sub}"):
            @pl.loop(local_experts - lag, local_experts)
            def _(e):
                combine(sub, e)

            emit(sub)

    with jax.named_scope("out"):
        for sub in range(SUBS):
            for c in range(OUT_CHUNKS):
                for copy in out_copies(sub, c):
                    copy.wait()


def solution(mesh):
    ep_size = mesh.shape["ep"]
    tok_spec = P(("dp", "ep"), None)
    id_spec = P(("dp", "ep"))

    def device_step(normed, residual, w_router, ws_gate, ws_up, ws_down, we_gate, we_up, we_down, first_id, alt_id):
        tok, d_model = normed.shape
        local_experts, _, ff_expert = we_gate.shape
        experts = local_experts * ep_size
        capacity = (5 * tok * ep_size + 4 * experts - 1) // (4 * experts)
        pad_cap = -(-capacity // 16) * 16
        half = d_model // 2
        slots = local_experts * pad_cap
        n_half = half // COL
        x_rows = tok // X_CHUNKS
        r_rows = tok // ROW_BLOCKS
        sub_cols = half // SUBS
        dma = pltpu.SemaphoreType.DMA
        any_spec = pl.BlockSpec(memory_space=pl.ANY)
        vmem_spec = pl.BlockSpec(memory_space=pltpu.VMEM)
        per_ret = dma((SUBS, local_experts))
        return pl.pallas_call(
            functools.partial(moe_kernel, (experts, capacity, pad_cap, local_experts, ep_size)),
            out_shape=jax.ShapeDtypeStruct((tok, d_model), BF16),
            in_specs=[any_spec] * 9 + [vmem_spec] * 2,
            out_specs=any_spec,
            scratch_shapes=[
                pltpu.VMEM((2, tok, d_model), BF16),
                pltpu.VMEM((X_CHUNKS, 2, x_rows, d_model), BF16),
                pltpu.VMEM((ep_size, 8, tok), jnp.int32),
                pltpu.VMEM((ep_size, 8, tok), F32),
                pltpu.VMEM((tok, LANES), F32),
                pltpu.VMEM((tok, LANES), F32),
                pltpu.VMEM((slots, d_model), BF16),
                pltpu.VMEM((n_half, tok, COL), F32),
                pltpu.VMEM((ROW_BLOCKS, n_half, r_rows, COL), F32),
                pltpu.VMEM((ROW_BLOCKS, n_half, r_rows, COL), F32),
                pltpu.VMEM((local_experts, pad_cap, d_model), F32),
                pltpu.VMEM((SUBS, local_experts, pad_cap, sub_cols), F32),
                pltpu.VMEM((SUBS, local_experts, ep_size, pad_cap, sub_cols), BF16),
                pltpu.VMEM((SUBS, tok, sub_cols), BF16),
                pltpu.VMEM((tok, half), BF16),
                pltpu.VMEM((experts, d_model), F32),
                dma((ROW_BLOCKS + 2,)), dma((3,)), dma((3,)), dma((1,)), dma((1,)), dma((X_CHUNKS,)), dma((X_CHUNKS,)), dma((X_CHUNKS,)), dma((X_CHUNKS,)),
                dma((ROW_BLOCKS, n_half)), dma((ROW_BLOCKS, n_half)), per_ret, per_ret, per_ret, per_ret, per_ret, per_ret, per_ret, per_ret,
                dma((SUBS, OUT_CHUNKS)), dma((SUBS, OUT_CHUNKS)), dma((SUBS, OUT_CHUNKS)),
            ],
            compiler_params=pltpu.CompilerParams(collective_id=0, has_side_effects=True, vmem_limit_bytes=67043328),
        )(normed, residual, w_router.T, ws_gate, ws_up, ws_down, jnp.swapaxes(we_gate, 1, 2), jnp.swapaxes(we_up, 1, 2), we_down,
          first_id.reshape(1, tok), alt_id.reshape(1, tok))

    return jax.shard_map(device_step, mesh=mesh, in_specs=(tok_spec, tok_spec, P(None, None), P(None, 'tp'), P(None, 'tp'), P('tp', None), P('ep', None, 'tp'), P('ep', None, 'tp'), P('ep', 'tp', None), id_spec, id_spec), out_specs=tok_spec, check_vma=False)
```

```python
import functools

import jax
import jax.numpy as jnp
from jax import lax
from jax.experimental import pallas as pl
from jax.experimental.pallas import tpu as pltpu
from jax.sharding import PartitionSpec as P

MESH = pl.DeviceIdType.MESH
F32 = jnp.float32
BF16 = jnp.bfloat16
LANES = 128
RANK_BLOCK = 256
X_CHUNKS = 4
ROW_BLOCKS = 2
COL = 256
SUBS = 2
EARLY_GROUPS = 2
SHARED_BUFS = 4


def dot(a, b):
    return jnp.dot(a, b, preferred_element_type=F32)


def dot_bt(a, b):
    return lax.dot_general(a, b, (((1,), (1,)), ((), ())), preferred_element_type=F32)


def dot_at(a, b):
    return lax.dot_general(a, b, (((0,), (0,)), ((), ())), preferred_element_type=F32)


def moe_kernel(dims, x_hbm, res_hbm, wr_hbm, wsg_hbm, wsu_hbm, wsd_hbm, weg_hbm, weu_hbm, wed_hbm, first_ref, alt_ref, o_hbm,
               x_near, x_far, ids_all, code_rows, code_col, gate_col, slot_x, sh_own, sh_send, sh_recv, ex_own, ex_send, ex_recv, ret, out_half, res_half, wr,
               ld_sem, id_send, id_recv, sib_send, sib_recv, xp_send, xp_recv, fw_send, fw_recv,
               ysh_send, ysh_recv, yex_send, yex_recv, rs_send, rs_recv, rx_send, rx_recv, rf_send, rf_recv, yo_send, yo_recv, lo_sem):
    experts, capacity, window, pack, bounds, local_experts, ep_size = dims
    groups = len(bounds) - 1
    last_expert = [-(-min(b, local_experts * capacity) // capacity) - 1 for b in bounds[1:]]
    tok, d_model = x_hbm.shape
    half = d_model // 2
    slots = local_experts * window
    spare = pack - local_experts * capacity
    ff_shared = wsg_hbm.shape[1]
    ff_expert = weg_hbm.shape[1]
    dp = lax.axis_index("dp")
    t = lax.axis_index("tp")
    me = lax.axis_index("ep")
    core = lax.rem(me, 2)
    sib = me + 1 - 2 * core
    xp = lax.rem(me + 2, ep_size)
    diag = lax.rem(sib + 2, ep_size)
    y_peer = (dp, 1 - t, me)
    sib_dev = (dp, t, sib)
    xp_dev = (dp, t, xp)
    diag_dev = (dp, t, diag)
    own_off = pl.multiple_of(t * half, half)
    peer_off = pl.multiple_of((1 - t) * half, half)
    x_rows = tok // X_CHUNKS
    r_rows = tok // ROW_BLOCKS
    n_hidden = ff_shared // COL
    n_half = half // COL
    sub_cols = half // SUBS
    sub_blocks = sub_cols // COL

    barrier = pltpu.get_barrier_semaphore()
    for dev in (y_peer, sib_dev, xp_dev, diag_dev):
        pl.semaphore_signal(barrier, inc=1, device_id=dev, device_id_type=MESH)

    def remote(src, dst, s_sem, r_sem, dev):
        return pltpu.make_async_remote_copy(src_ref=src, dst_ref=dst, send_sem=s_sem, recv_sem=r_sem, device_id=dev, device_id_type=MESH)

    id_copies = [remote(ids_all.at[me], ids_all.at[me], id_send.at[i], id_recv.at[i], dev) for i, dev in enumerate((sib_dev, xp_dev, diag_dev))]
    xp_copies = [remote(x_hbm.at[pl.ds(c * x_rows, x_rows)], x_far.at[c, 0], xp_send.at[c], xp_recv.at[c], xp_dev) for c in range(X_CHUNKS)]
    sib_copy = remote(x_hbm, x_near.at[1], sib_send.at[0], sib_recv.at[0], sib_dev)
    fw_copies = [remote(x_far.at[c, 0], x_far.at[c, 1], fw_send.at[c], fw_recv.at[c], sib_dev) for c in range(X_CHUNKS)]
    own_x = [pltpu.make_async_copy(x_hbm.at[pl.ds(r * r_rows, r_rows)], x_near.at[0, pl.ds(r * r_rows, r_rows)], ld_sem.at[r]) for r in range(ROW_BLOCKS)]
    res_load = pltpu.make_async_copy(res_hbm.at[:, pl.ds(own_off, half)], res_half, ld_sem.at[ROW_BLOCKS])
    wr_load = pltpu.make_async_copy(wr_hbm, wr, ld_sem.at[ROW_BLOCKS + 1])

    def ysh_copy(r, j):
        return remote(sh_send.at[r, j], sh_recv.at[r, j], ysh_send.at[r, j], ysh_recv.at[r, j], y_peer)

    def shared_phase(act, wg, wu, wd, g_sem, u_sem, d_sem):
        def gate_copy(c, slot):
            return pltpu.make_async_copy(wsg_hbm.at[:, pl.ds(pl.multiple_of(lax.rem(c, n_hidden) * COL, COL), COL)], wg.at[slot], g_sem.at[slot])

        def up_copy(c, slot):
            return pltpu.make_async_copy(wsu_hbm.at[:, pl.ds(pl.multiple_of(lax.rem(c, n_hidden) * COL, COL), COL)], wu.at[slot], u_sem.at[slot])

        def down_copy(k, slot):
            j = lax.rem(k, 2 * n_half)
            col = jnp.where(j < n_half, peer_off + j * COL, own_off + (j - n_half) * COL)
            return pltpu.make_async_copy(wsd_hbm.at[:, pl.ds(pl.multiple_of(col, COL), COL)], wd.at[slot], d_sem.at[slot])

        own_x[0].start()
        gate_copy(jnp.int32(0), 0).start()
        up_copy(jnp.int32(0), 0).start()
        for copy in own_x[1:]:
            copy.start()
        for slot in range(1, SHARED_BUFS):
            gate_copy(jnp.int32(slot), slot).start()
            up_copy(jnp.int32(slot), slot).start()
        for slot in range(SHARED_BUFS):
            down_copy(jnp.int32(slot), slot).start()
        res_load.start()
        wr_load.start()
        ids_all[pl.ds(me, 1), 0:1, :] = first_ref[...].reshape(1, 1, tok)
        ids_all[pl.ds(me, 1), 1:2, :] = alt_ref[...].reshape(1, 1, tok)
        pl.semaphore_wait(barrier, 4)
        for copy in id_copies:
            copy.start()
        for copy in xp_copies:
            copy.start()
        sib_copy.start()

        for r in range(ROW_BLOCKS):
            own_x[r].wait()

            with jax.named_scope(f"gateup{r}"):
                @pl.loop(0, n_hidden)
                def _(c):
                    k = c + r * n_hidden
                    slot = lax.rem(k, SHARED_BUFS)
                    gate_copy(k, slot).wait()
                    up_copy(k, slot).wait()
                    x = x_near[0, r * r_rows:(r + 1) * r_rows, :]
                    g = dot(x, wg[slot])
                    u = dot(x, wu[slot])
                    act[:, pl.ds(pl.multiple_of(c * COL, COL), COL)] = (jax.nn.silu(g) * u).astype(BF16)

                    @pl.when(k + SHARED_BUFS < ROW_BLOCKS * n_hidden)
                    def _():
                        gate_copy(k + SHARED_BUFS, slot).start()
                        up_copy(k + SHARED_BUFS, slot).start()

            def down_step(k, slot, store):
                down_copy(k, slot).wait()
                store(dot(act[...], wd[slot]))

                @pl.when(k + SHARED_BUFS < ROW_BLOCKS * 2 * n_half)
                def _():
                    down_copy(k + SHARED_BUFS, slot).start()

            with jax.named_scope(f"downpeer{r}"):
                @pl.loop(0, n_half)
                def _(j):
                    k = j + r * 2 * n_half

                    def store(value):
                        sh_send[r, j] = value
                        ysh_copy(r, j).start()

                    down_step(k, lax.rem(k, SHARED_BUFS), store)

            with jax.named_scope(f"downown{r}"):
                @pl.loop(0, n_half)
                def _(j):
                    k = j + r * 2 * n_half + n_half

                    def store(value):
                        sh_own[j, r * r_rows:(r + 1) * r_rows, :] = value

                    down_step(k, lax.rem(k, SHARED_BUFS), store)

    shared_sems = [pltpu.SemaphoreType.DMA((SHARED_BUFS,))] * 3
    pl.run_scoped(shared_phase, pltpu.VMEM((r_rows, ff_shared), BF16), pltpu.VMEM((SHARED_BUFS, d_model, COL), BF16), pltpu.VMEM((SHARED_BUFS, d_model, COL), BF16),
                  pltpu.VMEM((SHARED_BUFS, ff_shared, COL), BF16), *shared_sems)

    def yex_copy(sub, i):
        rows = pl.ds(bounds[i], bounds[i + 1] - bounds[i])
        return remote(ex_send.at[sub, rows], ex_recv.at[sub, rows], yex_send.at[sub, i], yex_recv.at[sub, i], y_peer)

    def expert_base(ids):
        owner = sum((ids >= q * local_experts).astype(jnp.int32) for q in range(1, ep_size))
        return (ids * capacity + owner * spare).astype(F32)

    def routed_phase(sel_near, sel_far, wg, wu, wd, g_sem, u_sem, d_sem):
        def gate_copy(e, slot):
            return pltpu.make_async_copy(weg_hbm.at[e], wg.at[slot], g_sem.at[slot])

        def up_copy(e, slot):
            return pltpu.make_async_copy(weu_hbm.at[e], wu.at[slot], u_sem.at[slot])

        def down_copy(e, slot):
            return pltpu.make_async_copy(wed_hbm.at[e], wd.at[slot], d_sem.at[slot])

        for slot in range(2):
            gate_copy(slot, slot).start()
            up_copy(slot, slot).start()
            down_copy(slot, slot).start()

        with jax.named_scope("routing"):
            for copy in id_copies:
                copy.wait()
            e_pad = -(-experts // 8) * 8
            e_iota = lax.broadcasted_iota(jnp.int32, (e_pad, RANK_BLOCK), 0)
            row_i = lax.broadcasted_iota(jnp.int32, (RANK_BLOCK, RANK_BLOCK), 0)
            col_i = lax.broadcasted_iota(jnp.int32, (RANK_BLOCK, RANK_BLOCK), 1)
            upper = (row_i <= col_i).astype(F32).astype(BF16)
            blocks = [(q, b * RANK_BLOCK) for q in range(ep_size) for b in range(tok // RANK_BLOCK)]
            cap = jnp.float32(capacity)
            total = jnp.zeros((e_pad, 1), F32)
            rank_first = []
            for q, lo in blocks:
                first = ids_all[q, 0:1, lo:lo + RANK_BLOCK]
                hot = (e_iota == first).astype(F32)
                cum = dot(hot.astype(BF16), upper) + total
                rank_first.append(jnp.sum(cum * hot, axis=0, keepdims=True) - 1.0)
                total = total + jnp.sum(hot, axis=1, keepdims=True)
            load = jnp.minimum(total, cap)
            room = cap - load
            total = jnp.zeros((e_pad, 1), F32)
            for i, (q, lo) in enumerate(blocks):
                first = ids_all[q, 0:1, lo:lo + RANK_BLOCK]
                alt = ids_all[q, 1:2, lo:lo + RANK_BLOCK]
                kept = rank_first[i] < cap
                over = jnp.where(kept, 0.0, 1.0)
                hot = (e_iota == alt).astype(F32) * over
                cum = dot(hot.astype(BF16), upper) + total
                rank_alt = jnp.sum(cum * hot, axis=0, keepdims=True) - 1.0
                total = total + jnp.sum(hot, axis=1, keepdims=True)
                room_tok = jnp.sum(hot * room, axis=0, keepdims=True)
                load_tok = jnp.sum(hot * load, axis=0, keepdims=True)
                code_first = expert_base(first) + rank_first[i]
                code_alt = jnp.where(rank_alt < room_tok, expert_base(alt) + load_tok + rank_alt, -1.0)
                code = jnp.where(kept, code_first, code_alt)
                code_rows[q, :, lo:lo + RANK_BLOCK] = jnp.broadcast_to(code, (8, RANK_BLOCK))

            pos = lax.broadcasted_iota(jnp.int32, (slots, x_rows), 0)
            slot_expert = sum((pos >= e * window).astype(jnp.int32) for e in range(1, local_experts))
            first_row = slot_expert * capacity
            row = (first_row // 8) * 8 + (pos - slot_expert * window)
            slot_code = jnp.where((row >= first_row) & (row < first_row + capacity), row + me * pack, -2).astype(F32)
            for i, q in enumerate((me, sib)):
                codes = code_rows[q]
                for lo in range(0, tok, x_rows):
                    sel_near[:, i * tok + lo:i * tok + lo + x_rows] = (slot_code == codes[0:1, lo:lo + x_rows]).astype(F32).astype(BF16)
            for i, q in enumerate((xp, diag)):
                codes = code_rows[q]
                for c in range(X_CHUNKS):
                    sel_far[c, :, i * x_rows:(i + 1) * x_rows] = (slot_code == codes[0:1, c * x_rows:(c + 1) * x_rows]).astype(F32).astype(BF16)

            code_t = jnp.broadcast_to(code_rows[me][0:1, :], (LANES, tok)).T
            code_col[...] = code_t

        with jax.named_scope("router"):
            wr_load.wait()
            x = x_near[0]
            w = wr[...]
            w_hi = w.astype(BF16)
            w_rest = w - w_hi.astype(F32)
            w_mid = w_rest.astype(BF16)
            w_lo = (w_rest - w_mid.astype(F32)).astype(BF16)
            logits = dot_bt(x, w_hi) + (dot_bt(x, w_mid) + dot_bt(x, w_lo))
            top = jnp.max(logits, axis=1, keepdims=True)
            prob = jnp.exp(logits - top)
            denom = jnp.sum(prob, axis=1, keepdims=True)
            lane_lo = expert_base(lax.broadcasted_iota(jnp.int32, (tok, experts), 1))
            code_e = code_t[:, 0:experts]
            picked = (code_e >= lane_lo) & (code_e < lane_lo + cap)
            gate = jnp.sum(jnp.where(picked, prob, 0.0), axis=1, keepdims=True) / denom
            gate_col[...] = jnp.broadcast_to(gate, (tok, LANES))

        nc = 512
        with jax.named_scope("near"):
            sib_copy.wait()

            @pl.loop(0, d_model // nc)
            def _(n):
                cols = pl.ds(pl.multiple_of(n * nc, nc), nc)
                slot_x[:, cols] = dot(sel_near[...], x_near[:, :, cols].reshape(2 * tok, nc)).astype(BF16)

        with jax.named_scope("far"):
            xp_copies[0].wait_recv()
            fw_copies[0].start()
            for c in range(X_CHUNKS):
                if c + 1 < X_CHUNKS:
                    xp_copies[c + 1].wait_recv()
                    fw_copies[c + 1].start()
                fw_copies[c].wait_recv()

                @pl.loop(0, d_model // nc)
                def _(n):
                    cols = pl.ds(pl.multiple_of(n * nc, nc), nc)
                    rows = x_far[c, :, :, cols].reshape(2 * x_rows, nc)
                    slot_x[:, cols] += dot(sel_far[c], rows).astype(BF16)

        with jax.named_scope("experts"):
            for sub in range(SUBS):
                ex_send[sub, 0:8, :] = jnp.zeros((8, sub_cols), F32)
                ex_own[sub, 0:8, :] = jnp.zeros((8, sub_cols), F32)

            @pl.loop(0, local_experts)
            def _(e):
                slot = lax.rem(e, 2)
                gate_copy(e, slot).wait()
                up_copy(e, slot).wait()
                rows = slot_x[pl.ds(pl.multiple_of(e * window, window), window), :]
                g = dot_bt(wg[slot], rows)
                u = dot_bt(wu[slot], rows)
                hidden = (jax.nn.silu(g) * u).astype(BF16)

                @pl.when(e + 2 < local_experts)
                def _():
                    gate_copy(e + 2, slot).start()
                    up_copy(e + 2, slot).start()

                down_copy(e, slot).wait()
                row = pl.multiple_of((e * capacity) // 8 * 8, 8)
                for buf, off in ((ex_send, peer_off), (ex_own, own_off)):
                    value = dot_at(hidden, wd[slot, :, pl.ds(off, half)])
                    for sub in range(SUBS):
                        part = value[:, sub * sub_cols:(sub + 1) * sub_cols]
                        buf[sub, pl.ds(row, 8), :] += part[0:8]
                        buf[sub, pl.ds(row + 8, window - 8), :] = part[8:]

                @pl.when(e + 2 < local_experts)
                def _():
                    down_copy(e + 2, slot).start()

                for i in range(groups):
                    @pl.when(e == last_expert[i])
                    def _():
                        yex_copy(0, i).start()
                        if i < EARLY_GROUPS:
                            yex_copy(1, i).start()

            for i in range(EARLY_GROUPS, groups):
                yex_copy(1, i).start()

    pl.run_scoped(routed_phase, pltpu.VMEM((slots, 2 * tok), BF16), pltpu.VMEM((X_CHUNKS, slots, 2 * x_rows), BF16),
                  pltpu.VMEM((2, ff_expert, d_model), BF16), pltpu.VMEM((2, ff_expert, d_model), BF16),
                  pltpu.VMEM((2, ff_expert, d_model), BF16), pltpu.SemaphoreType.DMA((2,)), pltpu.SemaphoreType.DMA((2,)), pltpu.SemaphoreType.DMA((2,)))

    with jax.named_scope("fin_shared"):
        for copy in xp_copies + fw_copies:
            copy.wait_send()
        res_load.wait()
        for r in range(ROW_BLOCKS):
            @pl.loop(0, n_half)
            def _(j):
                ysh_copy(r, j).wait()
                cols = pl.ds(pl.multiple_of(j * COL, COL), COL)
                rows = slice(r * r_rows, (r + 1) * r_rows)
                sh_own[j, rows, :] = res_half[rows, cols].astype(F32) + (sh_own[j, rows, :] + sh_recv[r, j])

    def ret_copy(sub, i, who, s_sem, r_sem, dev):
        ref = ret.at[sub, who, pl.ds(bounds[i], bounds[i + 1] - bounds[i])]
        return remote(ref, ref, s_sem.at[sub, i], r_sem.at[sub, i], dev)

    def give(sub, i):
        yex_copy(sub, i).wait()
        rows = slice(bounds[i], bounds[i + 1])
        ret[sub, pl.ds(me, 1), rows, :] = (ex_own[sub, rows, :] + ex_recv[sub, rows, :]).astype(BF16).reshape(1, bounds[i + 1] - bounds[i], sub_cols)
        ret_copy(sub, i, me, rx_send, rx_recv, xp_dev).start()
        ret_copy(sub, i, me, rs_send, rs_recv, sib_dev).start()

    def combine(sub, i):
        ret_copy(sub, i, me, rx_send, rx_recv, xp_dev).wait()
        ret_copy(sub, i, xp, rf_send, rf_recv, sib_dev).start()
        ret_copy(sub, i, me, rs_send, rs_recv, sib_dev).wait()
        n = bounds[i + 1] - bounds[i]
        lane = lax.broadcasted_iota(jnp.int32, (tok, ep_size * n), 1)
        owner = sum((lane >= q * n).astype(jnp.int32) for q in range(1, ep_size))
        lane_code = (lane + owner * (pack - n) + bounds[i]).astype(F32)
        pick = (code_col[:, 0:1] == lane_code).astype(F32).astype(BF16)
        ret_copy(sub, i, xp, rf_send, rf_recv, sib_dev).wait()
        rows = ret[sub, :, bounds[i]:bounds[i + 1], :].reshape(ep_size * n, sub_cols)
        gate = gate_col[:, 0:1]
        for j in range(sub_blocks):
            jj = sub * sub_blocks + j
            sh_own[jj] = sh_own[jj] + gate * dot(pick, rows[:, j * COL:(j + 1) * COL])

    def out_copies(sub):
        src = out_half.at[sub]
        dst = o_hbm.at[:, pl.ds(pl.multiple_of(own_off + sub * sub_cols, sub_cols), sub_cols)]
        return remote(src, dst, yo_send.at[sub], yo_recv.at[sub], y_peer), pltpu.make_async_copy(src, dst, lo_sem.at[sub])

    def emit(sub):
        for j in range(sub_blocks):
            out_half[sub, :, j * COL:(j + 1) * COL] = sh_own[sub * sub_blocks + j].astype(BF16)

    def start_out(sub):
        for copy in out_copies(sub):
            copy.start()

    order = [(sub, i) for sub in range(SUBS) for i in range(groups)]
    for n, (sub, i) in enumerate(order):
        with jax.named_scope(f"give{sub}{i}"):
            give(sub, i)
        if n == len(order) - 1:
            start_out(0)
        if n > 0:
            with jax.named_scope(f"comb{n}"):
                combine(*order[n - 1])
                if n == groups:
                    emit(0)
    with jax.named_scope("last"):
        combine(*order[-1])
        emit(1)
        start_out(1)

    with jax.named_scope("out"):
        for sub in range(SUBS):
            for copy in out_copies(sub):
                copy.wait()


def solution(mesh):
    ep_size = mesh.shape["ep"]
    tok_spec = P(("dp", "ep"), None)
    id_spec = P(("dp", "ep"))

    def device_step(normed, residual, w_router, ws_gate, ws_up, ws_down, we_gate, we_up, we_down, first_id, alt_id):
        tok, d_model = normed.shape
        local_experts, _, ff_expert = we_gate.shape
        experts = local_experts * ep_size
        capacity = (5 * tok * ep_size + 4 * experts - 1) // (4 * experts)
        window = -(-(capacity + 7) // 16) * 16
        pack = -(-local_experts * capacity // 16) * 16
        pack_buf = max(pack, (local_experts - 1) * capacity // 8 * 8 + window)
        bounds = [0] + [int(pack * f) // 16 * 16 for f in (0.2, 0.47, 0.74)] + [pack]
        half = d_model // 2
        slots = local_experts * window
        n_half = half // COL
        x_rows = tok // X_CHUNKS
        r_rows = tok // ROW_BLOCKS
        sub_cols = half // SUBS
        dma = pltpu.SemaphoreType.DMA
        any_spec = pl.BlockSpec(memory_space=pl.ANY)
        vmem_spec = pl.BlockSpec(memory_space=pltpu.VMEM)
        per_ret = dma((SUBS, len(bounds) - 1))
        return pl.pallas_call(
            functools.partial(moe_kernel, (experts, capacity, window, pack, bounds, local_experts, ep_size)),
            out_shape=jax.ShapeDtypeStruct((tok, d_model), BF16),
            in_specs=[any_spec] * 9 + [vmem_spec] * 2,
            out_specs=any_spec,
            scratch_shapes=[
                pltpu.VMEM((2, tok, d_model), BF16),
                pltpu.VMEM((X_CHUNKS, 2, x_rows, d_model), BF16),
                pltpu.VMEM((ep_size, 8, tok), jnp.int32),
                pltpu.VMEM((ep_size, 8, tok), F32),
                pltpu.VMEM((tok, LANES), F32),
                pltpu.VMEM((tok, LANES), F32),
                pltpu.VMEM((slots, d_model), BF16),
                pltpu.VMEM((n_half, tok, COL), F32),
                pltpu.VMEM((ROW_BLOCKS, n_half, r_rows, COL), F32),
                pltpu.VMEM((ROW_BLOCKS, n_half, r_rows, COL), F32),
                pltpu.VMEM((SUBS, pack_buf, sub_cols), F32),
                pltpu.VMEM((SUBS, pack_buf, sub_cols), F32),
                pltpu.VMEM((SUBS, pack, sub_cols), F32),
                pltpu.VMEM((SUBS, ep_size, pack, sub_cols), BF16),
                pltpu.VMEM((SUBS, tok, sub_cols), BF16),
                pltpu.VMEM((tok, half), BF16),
                pltpu.VMEM((experts, d_model), F32),
                dma((ROW_BLOCKS + 2,)), dma((3,)), dma((3,)), dma((1,)), dma((1,)), dma((X_CHUNKS,)), dma((X_CHUNKS,)), dma((X_CHUNKS,)), dma((X_CHUNKS,)),
                dma((ROW_BLOCKS, n_half)), dma((ROW_BLOCKS, n_half)), per_ret, per_ret, per_ret, per_ret, per_ret, per_ret, per_ret, per_ret,
                dma((SUBS,)), dma((SUBS,)), dma((SUBS,)),
            ],
            compiler_params=pltpu.CompilerParams(collective_id=0, has_side_effects=True, vmem_limit_bytes=67043328),
        )(normed, residual, w_router.T, ws_gate, ws_up, ws_down, jnp.swapaxes(we_gate, 1, 2), jnp.swapaxes(we_up, 1, 2), we_down,
          first_id.reshape(1, tok), alt_id.reshape(1, tok))

    return jax.shard_map(device_step, mesh=mesh, in_specs=(tok_spec, tok_spec, P(None, None), P(None, 'tp'), P(None, 'tp'), P('tp', None), P('ep', None, 'tp'), P('ep', None, 'tp'), P('ep', 'tp', None), id_spec, id_spec), out_specs=tok_spec, check_vma=False)
```

```python
import functools

import jax
import jax.numpy as jnp
from jax import lax
from jax.experimental import pallas as pl
from jax.experimental.pallas import tpu as pltpu
from jax.sharding import PartitionSpec as P

MESH = pl.DeviceIdType.MESH
F32 = jnp.float32
BF16 = jnp.bfloat16
LANES = 128
RANK_BLOCK = 256
X_CHUNKS = 4
ROW_BLOCKS = 2
COL = 256
SUBS = 2
EARLY_GROUPS = 3
SHARED_BUFS = 4


def dot(a, b):
    return jnp.dot(a, b, preferred_element_type=F32)


def dot_bt(a, b):
    return lax.dot_general(a, b, (((1,), (1,)), ((), ())), preferred_element_type=F32)


def dot_at(a, b):
    return lax.dot_general(a, b, (((0,), (0,)), ((), ())), preferred_element_type=F32)


def moe_kernel(dims, x_hbm, res_hbm, wr_hbm, wsg_hbm, wsu_hbm, wsd_hbm, weg_hbm, weu_hbm, wed_hbm, first_ref, alt_ref, o_hbm,
               x_near, x_far, ids_all, code_rows, code_col, gate_col, slot_x, sh_own, sh_send, sh_recv, ex_own, ex_send, ex_recv, ret, out_half, res_half, wr,
               ld_sem, id_send, id_recv, sib_send, sib_recv, xp_send, xp_recv, fw_send, fw_recv,
               ysh_send, ysh_recv, yex_send, yex_recv, rs_send, rs_recv, rx_send, rx_recv, rf_send, rf_recv, yo_send, yo_recv, lo_sem):
    experts, capacity, window, pack, bounds, local_experts, ep_size = dims
    groups = len(bounds) - 1
    last_expert = [-(-min(b, local_experts * capacity) // capacity) - 1 for b in bounds[1:]]
    tok, d_model = x_hbm.shape
    half = d_model // 2
    slots = local_experts * window
    spare = pack - local_experts * capacity
    ff_shared = wsg_hbm.shape[1]
    ff_expert = weg_hbm.shape[1]
    dp = lax.axis_index("dp")
    t = lax.axis_index("tp")
    me = lax.axis_index("ep")
    core = lax.rem(me, 2)
    sib = me + 1 - 2 * core
    xp = lax.rem(me + 2, ep_size)
    diag = lax.rem(sib + 2, ep_size)
    y_peer = (dp, 1 - t, me)
    sib_dev = (dp, t, sib)
    xp_dev = (dp, t, xp)
    diag_dev = (dp, t, diag)
    own_off = pl.multiple_of(t * half, half)
    peer_off = pl.multiple_of((1 - t) * half, half)
    x_rows = tok // X_CHUNKS
    r_rows = tok // ROW_BLOCKS
    n_hidden = ff_shared // COL
    n_half = half // COL
    sub_cols = half // SUBS
    sub_blocks = sub_cols // COL

    barrier = pltpu.get_barrier_semaphore()
    for dev in (y_peer, sib_dev, xp_dev, diag_dev):
        pl.semaphore_signal(barrier, inc=1, device_id=dev, device_id_type=MESH)

    def remote(src, dst, s_sem, r_sem, dev):
        return pltpu.make_async_remote_copy(src_ref=src, dst_ref=dst, send_sem=s_sem, recv_sem=r_sem, device_id=dev, device_id_type=MESH)

    id_copies = [remote(ids_all.at[me], ids_all.at[me], id_send.at[i], id_recv.at[i], dev) for i, dev in enumerate((sib_dev, xp_dev, diag_dev))]
    xp_copies = [remote(x_hbm.at[pl.ds(c * x_rows, x_rows)], x_far.at[c, 0], xp_send.at[c], xp_recv.at[c], xp_dev) for c in range(X_CHUNKS)]
    sib_copy = remote(x_hbm, x_near.at[1], sib_send.at[0], sib_recv.at[0], sib_dev)
    fw_copies = [remote(x_far.at[c, 0], x_far.at[c, 1], fw_send.at[c], fw_recv.at[c], sib_dev) for c in range(X_CHUNKS)]
    own_x = [pltpu.make_async_copy(x_hbm.at[pl.ds(r * r_rows, r_rows)], x_near.at[0, pl.ds(r * r_rows, r_rows)], ld_sem.at[r]) for r in range(ROW_BLOCKS)]
    res_load = pltpu.make_async_copy(res_hbm.at[:, pl.ds(own_off, half)], res_half, ld_sem.at[ROW_BLOCKS])
    wr_load = pltpu.make_async_copy(wr_hbm, wr, ld_sem.at[ROW_BLOCKS + 1])

    def ysh_copy(r, j):
        return remote(sh_send.at[r, j], sh_recv.at[r, j], ysh_send.at[r, j], ysh_recv.at[r, j], y_peer)

    def shared_phase(act, wg, wu, wd, g_sem, u_sem, d_sem):
        def gate_copy(c, slot):
            return pltpu.make_async_copy(wsg_hbm.at[:, pl.ds(pl.multiple_of(lax.rem(c, n_hidden) * COL, COL), COL)], wg.at[slot], g_sem.at[slot])

        def up_copy(c, slot):
            return pltpu.make_async_copy(wsu_hbm.at[:, pl.ds(pl.multiple_of(lax.rem(c, n_hidden) * COL, COL), COL)], wu.at[slot], u_sem.at[slot])

        def down_copy(k, slot):
            j = lax.rem(k, 2 * n_half)
            col = jnp.where(j < n_half, peer_off + j * COL, own_off + (j - n_half) * COL)
            return pltpu.make_async_copy(wsd_hbm.at[:, pl.ds(pl.multiple_of(col, COL), COL)], wd.at[slot], d_sem.at[slot])

        own_x[0].start()
        gate_copy(jnp.int32(0), 0).start()
        up_copy(jnp.int32(0), 0).start()
        for copy in own_x[1:]:
            copy.start()
        for slot in range(1, SHARED_BUFS):
            gate_copy(jnp.int32(slot), slot).start()
            up_copy(jnp.int32(slot), slot).start()
        for slot in range(SHARED_BUFS):
            down_copy(jnp.int32(slot), slot).start()
        res_load.start()
        wr_load.start()
        ids_all[pl.ds(me, 1), 0:1, :] = first_ref[...].reshape(1, 1, tok)
        ids_all[pl.ds(me, 1), 1:2, :] = alt_ref[...].reshape(1, 1, tok)
        pl.semaphore_wait(barrier, 4)
        for copy in id_copies:
            copy.start()
        for copy in xp_copies:
            copy.start()
        sib_copy.start()

        for r in range(ROW_BLOCKS):
            own_x[r].wait()

            def gateup_step(c):
                k = c + r * n_hidden
                slot = lax.rem(k, SHARED_BUFS)
                gate_copy(k, slot).wait()
                up_copy(k, slot).wait()
                return slot

            def gateup(cs):
                slots_now = [gateup_step(c) for c in cs]
                x = x_near[0, r * r_rows:(r + 1) * r_rows, :]
                for c, slot in zip(cs, slots_now):
                    g = dot(x, wg[slot])
                    u = dot(x, wu[slot])
                    act[:, pl.ds(pl.multiple_of(c * COL, COL), COL)] = (jax.nn.silu(g) * u).astype(BF16)
                for c, slot in zip(cs, slots_now):
                    k = c + r * n_hidden

                    @pl.when(k + SHARED_BUFS < ROW_BLOCKS * n_hidden)
                    def _():
                        gate_copy(k + SHARED_BUFS, slot).start()
                        up_copy(k + SHARED_BUFS, slot).start()

            with jax.named_scope(f"gateup{r}"):
                @pl.loop(0, n_hidden // 2)
                def _(p):
                    gateup([2 * p, 2 * p + 1])

                if n_hidden % 2:
                    gateup([jnp.int32(n_hidden - 1)])

            def down(js, base, store):
                ks = [j + r * 2 * n_half + base for j in js]
                slots_now = [lax.rem(k, SHARED_BUFS) for k in ks]
                for k, slot in zip(ks, slots_now):
                    down_copy(k, slot).wait()
                for j, slot in zip(js, slots_now):
                    store(j, dot(act[...], wd[slot]))
                for k, slot in zip(ks, slots_now):
                    @pl.when(k + SHARED_BUFS < ROW_BLOCKS * 2 * n_half)
                    def _():
                        down_copy(k + SHARED_BUFS, slot).start()

            with jax.named_scope(f"downpeer{r}"):
                @pl.loop(0, n_half)
                def _(j):
                    def store(j, value):
                        sh_send[r, j] = value
                        ysh_copy(r, j).start()

                    down([j], 0, store)

            with jax.named_scope(f"downown{r}"):
                @pl.loop(0, n_half // 2)
                def _(p):
                    def store(j, value):
                        sh_own[j, r * r_rows:(r + 1) * r_rows, :] = value

                    down([2 * p, 2 * p + 1], n_half, store)

    shared_sems = [pltpu.SemaphoreType.DMA((SHARED_BUFS,))] * 3
    pl.run_scoped(shared_phase, pltpu.VMEM((r_rows, ff_shared), BF16), pltpu.VMEM((SHARED_BUFS, d_model, COL), BF16), pltpu.VMEM((SHARED_BUFS, d_model, COL), BF16),
                  pltpu.VMEM((SHARED_BUFS, ff_shared, COL), BF16), *shared_sems)

    def yex_copy(sub, i):
        rows = pl.ds(bounds[i], bounds[i + 1] - bounds[i])
        return remote(ex_send.at[sub, rows], ex_recv.at[sub, rows], yex_send.at[sub, i], yex_recv.at[sub, i], y_peer)

    def ret_copy(sub, i, who, s_sem, r_sem, dev):
        ref = ret.at[sub, who, pl.ds(bounds[i], bounds[i + 1] - bounds[i])]
        return remote(ref, ref, s_sem.at[sub, i], r_sem.at[sub, i], dev)

    def give(sub, i):
        yex_copy(sub, i).wait()
        rows = slice(bounds[i], bounds[i + 1])
        ret[sub, pl.ds(me, 1), rows, :] = (ex_own[sub, rows, :] + ex_recv[sub, rows, :]).astype(BF16).reshape(1, bounds[i + 1] - bounds[i], sub_cols)
        ret_copy(sub, i, me, rx_send, rx_recv, xp_dev).start()
        ret_copy(sub, i, me, rs_send, rs_recv, sib_dev).start()

    def forward(sub, i):
        ret_copy(sub, i, me, rx_send, rx_recv, xp_dev).wait()
        ret_copy(sub, i, xp, rf_send, rf_recv, sib_dev).start()

    def expert_base(ids):
        owner = sum((ids >= q * local_experts).astype(jnp.int32) for q in range(1, ep_size))
        return (ids * capacity + owner * spare).astype(F32)

    def routed_phase(sel_near, sel_far, wg, wu, wd, g_sem, u_sem, d_sem):
        def gate_copy(e, slot):
            return pltpu.make_async_copy(weg_hbm.at[e], wg.at[slot], g_sem.at[slot])

        def up_copy(e, slot):
            return pltpu.make_async_copy(weu_hbm.at[e], wu.at[slot], u_sem.at[slot])

        def down_copy(e, slot):
            return pltpu.make_async_copy(wed_hbm.at[e], wd.at[slot], d_sem.at[slot])

        for slot in range(2):
            gate_copy(slot, slot).start()
            up_copy(slot, slot).start()
            down_copy(slot, slot).start()

        with jax.named_scope("routing"):
            for copy in id_copies:
                copy.wait()
            e_pad = -(-experts // 8) * 8
            e_iota = lax.broadcasted_iota(jnp.int32, (e_pad, RANK_BLOCK), 0)
            row_i = lax.broadcasted_iota(jnp.int32, (RANK_BLOCK, RANK_BLOCK), 0)
            col_i = lax.broadcasted_iota(jnp.int32, (RANK_BLOCK, RANK_BLOCK), 1)
            upper = (row_i <= col_i).astype(F32).astype(BF16)
            blocks = [(q, b * RANK_BLOCK) for q in range(ep_size) for b in range(tok // RANK_BLOCK)]
            cap = jnp.float32(capacity)
            total = jnp.zeros((e_pad, 1), F32)
            rank_first = []
            for q, lo in blocks:
                first = ids_all[q, 0:1, lo:lo + RANK_BLOCK]
                hot = (e_iota == first).astype(F32)
                cum = dot(hot.astype(BF16), upper) + total
                rank_first.append(jnp.sum(cum * hot, axis=0, keepdims=True) - 1.0)
                total = total + jnp.sum(hot, axis=1, keepdims=True)
            load = jnp.minimum(total, cap)
            room = cap - load
            total = jnp.zeros((e_pad, 1), F32)
            for i, (q, lo) in enumerate(blocks):
                first = ids_all[q, 0:1, lo:lo + RANK_BLOCK]
                alt = ids_all[q, 1:2, lo:lo + RANK_BLOCK]
                kept = rank_first[i] < cap
                over = jnp.where(kept, 0.0, 1.0)
                hot = (e_iota == alt).astype(F32) * over
                cum = dot(hot.astype(BF16), upper) + total
                rank_alt = jnp.sum(cum * hot, axis=0, keepdims=True) - 1.0
                total = total + jnp.sum(hot, axis=1, keepdims=True)
                room_tok = jnp.sum(hot * room, axis=0, keepdims=True)
                load_tok = jnp.sum(hot * load, axis=0, keepdims=True)
                code_first = expert_base(first) + rank_first[i]
                code_alt = jnp.where(rank_alt < room_tok, expert_base(alt) + load_tok + rank_alt, -1.0)
                code = jnp.where(kept, code_first, code_alt)
                code_rows[q, :, lo:lo + RANK_BLOCK] = jnp.broadcast_to(code, (8, RANK_BLOCK))

            pos = lax.broadcasted_iota(jnp.int32, (slots, x_rows), 0)
            slot_expert = sum((pos >= e * window).astype(jnp.int32) for e in range(1, local_experts))
            first_row = slot_expert * capacity
            row = (first_row // 8) * 8 + (pos - slot_expert * window)
            slot_code = jnp.where((row >= first_row) & (row < first_row + capacity), row + me * pack, -2).astype(F32)
            for i, q in enumerate((me, sib)):
                codes = code_rows[q]
                for lo in range(0, tok, x_rows):
                    sel_near[:, i * tok + lo:i * tok + lo + x_rows] = (slot_code == codes[0:1, lo:lo + x_rows]).astype(F32).astype(BF16)
            for i, q in enumerate((xp, diag)):
                codes = code_rows[q]
                for c in range(X_CHUNKS):
                    sel_far[c, :, i * x_rows:(i + 1) * x_rows] = (slot_code == codes[0:1, c * x_rows:(c + 1) * x_rows]).astype(F32).astype(BF16)

            code_t = jnp.broadcast_to(code_rows[me][0:1, :], (LANES, tok)).T
            code_col[...] = code_t

        with jax.named_scope("router"):
            wr_load.wait()
            x = x_near[0]
            w = wr[...]
            w_hi = w.astype(BF16)
            w_rest = w - w_hi.astype(F32)
            w_mid = w_rest.astype(BF16)
            w_lo = (w_rest - w_mid.astype(F32)).astype(BF16)
            logits = dot_bt(x, w_hi) + (dot_bt(x, w_mid) + dot_bt(x, w_lo))
            top = jnp.max(logits, axis=1, keepdims=True)
            prob = jnp.exp(logits - top)
            denom = jnp.sum(prob, axis=1, keepdims=True)
            lane_lo = expert_base(lax.broadcasted_iota(jnp.int32, (tok, experts), 1))
            code_e = code_t[:, 0:experts]
            picked = (code_e >= lane_lo) & (code_e < lane_lo + cap)
            gate = jnp.sum(jnp.where(picked, prob, 0.0), axis=1, keepdims=True) / denom
            gate_col[...] = jnp.broadcast_to(gate, (tok, LANES))

        nc = 512
        with jax.named_scope("near"):
            sib_copy.wait()

            @pl.loop(0, d_model // nc)
            def _(n):
                cols = pl.ds(pl.multiple_of(n * nc, nc), nc)
                slot_x[:, cols] = dot(sel_near[...], x_near[:, :, cols].reshape(2 * tok, nc)).astype(BF16)

        with jax.named_scope("far"):
            xp_copies[0].wait_recv()
            fw_copies[0].start()
            for c in range(X_CHUNKS):
                if c + 1 < X_CHUNKS:
                    xp_copies[c + 1].wait_recv()
                    fw_copies[c + 1].start()
                fw_copies[c].wait_recv()

                @pl.loop(0, d_model // nc)
                def _(n):
                    cols = pl.ds(pl.multiple_of(n * nc, nc), nc)
                    rows = x_far[c, :, :, cols].reshape(2 * x_rows, nc)
                    slot_x[:, cols] += dot(sel_far[c], rows).astype(BF16)

        loop_steps = [(5, give, 0, 0), (6, give, 1, 0), (7, give, 0, 1), (8, forward, 0, 0), (8, give, 1, 1), (9, forward, 1, 0), (10, forward, 0, 1), (11, forward, 1, 1), (12, give, 0, 2)]
        with jax.named_scope("experts"):
            for sub in range(SUBS):
                ex_send[sub, 0:8, :] = jnp.zeros((8, sub_cols), F32)
                ex_own[sub, 0:8, :] = jnp.zeros((8, sub_cols), F32)

            @pl.loop(0, local_experts)
            def _(e):
                slot = lax.rem(e, 2)
                gate_copy(e, slot).wait()
                up_copy(e, slot).wait()
                rows = slot_x[pl.ds(pl.multiple_of(e * window, window), window), :]
                g = dot_bt(wg[slot], rows)
                u = dot_bt(wu[slot], rows)
                hidden = (jax.nn.silu(g) * u).astype(BF16)

                @pl.when(e + 2 < local_experts)
                def _():
                    gate_copy(e + 2, slot).start()
                    up_copy(e + 2, slot).start()

                down_copy(e, slot).wait()
                row = pl.multiple_of((e * capacity) // 8 * 8, 8)
                for buf, off in ((ex_send, peer_off), (ex_own, own_off)):
                    value = dot_at(hidden, wd[slot, :, pl.ds(off, half)])
                    for sub in range(SUBS):
                        part = value[:, sub * sub_cols:(sub + 1) * sub_cols]
                        buf[sub, pl.ds(row, 8), :] += part[0:8]
                        buf[sub, pl.ds(row + 8, window - 8), :] = part[8:]

                @pl.when(e + 2 < local_experts)
                def _():
                    down_copy(e + 2, slot).start()

                for i in range(groups):
                    @pl.when(e == last_expert[i])
                    def _():
                        yex_copy(0, i).start()
                        if i < EARLY_GROUPS:
                            yex_copy(1, i).start()

                for when, action, sub, i in loop_steps:
                    @pl.when(e == when)
                    def _():
                        action(sub, i)

            for i in range(EARLY_GROUPS, groups):
                yex_copy(1, i).start()

    pl.run_scoped(routed_phase, pltpu.VMEM((slots, 2 * tok), BF16), pltpu.VMEM((X_CHUNKS, slots, 2 * x_rows), BF16),
                  pltpu.VMEM((2, ff_expert, d_model), BF16), pltpu.VMEM((2, ff_expert, d_model), BF16),
                  pltpu.VMEM((2, ff_expert, d_model), BF16), pltpu.SemaphoreType.DMA((2,)), pltpu.SemaphoreType.DMA((2,)), pltpu.SemaphoreType.DMA((2,)))

    with jax.named_scope("fin_shared"):
        for copy in xp_copies + fw_copies:
            copy.wait_send()
        res_load.wait()
        for r in range(ROW_BLOCKS):
            @pl.loop(0, n_half)
            def _(j):
                ysh_copy(r, j).wait()
                cols = pl.ds(pl.multiple_of(j * COL, COL), COL)
                rows = slice(r * r_rows, (r + 1) * r_rows)
                sh_own[j, rows, :] = res_half[rows, cols].astype(F32) + (sh_own[j, rows, :] + sh_recv[r, j])

    def combine(pick, sub, i):
        n = bounds[i + 1] - bounds[i]
        lanes = slice(ep_size * bounds[i], ep_size * bounds[i + 1])
        if sub == 0:
            lane = lax.broadcasted_iota(jnp.int32, (tok, ep_size * n), 1)
            owner = sum((lane >= q * n).astype(jnp.int32) for q in range(1, ep_size))
            lane_code = (lane + owner * (pack - n) + bounds[i]).astype(F32)
            pick[:, lanes] = (code_col[:, 0:1] == lane_code).astype(F32).astype(BF16)
        ret_copy(sub, i, me, rs_send, rs_recv, sib_dev).wait()
        ret_copy(sub, i, xp, rf_send, rf_recv, sib_dev).wait()
        rows = ret[sub, :, bounds[i]:bounds[i + 1], :].reshape(ep_size * n, sub_cols)
        gate = gate_col[:, 0:1]
        for j in range(sub_blocks):
            jj = sub * sub_blocks + j
            sh_own[jj] = sh_own[jj] + gate * dot(pick[:, lanes], rows[:, j * COL:(j + 1) * COL])

    def out_copies(sub):
        src = out_half.at[sub]
        dst = o_hbm.at[:, pl.ds(pl.multiple_of(own_off + sub * sub_cols, sub_cols), sub_cols)]
        return remote(src, dst, yo_send.at[sub], yo_recv.at[sub], y_peer), pltpu.make_async_copy(src, dst, lo_sem.at[sub])

    def emit(sub):
        for j in range(sub_blocks):
            out_half[sub, :, j * COL:(j + 1) * COL] = sh_own[sub * sub_blocks + j].astype(BF16)

    def start_out(sub):
        for copy in out_copies(sub):
            copy.start()

    def return_phase(pick):
        steps = [(give, 1, 2), (forward, 0, 2), (combine, 0, 0), (combine, 1, 0), (combine, 0, 1), (combine, 1, 1), (give, 0, 3), (forward, 1, 2), (combine, 0, 2),
                 (forward, 0, 3), (combine, 1, 2), (give, 0, 4), (combine, 0, 3), (forward, 0, 4), (combine, 0, 4), (emit, 0), (start_out, 0),
                 (give, 1, 3), (forward, 1, 3), (give, 1, 4), (combine, 1, 3), (forward, 1, 4), (combine, 1, 4), (emit, 1), (start_out, 1)]
        for step in steps:
            with jax.named_scope(step[0].__name__ + "".join(str(a) for a in step[1:])):
                if step[0] is combine:
                    combine(pick, *step[1:])
                else:
                    step[0](*step[1:])

    pl.run_scoped(return_phase, pltpu.VMEM((tok, ep_size * pack), BF16))

    with jax.named_scope("out"):
        for sub in range(SUBS):
            for copy in out_copies(sub):
                copy.wait()


def solution(mesh):
    ep_size = mesh.shape["ep"]
    tok_spec = P(("dp", "ep"), None)
    id_spec = P(("dp", "ep"))

    def device_step(normed, residual, w_router, ws_gate, ws_up, ws_down, we_gate, we_up, we_down, first_id, alt_id):
        tok, d_model = normed.shape
        local_experts, _, ff_expert = we_gate.shape
        experts = local_experts * ep_size
        capacity = (5 * tok * ep_size + 4 * experts - 1) // (4 * experts)
        window = -(-(capacity + 7) // 16) * 16
        pack = -(-local_experts * capacity // 16) * 16
        pack_buf = max(pack, (local_experts - 1) * capacity // 8 * 8 + window)
        bounds = [0] + [int(pack * f) // 32 * 32 for f in (0.13, 0.255, 0.52, 0.76)] + [pack]
        half = d_model // 2
        slots = local_experts * window
        n_half = half // COL
        x_rows = tok // X_CHUNKS
        r_rows = tok // ROW_BLOCKS
        sub_cols = half // SUBS
        dma = pltpu.SemaphoreType.DMA
        any_spec = pl.BlockSpec(memory_space=pl.ANY)
        vmem_spec = pl.BlockSpec(memory_space=pltpu.VMEM)
        per_ret = dma((SUBS, len(bounds) - 1))
        return pl.pallas_call(
            functools.partial(moe_kernel, (experts, capacity, window, pack, bounds, local_experts, ep_size)),
            out_shape=jax.ShapeDtypeStruct((tok, d_model), BF16),
            in_specs=[any_spec] * 9 + [vmem_spec] * 2,
            out_specs=any_spec,
            scratch_shapes=[
                pltpu.VMEM((2, tok, d_model), BF16),
                pltpu.VMEM((X_CHUNKS, 2, x_rows, d_model), BF16),
                pltpu.VMEM((ep_size, 8, tok), jnp.int32),
                pltpu.VMEM((ep_size, 8, tok), F32),
                pltpu.VMEM((tok, LANES), F32),
                pltpu.VMEM((tok, LANES), F32),
                pltpu.VMEM((slots, d_model), BF16),
                pltpu.VMEM((n_half, tok, COL), F32),
                pltpu.VMEM((ROW_BLOCKS, n_half, r_rows, COL), F32),
                pltpu.VMEM((ROW_BLOCKS, n_half, r_rows, COL), F32),
                pltpu.VMEM((SUBS, pack_buf, sub_cols), F32),
                pltpu.VMEM((SUBS, pack_buf, sub_cols), F32),
                pltpu.VMEM((SUBS, pack, sub_cols), F32),
                pltpu.VMEM((SUBS, ep_size, pack, sub_cols), BF16),
                pltpu.VMEM((SUBS, tok, sub_cols), BF16),
                pltpu.VMEM((tok, half), BF16),
                pltpu.VMEM((experts, d_model), F32),
                dma((ROW_BLOCKS + 2,)), dma((3,)), dma((3,)), dma((1,)), dma((1,)), dma((X_CHUNKS,)), dma((X_CHUNKS,)), dma((X_CHUNKS,)), dma((X_CHUNKS,)),
                dma((ROW_BLOCKS, n_half)), dma((ROW_BLOCKS, n_half)), per_ret, per_ret, per_ret, per_ret, per_ret, per_ret, per_ret, per_ret,
                dma((SUBS,)), dma((SUBS,)), dma((SUBS,)),
            ],
            compiler_params=pltpu.CompilerParams(collective_id=0, has_side_effects=True, vmem_limit_bytes=67043328),
        )(normed, residual, w_router.T, ws_gate, ws_up, ws_down, jnp.swapaxes(we_gate, 1, 2), jnp.swapaxes(we_up, 1, 2), we_down,
          first_id.reshape(1, tok), alt_id.reshape(1, tok))

    return jax.shard_map(device_step, mesh=mesh, in_specs=(tok_spec, tok_spec, P(None, None), P(None, 'tp'), P(None, 'tp'), P('tp', None), P('ep', None, 'tp'), P('ep', None, 'tp'), P('ep', 'tp', None), id_spec, id_spec), out_specs=tok_spec, check_vma=False)
```

```python
import functools

import jax
import jax.numpy as jnp
from jax import lax
from jax.experimental import pallas as pl
from jax.experimental.pallas import tpu as pltpu
from jax.sharding import PartitionSpec as P

MESH = pl.DeviceIdType.MESH
F32 = jnp.float32
BF16 = jnp.bfloat16
LANES = 128
RANK_BLOCK = 256
X_SPLIT = (0, 192, 384, 448, 512)
X_CHUNKS = 4
WIDE = 512
ROW_BLOCKS = 2
COL = 256
SUBS = 2
EARLY_GROUPS = 3
SHARED_BUFS = 3


def dot(a, b):
    return jnp.dot(a, b, preferred_element_type=F32)


def dot_bt(a, b):
    return lax.dot_general(a, b, (((1,), (1,)), ((), ())), preferred_element_type=F32)


def dot_at(a, b):
    return lax.dot_general(a, b, (((0,), (0,)), ((), ())), preferred_element_type=F32)


def moe_kernel(dims, x_hbm, res_hbm, wr_hbm, wsg_hbm, wsu_hbm, wsd_hbm, weg_hbm, weu_hbm, wed_hbm, first_ref, alt_ref, o_hbm,
               x_near, x_far, ids_all, code_rows, code_col, gate_col, slot_x, sh_own, sh_send, sh_recv, ex_own, ex_send, ex_recv, ret, out_half, res_half, wr,
               ld_sem, id_send, id_recv, sib_send, sib_recv, xp_send, xp_recv, fw_send, fw_recv,
               ysh_send, ysh_recv, yex_send, yex_recv, rs_send, rs_recv, rx_send, rx_recv, rf_send, rf_recv, yo_send, yo_recv, lo_sem):
    experts, capacity, window, pack, bounds, local_experts, ep_size = dims
    groups = len(bounds) - 1
    last_expert = [-(-min(b, local_experts * capacity) // capacity) - 1 for b in bounds[1:]]
    tok, d_model = x_hbm.shape
    half = d_model // 2
    slots = local_experts * window
    spare = pack - local_experts * capacity
    ff_shared = wsg_hbm.shape[1]
    ff_expert = weg_hbm.shape[1]
    dp = lax.axis_index("dp")
    t = lax.axis_index("tp")
    me = lax.axis_index("ep")
    core = lax.rem(me, 2)
    sib = me + 1 - 2 * core
    xp = lax.rem(me + 2, ep_size)
    diag = lax.rem(sib + 2, ep_size)
    y_peer = (dp, 1 - t, me)
    sib_dev = (dp, t, sib)
    xp_dev = (dp, t, xp)
    diag_dev = (dp, t, diag)
    own_off = pl.multiple_of(t * half, half)
    peer_off = pl.multiple_of((1 - t) * half, half)
    x_cuts = [tok * v // X_SPLIT[-1] for v in X_SPLIT]
    r_rows = tok // ROW_BLOCKS
    n_wide, tail = ff_shared // WIDE, ff_shared % WIDE
    n_chunks = n_wide + (tail > 0)
    n_half = half // WIDE
    sub_cols = half // SUBS
    sub_blocks = sub_cols // WIDE
    sent = -(-local_experts * capacity // 8) * 8

    barrier = pltpu.get_barrier_semaphore()
    for dev in (y_peer, sib_dev, xp_dev, diag_dev):
        pl.semaphore_signal(barrier, inc=1, device_id=dev, device_id_type=MESH)

    def remote(src, dst, s_sem, r_sem, dev):
        return pltpu.make_async_remote_copy(src_ref=src, dst_ref=dst, send_sem=s_sem, recv_sem=r_sem, device_id=dev, device_id_type=MESH)

    id_copies = [remote(ids_all.at[me], ids_all.at[me], id_send.at[i], id_recv.at[i], dev) for i, dev in enumerate((sib_dev, xp_dev, diag_dev))]
    def far_rows(c, i):
        n = x_cuts[c + 1] - x_cuts[c]
        return pl.ds(2 * x_cuts[c] + i * n, n)

    xp_copies = [remote(x_hbm.at[pl.ds(x_cuts[c], x_cuts[c + 1] - x_cuts[c])], x_far.at[far_rows(c, 0)], xp_send.at[c], xp_recv.at[c], xp_dev) for c in range(X_CHUNKS)]
    sib_copy = remote(x_hbm, x_near.at[1], sib_send.at[0], sib_recv.at[0], sib_dev)
    fw_copies = [remote(x_far.at[far_rows(c, 0)], x_far.at[far_rows(c, 1)], fw_send.at[c], fw_recv.at[c], sib_dev) for c in range(X_CHUNKS)]
    own_x = [pltpu.make_async_copy(x_hbm.at[pl.ds(r * r_rows, r_rows)], x_near.at[0, pl.ds(r * r_rows, r_rows)], ld_sem.at[r]) for r in range(ROW_BLOCKS)]
    res_load = pltpu.make_async_copy(res_hbm.at[:, pl.ds(own_off, half)], res_half, ld_sem.at[ROW_BLOCKS])
    wr_load = pltpu.make_async_copy(wr_hbm, wr, ld_sem.at[ROW_BLOCKS + 1])

    def ysh_copy(r, j):
        return remote(sh_send.at[r, j], sh_recv.at[r, j], ysh_send.at[r, j], ysh_recv.at[r, j], y_peer)

    def shared_phase(act, wg, wu, wd, g_sem, u_sem, d_sem):
        def weight_copies(c, slot, width):
            cols = pl.ds(pl.multiple_of(c * WIDE, WIDE), width)
            dst = pl.ds(0, width)
            return (pltpu.make_async_copy(wsg_hbm.at[:, cols], wg.at[slot, :, dst], g_sem.at[slot]),
                    pltpu.make_async_copy(wsu_hbm.at[:, cols], wu.at[slot, :, dst], u_sem.at[slot]))

        def start_weights(k, slot):
            c = lax.rem(k, n_chunks)

            @pl.when(c < n_wide)
            def _():
                for copy in weight_copies(c, slot, WIDE):
                    copy.start()

            if tail:
                @pl.when(c == n_wide)
                def _():
                    for copy in weight_copies(c, slot, tail):
                        copy.start()

        def down_copy(k, slot):
            j = lax.rem(k, 2 * n_half)
            col = jnp.where(j < n_half, peer_off + j * WIDE, own_off + (j - n_half) * WIDE)
            return pltpu.make_async_copy(wsd_hbm.at[:, pl.ds(pl.multiple_of(col, WIDE), WIDE)], wd.at[slot], d_sem.at[slot])

        own_x[0].start()
        start_weights(jnp.int32(0), 0)
        for copy in own_x[1:]:
            copy.start()
        for slot in range(1, SHARED_BUFS):
            start_weights(jnp.int32(slot), slot)
        for slot in range(2):
            down_copy(jnp.int32(slot), slot).start()
        res_load.start()
        wr_load.start()
        ids_all[pl.ds(me, 1), 0:1, :] = first_ref[...].reshape(1, 1, tok)
        ids_all[pl.ds(me, 1), 1:2, :] = alt_ref[...].reshape(1, 1, tok)
        pl.semaphore_wait(barrier, 4)
        for copy in id_copies:
            copy.start()
        for copy in xp_copies:
            copy.start()
        sib_copy.start()

        for r in range(ROW_BLOCKS):
            own_x[r].wait()

            def gateup(c, width):
                k = c + r * n_chunks
                slot = lax.rem(k, SHARED_BUFS)
                for copy in weight_copies(c, slot, width):
                    copy.wait()
                x = x_near[0, r * r_rows:(r + 1) * r_rows, :]
                for lo in range(0, width, COL):
                    g = dot(x, wg[slot, :, lo:lo + COL])
                    u = dot(x, wu[slot, :, lo:lo + COL])
                    act[:, pl.ds(pl.multiple_of(c * WIDE + lo, COL), COL)] = (jax.nn.silu(g) * u).astype(BF16)

                @pl.when(k + SHARED_BUFS < ROW_BLOCKS * n_chunks)
                def _():
                    start_weights(k + SHARED_BUFS, slot)

            with jax.named_scope(f"gateup{r}"):
                @pl.loop(0, n_wide)
                def _(c):
                    gateup(c, WIDE)

                if tail:
                    gateup(jnp.int32(n_wide), tail)

            def down(j, base, store):
                k = j + r * 2 * n_half + base
                slot = lax.rem(k, 2)
                down_copy(k, slot).wait()
                store(dot(act[...], wd[slot]))

                @pl.when(k + 2 < ROW_BLOCKS * 2 * n_half)
                def _():
                    down_copy(k + 2, slot).start()

            with jax.named_scope(f"downpeer{r}"):
                @pl.loop(0, n_half)
                def _(j):
                    def store(value):
                        sh_send[r, j] = value
                        ysh_copy(r, j).start()

                    down(j, 0, store)

            with jax.named_scope(f"downown{r}"):
                @pl.loop(0, n_half)
                def _(j):
                    def store(value):
                        sh_own[j, r * r_rows:(r + 1) * r_rows, :] = value

                    down(j, n_half, store)

    shared_sems = [pltpu.SemaphoreType.DMA((SHARED_BUFS,))] * 3
    pl.run_scoped(shared_phase, pltpu.VMEM((r_rows, ff_shared), BF16), pltpu.VMEM((SHARED_BUFS, d_model, WIDE), BF16), pltpu.VMEM((SHARED_BUFS, d_model, WIDE), BF16),
                  pltpu.VMEM((2, ff_shared, WIDE), BF16), *shared_sems)

    def yex_copy(sub, i):
        rows = pl.ds(bounds[i], min(bounds[i + 1], sent) - bounds[i])
        return remote(ex_send.at[sub, rows], ex_recv.at[sub, rows], yex_send.at[sub, i], yex_recv.at[sub, i], y_peer)

    def ret_copy(sub, i, who, s_sem, r_sem, dev):
        ref = ret.at[sub, who, pl.ds(bounds[i], bounds[i + 1] - bounds[i])]
        return remote(ref, ref, s_sem.at[sub, i], r_sem.at[sub, i], dev)

    def give(sub, i):
        yex_copy(sub, i).wait()
        rows = slice(bounds[i], bounds[i + 1])
        ret[sub, pl.ds(me, 1), rows, :] = (ex_own[sub, rows, :] + ex_recv[sub, rows, :]).astype(BF16).reshape(1, bounds[i + 1] - bounds[i], sub_cols)
        ret_copy(sub, i, me, rx_send, rx_recv, xp_dev).start()
        ret_copy(sub, i, me, rs_send, rs_recv, sib_dev).start()

    def forward(sub, i):
        ret_copy(sub, i, me, rx_send, rx_recv, xp_dev).wait()
        ret_copy(sub, i, xp, rf_send, rf_recv, sib_dev).start()

    def expert_base(ids):
        owner = sum((ids >= q * local_experts).astype(jnp.int32) for q in range(1, ep_size))
        return (ids * capacity + owner * spare).astype(F32)

    def routed_phase(sel_near, sel_far, wg, wu, wd, g_sem, u_sem, d_sem):
        def gate_copy(e, slot):
            return pltpu.make_async_copy(weg_hbm.at[e], wg.at[slot], g_sem.at[slot])

        def up_copy(e, slot):
            return pltpu.make_async_copy(weu_hbm.at[e], wu.at[slot], u_sem.at[slot])

        def down_copy(e, slot):
            return pltpu.make_async_copy(wed_hbm.at[e], wd.at[slot], d_sem.at[slot])

        for slot in range(2):
            gate_copy(slot, slot).start()
            up_copy(slot, slot).start()
            down_copy(slot, slot).start()

        with jax.named_scope("routing"):
            for copy in id_copies:
                copy.wait()
            e_pad = -(-experts // 8) * 8
            e_iota = lax.broadcasted_iota(jnp.int32, (e_pad, RANK_BLOCK), 0)
            row_i = lax.broadcasted_iota(jnp.int32, (RANK_BLOCK, RANK_BLOCK), 0)
            col_i = lax.broadcasted_iota(jnp.int32, (RANK_BLOCK, RANK_BLOCK), 1)
            upper = (row_i <= col_i).astype(F32).astype(BF16)
            blocks = [(q, b * RANK_BLOCK) for q in range(ep_size) for b in range(tok // RANK_BLOCK)]
            cap = jnp.float32(capacity)
            total = jnp.zeros((e_pad, 1), F32)
            rank_first = []
            for q, lo in blocks:
                first = ids_all[q, 0:1, lo:lo + RANK_BLOCK]
                hot = (e_iota == first).astype(F32)
                cum = dot(hot.astype(BF16), upper) + total
                rank_first.append(jnp.sum(cum * hot, axis=0, keepdims=True) - 1.0)
                total = total + jnp.sum(hot, axis=1, keepdims=True)
            load = jnp.minimum(total, cap)
            room = cap - load
            total = jnp.zeros((e_pad, 1), F32)
            for i, (q, lo) in enumerate(blocks):
                first = ids_all[q, 0:1, lo:lo + RANK_BLOCK]
                alt = ids_all[q, 1:2, lo:lo + RANK_BLOCK]
                kept = rank_first[i] < cap
                over = jnp.where(kept, 0.0, 1.0)
                hot = (e_iota == alt).astype(F32) * over
                cum = dot(hot.astype(BF16), upper) + total
                rank_alt = jnp.sum(cum * hot, axis=0, keepdims=True) - 1.0
                total = total + jnp.sum(hot, axis=1, keepdims=True)
                room_tok = jnp.sum(hot * room, axis=0, keepdims=True)
                load_tok = jnp.sum(hot * load, axis=0, keepdims=True)
                code_first = expert_base(first) + rank_first[i]
                code_alt = jnp.where(rank_alt < room_tok, expert_base(alt) + load_tok + rank_alt, -1.0)
                code = jnp.where(kept, code_first, code_alt)
                code_rows[q, :, lo:lo + RANK_BLOCK] = jnp.broadcast_to(code, (8, RANK_BLOCK))

            pos = lax.broadcasted_iota(jnp.int32, (slots, LANES), 0)
            slot_expert = sum((pos >= e * window).astype(jnp.int32) for e in range(1, local_experts))
            first_row = slot_expert * capacity
            row = (first_row // 8) * 8 + (pos - slot_expert * window)
            slot_code = jnp.where((row >= first_row) & (row < first_row + capacity), row + me * pack, -2).astype(F32)
            def pick_rows(codes):
                return (jnp.broadcast_to(slot_code[:, 0:1], (slots, codes.shape[1])) == codes).astype(F32).astype(BF16)

            for i, q in enumerate((me, sib)):
                codes = code_rows[q]
                for lo in range(0, tok, LANES):
                    sel_near[:, i * tok + lo:i * tok + lo + LANES] = pick_rows(codes[0:1, lo:lo + LANES])
            codes_xp, codes_diag = code_rows[xp][0:1, :], code_rows[diag][0:1, :]
            for c in range(X_CHUNKS):
                both = jnp.concatenate([codes_xp[:, x_cuts[c]:x_cuts[c + 1]], codes_diag[:, x_cuts[c]:x_cuts[c + 1]]], axis=1)
                for lo in range(0, 2 * (x_cuts[c + 1] - x_cuts[c]), LANES):
                    dst = 2 * x_cuts[c] + lo
                    sel_far[:, dst:dst + LANES] = pick_rows(both[:, lo:lo + LANES])

            code_t = jnp.broadcast_to(code_rows[me][0:1, :], (LANES, tok)).T
            code_col[...] = code_t

        with jax.named_scope("router"):
            wr_load.wait()
            x = x_near[0]
            w = wr[...]
            w_hi = w.astype(BF16)
            w_rest = w - w_hi.astype(F32)
            w_mid = w_rest.astype(BF16)
            w_lo = (w_rest - w_mid.astype(F32)).astype(BF16)
            logits = dot_bt(x, w_hi) + (dot_bt(x, w_mid) + dot_bt(x, w_lo))
            top = jnp.max(logits, axis=1, keepdims=True)
            prob = jnp.exp(logits - top)
            denom = jnp.sum(prob, axis=1, keepdims=True)
            lane_lo = expert_base(lax.broadcasted_iota(jnp.int32, (tok, experts), 1))
            code_e = code_t[:, 0:experts]
            picked = (code_e >= lane_lo) & (code_e < lane_lo + cap)
            gate = jnp.sum(jnp.where(picked, prob, 0.0), axis=1, keepdims=True) / denom
            gate_col[...] = jnp.broadcast_to(gate, (tok, LANES))

        nc = 512
        with jax.named_scope("near"):
            sib_copy.wait()

            @pl.loop(0, d_model // nc)
            def _(n):
                cols = pl.ds(pl.multiple_of(n * nc, nc), nc)
                slot_x[:, cols] = dot(sel_near[...], x_near[:, :, cols].reshape(2 * tok, nc)).astype(BF16)

        with jax.named_scope("far"):
            xp_copies[0].wait_recv()
            fw_copies[0].start()
            for c in range(X_CHUNKS):
                if c + 1 < X_CHUNKS:
                    xp_copies[c + 1].wait_recv()
                    fw_copies[c + 1].start()
                fw_copies[c].wait_recv()

                @pl.loop(0, d_model // nc)
                def _(n):
                    cols = pl.ds(pl.multiple_of(n * nc, nc), nc)
                    span = slice(2 * x_cuts[c], 2 * x_cuts[c + 1])
                    slot_x[:, cols] += dot(sel_far[:, span], x_far[span, cols]).astype(BF16)

        loop_steps = [(5, give, 0, 0), (6, give, 1, 0), (7, give, 0, 1), (8, forward, 0, 0), (8, give, 1, 1), (9, forward, 1, 0), (10, forward, 0, 1), (11, forward, 1, 1), (12, give, 0, 2)]
        if sent < pack:
            for sub in range(SUBS):
                ex_recv[sub, sent:pack, :] = jnp.zeros((pack - sent, sub_cols), F32)

        with jax.named_scope("experts"):
            for sub in range(SUBS):
                ex_send[sub, 0:8, :] = jnp.zeros((8, sub_cols), F32)
                ex_own[sub, 0:8, :] = jnp.zeros((8, sub_cols), F32)

            @pl.loop(0, local_experts)
            def _(e):
                slot = lax.rem(e, 2)
                gate_copy(e, slot).wait()
                up_copy(e, slot).wait()
                rows = slot_x[pl.ds(pl.multiple_of(e * window, window), window), :]
                g = dot_bt(wg[slot], rows)
                u = dot_bt(wu[slot], rows)
                hidden = (jax.nn.silu(g) * u).astype(BF16)

                @pl.when(e + 2 < local_experts)
                def _():
                    gate_copy(e + 2, slot).start()
                    up_copy(e + 2, slot).start()

                down_copy(e, slot).wait()
                row = pl.multiple_of((e * capacity) // 8 * 8, 8)
                for buf, off in ((ex_send, peer_off), (ex_own, own_off)):
                    value = dot_at(hidden, wd[slot, :, pl.ds(off, half)])
                    for sub in range(SUBS):
                        part = value[:, sub * sub_cols:(sub + 1) * sub_cols]
                        buf[sub, pl.ds(row, 8), :] += part[0:8]
                        buf[sub, pl.ds(row + 8, window - 8), :] = part[8:]

                @pl.when(e + 2 < local_experts)
                def _():
                    down_copy(e + 2, slot).start()

                for i in range(groups):
                    @pl.when(e == last_expert[i])
                    def _():
                        yex_copy(0, i).start()
                        if i < EARLY_GROUPS:
                            yex_copy(1, i).start()

                for when, action, sub, i in loop_steps:
                    @pl.when(e == when)
                    def _():
                        action(sub, i)

            for i in range(EARLY_GROUPS, groups):
                yex_copy(1, i).start()

    pl.run_scoped(routed_phase, pltpu.VMEM((slots, 2 * tok), BF16), pltpu.VMEM((slots, 2 * tok), BF16),
                  pltpu.VMEM((2, ff_expert, d_model), BF16), pltpu.VMEM((2, ff_expert, d_model), BF16),
                  pltpu.VMEM((2, ff_expert, d_model), BF16), pltpu.SemaphoreType.DMA((2,)), pltpu.SemaphoreType.DMA((2,)), pltpu.SemaphoreType.DMA((2,)))

    with jax.named_scope("fin_shared"):
        for copy in xp_copies + fw_copies:
            copy.wait_send()
        res_load.wait()
        for r in range(ROW_BLOCKS):
            @pl.loop(0, n_half)
            def _(j):
                ysh_copy(r, j).wait()
                cols = pl.ds(pl.multiple_of(j * WIDE, WIDE), WIDE)
                rows = slice(r * r_rows, (r + 1) * r_rows)
                sh_own[j, rows, :] = res_half[rows, cols].astype(F32) + (sh_own[j, rows, :] + sh_recv[r, j])

    def combine(pick, sub, i):
        n = bounds[i + 1] - bounds[i]
        lanes = slice(ep_size * bounds[i], ep_size * bounds[i + 1])
        if sub == 0:
            lane = lax.broadcasted_iota(jnp.int32, (tok, ep_size * n), 1)
            owner = sum((lane >= q * n).astype(jnp.int32) for q in range(1, ep_size))
            lane_code = (lane + owner * (pack - n) + bounds[i]).astype(F32)
            pick[:, lanes] = (code_col[:, 0:1] == lane_code).astype(F32).astype(BF16)
        ret_copy(sub, i, me, rs_send, rs_recv, sib_dev).wait()
        ret_copy(sub, i, xp, rf_send, rf_recv, sib_dev).wait()
        rows = ret[sub, :, bounds[i]:bounds[i + 1], :].reshape(ep_size * n, sub_cols)
        gate = gate_col[:, 0:1]
        for j in range(sub_blocks):
            jj = sub * sub_blocks + j
            sh_own[jj] = sh_own[jj] + gate * dot(pick[:, lanes], rows[:, j * WIDE:(j + 1) * WIDE])

    def out_copies(sub):
        src = out_half.at[sub]
        dst = o_hbm.at[:, pl.ds(pl.multiple_of(own_off + sub * sub_cols, sub_cols), sub_cols)]
        return remote(src, dst, yo_send.at[sub], yo_recv.at[sub], y_peer), pltpu.make_async_copy(src, dst, lo_sem.at[sub])

    def emit(sub):
        for j in range(sub_blocks):
            out_half[sub, :, j * WIDE:(j + 1) * WIDE] = sh_own[sub * sub_blocks + j].astype(BF16)

    def start_out(sub):
        for copy in out_copies(sub):
            copy.start()

    def return_phase(pick):
        steps = [(give, 1, 2), (forward, 0, 2), (combine, 0, 0), (combine, 1, 0), (combine, 0, 1), (combine, 1, 1), (give, 0, 3), (forward, 1, 2), (combine, 0, 2),
                 (forward, 0, 3), (combine, 1, 2), (give, 0, 4), (combine, 0, 3), (forward, 0, 4), (combine, 0, 4), (emit, 0), (start_out, 0),
                 (give, 1, 3), (forward, 1, 3), (give, 1, 4), (combine, 1, 3), (forward, 1, 4), (combine, 1, 4), (emit, 1), (start_out, 1)]
        for step in steps:
            with jax.named_scope(step[0].__name__ + "".join(str(a) for a in step[1:])):
                if step[0] is combine:
                    combine(pick, *step[1:])
                else:
                    step[0](*step[1:])

    pl.run_scoped(return_phase, pltpu.VMEM((tok, ep_size * pack), BF16))

    with jax.named_scope("out"):
        for sub in range(SUBS):
            for copy in out_copies(sub):
                copy.wait()


def solution(mesh):
    ep_size = mesh.shape["ep"]
    tok_spec = P(("dp", "ep"), None)
    id_spec = P(("dp", "ep"))

    def device_step(normed, residual, w_router, ws_gate, ws_up, ws_down, we_gate, we_up, we_down, first_id, alt_id):
        tok, d_model = normed.shape
        local_experts, _, ff_expert = we_gate.shape
        experts = local_experts * ep_size
        capacity = (5 * tok * ep_size + 4 * experts - 1) // (4 * experts)
        window = -(-(capacity + 7) // 16) * 16
        pack = -(-local_experts * capacity // 16) * 16
        pack_buf = max(pack, (local_experts - 1) * capacity // 8 * 8 + window)
        bounds = [0] + [int(pack * f) // 32 * 32 for f in (0.13, 0.255, 0.52, 0.76)] + [pack]
        half = d_model // 2
        slots = local_experts * window
        n_half = half // WIDE
        r_rows = tok // ROW_BLOCKS
        sub_cols = half // SUBS
        dma = pltpu.SemaphoreType.DMA
        any_spec = pl.BlockSpec(memory_space=pl.ANY)
        vmem_spec = pl.BlockSpec(memory_space=pltpu.VMEM)
        per_ret = dma((SUBS, len(bounds) - 1))
        return pl.pallas_call(
            functools.partial(moe_kernel, (experts, capacity, window, pack, bounds, local_experts, ep_size)),
            out_shape=jax.ShapeDtypeStruct((tok, d_model), BF16),
            in_specs=[any_spec] * 9 + [vmem_spec] * 2,
            out_specs=any_spec,
            scratch_shapes=[
                pltpu.VMEM((2, tok, d_model), BF16),
                pltpu.VMEM((2 * tok, d_model), BF16),
                pltpu.VMEM((ep_size, 8, tok), jnp.int32),
                pltpu.VMEM((ep_size, 8, tok), F32),
                pltpu.VMEM((tok, LANES), F32),
                pltpu.VMEM((tok, LANES), F32),
                pltpu.VMEM((slots, d_model), BF16),
                pltpu.VMEM((n_half, tok, WIDE), F32),
                pltpu.VMEM((ROW_BLOCKS, n_half, r_rows, WIDE), F32),
                pltpu.VMEM((ROW_BLOCKS, n_half, r_rows, WIDE), F32),
                pltpu.VMEM((SUBS, pack_buf, sub_cols), F32),
                pltpu.VMEM((SUBS, pack_buf, sub_cols), F32),
                pltpu.VMEM((SUBS, pack, sub_cols), F32),
                pltpu.VMEM((SUBS, ep_size, pack, sub_cols), BF16),
                pltpu.VMEM((SUBS, tok, sub_cols), BF16),
                pltpu.VMEM((tok, half), BF16),
                pltpu.VMEM((experts, d_model), F32),
                dma((ROW_BLOCKS + 2,)), dma((3,)), dma((3,)), dma((1,)), dma((1,)), dma((X_CHUNKS,)), dma((X_CHUNKS,)), dma((X_CHUNKS,)), dma((X_CHUNKS,)),
                dma((ROW_BLOCKS, n_half)), dma((ROW_BLOCKS, n_half)), per_ret, per_ret, per_ret, per_ret, per_ret, per_ret, per_ret, per_ret,
                dma((SUBS,)), dma((SUBS,)), dma((SUBS,)),
            ],
            compiler_params=pltpu.CompilerParams(collective_id=0, has_side_effects=True, vmem_limit_bytes=67043328),
        )(normed, residual, w_router.T, ws_gate, ws_up, ws_down, jnp.swapaxes(we_gate, 1, 2), jnp.swapaxes(we_up, 1, 2), we_down,
          first_id.reshape(1, tok), alt_id.reshape(1, tok))

    return jax.shard_map(device_step, mesh=mesh, in_specs=(tok_spec, tok_spec, P(None, None), P(None, 'tp'), P(None, 'tp'), P('tp', None), P('ep', None, 'tp'), P('ep', None, 'tp'), P('ep', 'tp', None), id_spec, id_spec), out_specs=tok_spec, check_vma=False)
```

```python
import functools

import jax
import jax.numpy as jnp
from jax import lax
from jax.experimental import pallas as pl
from jax.experimental.pallas import tpu as pltpu
from jax.sharding import PartitionSpec as P

MESH = pl.DeviceIdType.MESH
F32 = jnp.float32
BF16 = jnp.bfloat16
LANES = 128
RANK_BLOCK = 256
X_SPLIT = (0, 192, 384, 448, 512)
X_CHUNKS = 4
WIDE = 512
COPY_CHUNKS = 4
ROW_BLOCKS = 2
COL = 256
SUBS = 2
EARLY_GROUPS = 3
SHARED_BUFS = 3


def dot(a, b):
    return jnp.dot(a, b, preferred_element_type=F32)


def dot_bt(a, b):
    return lax.dot_general(a, b, (((1,), (1,)), ((), ())), preferred_element_type=F32)


def dot_at(a, b):
    return lax.dot_general(a, b, (((0,), (0,)), ((), ())), preferred_element_type=F32)


def moe_kernel(dims, x_hbm, res_hbm, wr_hbm, wsg_hbm, wsu_hbm, wsd_hbm, weg_hbm, weu_hbm, wed_hbm, first_ref, alt_ref, o_hbm,
               x_near, x_far, ids_all, code_rows, code_col, gate_col, slot_x, sh_own, sh_send, sh_recv, ex_own, ex_send, ex_recv, ret, out_half, res_half, wr,
               ld_sem, id_send, id_recv, sib_send, sib_recv, xp_send, xp_recv, fw_send, fw_recv,
               ysh_send, ysh_recv, yex_send, yex_recv, rs_send, rs_recv, rx_send, rx_recv, rf_send, rf_recv, yo_send, yo_recv, lo_sem):
    experts, capacity, window, pack, bounds, local_experts, ep_size = dims
    groups = len(bounds) - 1
    last_expert = [-(-min(b, local_experts * capacity) // capacity) - 1 for b in bounds[1:]]
    tok, d_model = x_hbm.shape
    half = d_model // 2
    slots = local_experts * window
    spare = pack - local_experts * capacity
    ff_shared = wsg_hbm.shape[1]
    ff_expert = weg_hbm.shape[1]
    dp = lax.axis_index("dp")
    t = lax.axis_index("tp")
    me = lax.axis_index("ep")
    core = lax.rem(me, 2)
    sib = me + 1 - 2 * core
    xp = lax.rem(me + 2, ep_size)
    diag = lax.rem(sib + 2, ep_size)
    y_peer = (dp, 1 - t, me)
    sib_dev = (dp, t, sib)
    xp_dev = (dp, t, xp)
    diag_dev = (dp, t, diag)
    own_off = pl.multiple_of(t * half, half)
    peer_off = pl.multiple_of((1 - t) * half, half)
    x_cuts = [tok * v // X_SPLIT[-1] for v in X_SPLIT]
    r_rows = tok // ROW_BLOCKS
    n_wide, tail = ff_shared // WIDE, ff_shared % WIDE
    n_chunks = n_wide + (tail > 0)
    n_half = half // WIDE
    sub_cols = half // SUBS
    sub_blocks = sub_cols // WIDE
    sent = -(-local_experts * capacity // 8) * 8

    barrier = pltpu.get_barrier_semaphore()
    for dev in (y_peer, sib_dev, xp_dev, diag_dev):
        pl.semaphore_signal(barrier, inc=1, device_id=dev, device_id_type=MESH)

    def remote(src, dst, s_sem, r_sem, dev):
        return pltpu.make_async_remote_copy(src_ref=src, dst_ref=dst, send_sem=s_sem, recv_sem=r_sem, device_id=dev, device_id_type=MESH)

    id_copies = [remote(ids_all.at[me], ids_all.at[me], id_send.at[i], id_recv.at[i], dev) for i, dev in enumerate((sib_dev, xp_dev, diag_dev))]
    def far_rows(c, i):
        n = x_cuts[c + 1] - x_cuts[c]
        return pl.ds(2 * x_cuts[c] + i * n, n)

    xp_copies = [remote(x_near.at[0, pl.ds(x_cuts[c], x_cuts[c + 1] - x_cuts[c])], x_far.at[far_rows(c, 0)], xp_send.at[c], xp_recv.at[c], xp_dev) for c in range(X_CHUNKS)]
    sib_copy = remote(x_near.at[0], x_near.at[1], sib_send.at[0], sib_recv.at[0], sib_dev)
    fw_copies = [remote(x_far.at[far_rows(c, 0)], x_far.at[far_rows(c, 1)], fw_send.at[c], fw_recv.at[c], sib_dev) for c in range(X_CHUNKS)]
    own_x = [pltpu.make_async_copy(x_hbm.at[pl.ds(r * r_rows, r_rows)], x_near.at[0, pl.ds(r * r_rows, r_rows)], ld_sem.at[r]) for r in range(ROW_BLOCKS)]
    res_load = pltpu.make_async_copy(res_hbm.at[:, pl.ds(own_off, half)], res_half, ld_sem.at[ROW_BLOCKS])
    wr_load = pltpu.make_async_copy(wr_hbm, wr, ld_sem.at[ROW_BLOCKS + 1])

    def ysh_copy(r, j):
        return remote(sh_send.at[r, j], sh_recv.at[r, j], ysh_send.at[r, j], ysh_recv.at[r, j], y_peer)

    def shared_phase(act, wg, wu, wd, g_sem, u_sem, d_sem):
        def weight_copies(c, slot, width):
            cols = pl.ds(pl.multiple_of(c * WIDE, WIDE), width)
            dst = pl.ds(0, width)
            return (pltpu.make_async_copy(wsg_hbm.at[:, cols], wg.at[slot, :, dst], g_sem.at[slot]),
                    pltpu.make_async_copy(wsu_hbm.at[:, cols], wu.at[slot, :, dst], u_sem.at[slot]))

        def start_weights(k, slot):
            c = lax.rem(k, n_chunks)

            @pl.when(c < n_wide)
            def _():
                for copy in weight_copies(c, slot, WIDE):
                    copy.start()

            if tail:
                @pl.when(c == n_wide)
                def _():
                    for copy in weight_copies(c, slot, tail):
                        copy.start()

        def down_copy(k, slot):
            j = lax.rem(k, 2 * n_half)
            col = jnp.where(j < n_half, peer_off + j * WIDE, own_off + (j - n_half) * WIDE)
            return pltpu.make_async_copy(wsd_hbm.at[:, pl.ds(pl.multiple_of(col, WIDE), WIDE)], wd.at[slot], d_sem.at[slot])

        own_x[0].start()
        start_weights(jnp.int32(0), 0)
        for copy in own_x[1:]:
            copy.start()
        for slot in range(1, SHARED_BUFS):
            start_weights(jnp.int32(slot), slot)
        ids_all[pl.ds(me, 1), 0:1, :] = first_ref[...].reshape(1, 1, tok)
        ids_all[pl.ds(me, 1), 1:2, :] = alt_ref[...].reshape(1, 1, tok)
        pl.semaphore_wait(barrier, 4)
        for copy in id_copies:
            copy.start()
        for copy in own_x:
            copy.wait()
        for copy in xp_copies:
            copy.start()
        sib_copy.start()

        for r in range(ROW_BLOCKS):
            def gateup(c, width):
                k = c + r * n_chunks
                slot = lax.rem(k, SHARED_BUFS)
                for copy in weight_copies(c, slot, width):
                    copy.wait()
                x = x_near[0, r * r_rows:(r + 1) * r_rows, :]
                for lo in range(0, width, COL):
                    g = dot(x, wg[slot, :, lo:lo + COL])
                    u = dot(x, wu[slot, :, lo:lo + COL])
                    act[:, pl.ds(pl.multiple_of(c * WIDE + lo, COL), COL)] = (jax.nn.silu(g) * u).astype(BF16)

                @pl.when(k + SHARED_BUFS < ROW_BLOCKS * n_chunks)
                def _():
                    start_weights(k + SHARED_BUFS, slot)

            with jax.named_scope(f"gateup{r}"):
                @pl.loop(0, n_wide)
                def _(c):
                    gateup(c, WIDE)

                    if r == 0:
                        @pl.when((c == 1) | (c == 3))
                        def _():
                            slot = lax.div(c, 2)
                            down_copy(slot, slot).start()

                if tail:
                    gateup(jnp.int32(n_wide), tail)

            def down(j, base, store):
                k = j + r * 2 * n_half + base
                slot = lax.rem(k, 2)
                down_copy(k, slot).wait()
                store(dot(act[...], wd[slot]))

                @pl.when(k + 2 < ROW_BLOCKS * 2 * n_half)
                def _():
                    down_copy(k + 2, slot).start()

            with jax.named_scope(f"downpeer{r}"):
                @pl.loop(0, n_half)
                def _(j):
                    def store(value):
                        sh_send[r, j] = value
                        ysh_copy(r, j).start()

                    down(j, 0, store)

            if r == 0:
                wr_load.start()
            with jax.named_scope(f"downown{r}"):
                @pl.loop(0, n_half)
                def _(j):
                    def store(value):
                        sh_own[j, r * r_rows:(r + 1) * r_rows, :] = value

                    down(j, n_half, store)

    shared_sems = [pltpu.SemaphoreType.DMA((SHARED_BUFS,))] * 3
    pl.run_scoped(shared_phase, pltpu.VMEM((r_rows, ff_shared), BF16), pltpu.VMEM((SHARED_BUFS, d_model, WIDE), BF16), pltpu.VMEM((SHARED_BUFS, d_model, WIDE), BF16),
                  pltpu.VMEM((2, ff_shared, WIDE), BF16), *shared_sems)

    def yex_copy(sub, i):
        rows = pl.ds(bounds[i], min(bounds[i + 1], sent) - bounds[i])
        return remote(ex_send.at[sub, rows], ex_recv.at[sub, rows], yex_send.at[sub, i], yex_recv.at[sub, i], y_peer)

    def ret_copy(sub, i, who, s_sem, r_sem, dev):
        ref = ret.at[sub, who, pl.ds(bounds[i], bounds[i + 1] - bounds[i])]
        return remote(ref, ref, s_sem.at[sub, i], r_sem.at[sub, i], dev)

    def give(sub, i):
        yex_copy(sub, i).wait()
        rows = slice(bounds[i], bounds[i + 1])
        ret[sub, pl.ds(me, 1), rows, :] = (ex_own[sub, rows, :] + ex_recv[sub, rows, :]).astype(BF16).reshape(1, bounds[i + 1] - bounds[i], sub_cols)
        ret_copy(sub, i, me, rx_send, rx_recv, xp_dev).start()
        ret_copy(sub, i, me, rs_send, rs_recv, sib_dev).start()

    def forward(sub, i):
        ret_copy(sub, i, me, rx_send, rx_recv, xp_dev).wait()
        ret_copy(sub, i, xp, rf_send, rf_recv, sib_dev).start()

    def expert_base(ids):
        owner = sum((ids >= q * local_experts).astype(jnp.int32) for q in range(1, ep_size))
        return (ids * capacity + owner * spare).astype(F32)

    def routed_phase(sel_near, sel_far, wg, wu, wd, g_sem, u_sem, d_sem):
        def gate_copy(e, slot):
            return pltpu.make_async_copy(weg_hbm.at[e], wg.at[slot], g_sem.at[slot])

        def up_copy(e, slot):
            return pltpu.make_async_copy(weu_hbm.at[e], wu.at[slot], u_sem.at[slot])

        def down_copy(e, slot):
            return pltpu.make_async_copy(wed_hbm.at[e], wd.at[slot], d_sem.at[slot])

        for slot in range(2):
            gate_copy(slot, slot).start()
            up_copy(slot, slot).start()
            down_copy(slot, slot).start()

        res_load.start()
        with jax.named_scope("routing"):
            for copy in id_copies:
                copy.wait()
            e_pad = -(-experts // 8) * 8
            e_iota = lax.broadcasted_iota(jnp.int32, (e_pad, RANK_BLOCK), 0)
            row_i = lax.broadcasted_iota(jnp.int32, (RANK_BLOCK, RANK_BLOCK), 0)
            col_i = lax.broadcasted_iota(jnp.int32, (RANK_BLOCK, RANK_BLOCK), 1)
            upper = (row_i <= col_i).astype(F32).astype(BF16)
            blocks = [(q, b * RANK_BLOCK) for q in range(ep_size) for b in range(tok // RANK_BLOCK)]
            cap = jnp.float32(capacity)
            total = jnp.zeros((e_pad, 1), F32)
            rank_first = []
            for q, lo in blocks:
                first = ids_all[q, 0:1, lo:lo + RANK_BLOCK]
                hot = (e_iota == first).astype(F32)
                cum = dot(hot.astype(BF16), upper) + total
                rank_first.append(jnp.sum(cum * hot, axis=0, keepdims=True) - 1.0)
                total = total + jnp.sum(hot, axis=1, keepdims=True)
            load = jnp.minimum(total, cap)
            room = cap - load
            total = jnp.zeros((e_pad, 1), F32)
            for i, (q, lo) in enumerate(blocks):
                first = ids_all[q, 0:1, lo:lo + RANK_BLOCK]
                alt = ids_all[q, 1:2, lo:lo + RANK_BLOCK]
                kept = rank_first[i] < cap
                over = jnp.where(kept, 0.0, 1.0)
                hot = (e_iota == alt).astype(F32) * over
                cum = dot(hot.astype(BF16), upper) + total
                rank_alt = jnp.sum(cum * hot, axis=0, keepdims=True) - 1.0
                total = total + jnp.sum(hot, axis=1, keepdims=True)
                room_tok = jnp.sum(hot * room, axis=0, keepdims=True)
                load_tok = jnp.sum(hot * load, axis=0, keepdims=True)
                code_first = expert_base(first) + rank_first[i]
                code_alt = jnp.where(rank_alt < room_tok, expert_base(alt) + load_tok + rank_alt, -1.0)
                code = jnp.where(kept, code_first, code_alt)
                code_rows[q, :, lo:lo + RANK_BLOCK] = jnp.broadcast_to(code, (8, RANK_BLOCK))

            pos = lax.broadcasted_iota(jnp.int32, (slots, LANES), 0)
            slot_expert = sum((pos >= e * window).astype(jnp.int32) for e in range(1, local_experts))
            first_row = slot_expert * capacity
            row = (first_row // 8) * 8 + (pos - slot_expert * window)
            slot_code = jnp.where((row >= first_row) & (row < first_row + capacity), row + me * pack, -2).astype(F32)
            def pick_rows(codes):
                return (jnp.broadcast_to(slot_code[:, 0:1], (slots, codes.shape[1])) == codes).astype(F32).astype(BF16)

            for i, q in enumerate((me, sib)):
                codes = code_rows[q]
                for lo in range(0, tok, LANES):
                    sel_near[:, i * tok + lo:i * tok + lo + LANES] = pick_rows(codes[0:1, lo:lo + LANES])
            codes_xp, codes_diag = code_rows[xp][0:1, :], code_rows[diag][0:1, :]
            for c in range(X_CHUNKS):
                both = jnp.concatenate([codes_xp[:, x_cuts[c]:x_cuts[c + 1]], codes_diag[:, x_cuts[c]:x_cuts[c + 1]]], axis=1)
                for lo in range(0, 2 * (x_cuts[c + 1] - x_cuts[c]), LANES):
                    dst = 2 * x_cuts[c] + lo
                    sel_far[:, dst:dst + LANES] = pick_rows(both[:, lo:lo + LANES])

            code_t = jnp.broadcast_to(code_rows[me][0:1, :], (LANES, tok)).T
            code_col[...] = code_t

        with jax.named_scope("router"):
            wr_load.wait()
            x = x_near[0]
            w = wr[...]
            w_hi = w.astype(BF16)
            w_rest = w - w_hi.astype(F32)
            w_mid = w_rest.astype(BF16)
            w_lo = (w_rest - w_mid.astype(F32)).astype(BF16)
            logits = dot_bt(x, w_hi) + (dot_bt(x, w_mid) + dot_bt(x, w_lo))
            top = jnp.max(logits, axis=1, keepdims=True)
            prob = jnp.exp(logits - top)
            denom = jnp.sum(prob, axis=1, keepdims=True)
            lane_lo = expert_base(lax.broadcasted_iota(jnp.int32, (tok, experts), 1))
            code_e = code_t[:, 0:experts]
            picked = (code_e >= lane_lo) & (code_e < lane_lo + cap)
            gate = jnp.sum(jnp.where(picked, prob, 0.0), axis=1, keepdims=True) / denom
            gate_col[...] = jnp.broadcast_to(gate, (tok, LANES))

        nc = 512
        with jax.named_scope("near"):
            sib_copy.wait()

            @pl.loop(0, d_model // nc)
            def _(n):
                cols = pl.ds(pl.multiple_of(n * nc, nc), nc)
                slot_x[:, cols] = dot(sel_near[...], x_near[:, :, cols].reshape(2 * tok, nc)).astype(BF16)

        with jax.named_scope("far"):
            xp_copies[0].wait_recv()
            fw_copies[0].start()
            for c in range(X_CHUNKS):
                if c + 1 < X_CHUNKS:
                    xp_copies[c + 1].wait_recv()
                    fw_copies[c + 1].start()
                fw_copies[c].wait_recv()

                @pl.loop(0, d_model // nc)
                def _(n):
                    cols = pl.ds(pl.multiple_of(n * nc, nc), nc)
                    span = slice(2 * x_cuts[c], 2 * x_cuts[c + 1])
                    slot_x[:, cols] += dot(sel_far[:, span], x_far[span, cols]).astype(BF16)

        loop_steps = [(5, give, 0, 0), (6, give, 1, 0), (7, give, 0, 1), (8, forward, 0, 0), (8, give, 1, 1), (9, forward, 1, 0), (10, forward, 0, 1), (11, forward, 1, 1), (12, give, 0, 2)]
        if sent < pack:
            for sub in range(SUBS):
                ex_recv[sub, sent:pack, :] = jnp.zeros((pack - sent, sub_cols), F32)

        with jax.named_scope("experts"):
            for sub in range(SUBS):
                ex_send[sub, 0:8, :] = jnp.zeros((8, sub_cols), F32)
                ex_own[sub, 0:8, :] = jnp.zeros((8, sub_cols), F32)

            @pl.loop(0, local_experts)
            def _(e):
                slot = lax.rem(e, 2)
                gate_copy(e, slot).wait()
                up_copy(e, slot).wait()
                rows = slot_x[pl.ds(pl.multiple_of(e * window, window), window), :]
                g = dot_bt(wg[slot], rows)
                u = dot_bt(wu[slot], rows)
                hidden = (jax.nn.silu(g) * u).astype(BF16)

                @pl.when(e + 2 < local_experts)
                def _():
                    gate_copy(e + 2, slot).start()
                    up_copy(e + 2, slot).start()

                down_copy(e, slot).wait()
                row = pl.multiple_of((e * capacity) // 8 * 8, 8)
                for buf, off in ((ex_send, peer_off), (ex_own, own_off)):
                    value = dot_at(hidden, wd[slot, :, pl.ds(off, half)])
                    for sub in range(SUBS):
                        part = value[:, sub * sub_cols:(sub + 1) * sub_cols]
                        buf[sub, pl.ds(row, 8), :] += part[0:8]
                        buf[sub, pl.ds(row + 8, window - 8), :] = part[8:]

                @pl.when(e + 2 < local_experts)
                def _():
                    down_copy(e + 2, slot).start()

                for i in range(groups):
                    @pl.when(e == last_expert[i])
                    def _():
                        yex_copy(0, i).start()
                        if i < EARLY_GROUPS:
                            yex_copy(1, i).start()

                for when, action, sub, i in loop_steps:
                    @pl.when(e == when)
                    def _():
                        action(sub, i)

            for i in range(EARLY_GROUPS, groups):
                yex_copy(1, i).start()

    pl.run_scoped(routed_phase, pltpu.VMEM((slots, 2 * tok), BF16), pltpu.VMEM((slots, 2 * tok), BF16),
                  pltpu.VMEM((2, ff_expert, d_model), BF16), pltpu.VMEM((2, ff_expert, d_model), BF16),
                  pltpu.VMEM((2, ff_expert, d_model), BF16), pltpu.SemaphoreType.DMA((2,)), pltpu.SemaphoreType.DMA((2,)), pltpu.SemaphoreType.DMA((2,)))

    with jax.named_scope("fin_shared"):
        for copy in xp_copies + fw_copies:
            copy.wait_send()
        res_load.wait()
        for r in range(ROW_BLOCKS):
            @pl.loop(0, n_half)
            def _(j):
                ysh_copy(r, j).wait()
                cols = pl.ds(pl.multiple_of(j * WIDE, WIDE), WIDE)
                rows = slice(r * r_rows, (r + 1) * r_rows)
                sh_own[j, rows, :] = res_half[rows, cols].astype(F32) + (sh_own[j, rows, :] + sh_recv[r, j])

    def combine(pick, sub, i):
        n = bounds[i + 1] - bounds[i]
        lanes = slice(ep_size * bounds[i], ep_size * bounds[i + 1])
        if sub == 0:
            lane = lax.broadcasted_iota(jnp.int32, (tok, ep_size * n), 1)
            owner = sum((lane >= q * n).astype(jnp.int32) for q in range(1, ep_size))
            lane_code = (lane + owner * (pack - n) + bounds[i]).astype(F32)
            pick[:, lanes] = (code_col[:, 0:1] == lane_code).astype(F32).astype(BF16)
        ret_copy(sub, i, me, rs_send, rs_recv, sib_dev).wait()
        ret_copy(sub, i, xp, rf_send, rf_recv, sib_dev).wait()
        rows = ret[sub, :, bounds[i]:bounds[i + 1], :].reshape(ep_size * n, sub_cols)
        gate = gate_col[:, 0:1]
        for j in range(sub_blocks):
            jj = sub * sub_blocks + j
            sh_own[jj] = sh_own[jj] + gate * dot(pick[:, lanes], rows[:, j * WIDE:(j + 1) * WIDE])

    def out_copies(sub):
        src = out_half.at[sub]
        dst = o_hbm.at[:, pl.ds(pl.multiple_of(own_off + sub * sub_cols, sub_cols), sub_cols)]
        return remote(src, dst, yo_send.at[sub], yo_recv.at[sub], y_peer), pltpu.make_async_copy(src, dst, lo_sem.at[sub])

    def emit(sub):
        for j in range(sub_blocks):
            out_half[sub, :, j * WIDE:(j + 1) * WIDE] = sh_own[sub * sub_blocks + j].astype(BF16)

    def start_out(sub):
        for copy in out_copies(sub):
            copy.start()

    def return_phase(pick):
        steps = [(give, 1, 2), (forward, 0, 2), (combine, 0, 0), (combine, 1, 0), (combine, 0, 1), (combine, 1, 1), (give, 0, 3), (forward, 1, 2), (combine, 0, 2),
                 (forward, 0, 3), (combine, 1, 2), (give, 0, 4), (combine, 0, 3), (forward, 0, 4), (combine, 0, 4), (emit, 0), (start_out, 0),
                 (give, 1, 3), (forward, 1, 3), (give, 1, 4), (combine, 1, 3), (forward, 1, 4), (combine, 1, 4), (emit, 1), (start_out, 1)]
        for step in steps:
            with jax.named_scope(step[0].__name__ + "".join(str(a) for a in step[1:])):
                if step[0] is combine:
                    combine(pick, *step[1:])
                else:
                    step[0](*step[1:])

    pl.run_scoped(return_phase, pltpu.VMEM((tok, ep_size * pack), BF16))

    with jax.named_scope("out"):
        for sub in range(SUBS):
            for copy in out_copies(sub):
                copy.wait()


def copy_kernel(src, dst, buf, in_sem, out_sem):
    n = src.shape[0] // COPY_CHUNKS
    reads = [pltpu.make_async_copy(src.at[pl.ds(c * n, n)], buf.at[pl.ds(c * n, n)], in_sem.at[c]) for c in range(COPY_CHUNKS)]
    writes = [pltpu.make_async_copy(buf.at[pl.ds(c * n, n)], dst.at[pl.ds(c * n, n)], out_sem.at[c]) for c in range(COPY_CHUNKS)]
    for copy in reads:
        copy.start()
    for read, write in zip(reads, writes):
        read.wait()
        write.start()
    for copy in writes:
        copy.wait()


def solution(mesh):
    ep_size = mesh.shape["ep"]
    tok_spec = P(("dp", "ep"), None)
    id_spec = P(("dp", "ep"))

    def device_step(normed, residual, w_router, ws_gate, ws_up, ws_down, we_gate, we_up, we_down, first_id, alt_id):
        tok, d_model = normed.shape
        local_experts, _, ff_expert = we_gate.shape
        experts = local_experts * ep_size
        capacity = (5 * tok * ep_size + 4 * experts - 1) // (4 * experts)
        window = -(-(capacity + 7) // 16) * 16
        pack = -(-local_experts * capacity // 16) * 16
        pack_buf = max(pack, (local_experts - 1) * capacity // 8 * 8 + window)
        bounds = [0] + [int(pack * f) // 32 * 32 for f in (0.13, 0.255, 0.52, 0.76)] + [pack]
        half = d_model // 2
        slots = local_experts * window
        n_half = half // WIDE
        r_rows = tok // ROW_BLOCKS
        sub_cols = half // SUBS
        dma = pltpu.SemaphoreType.DMA
        any_spec = pl.BlockSpec(memory_space=pl.ANY)
        vmem_spec = pl.BlockSpec(memory_space=pltpu.VMEM)
        per_ret = dma((SUBS, len(bounds) - 1))
        out = pl.pallas_call(
            functools.partial(moe_kernel, (experts, capacity, window, pack, bounds, local_experts, ep_size)),
            out_shape=jax.ShapeDtypeStruct((tok, d_model), BF16),
            in_specs=[any_spec] * 9 + [vmem_spec] * 2,
            out_specs=any_spec,
            scratch_shapes=[
                pltpu.VMEM((2, tok, d_model), BF16),
                pltpu.VMEM((2 * tok, d_model), BF16),
                pltpu.VMEM((ep_size, 8, tok), jnp.int32),
                pltpu.VMEM((ep_size, 8, tok), F32),
                pltpu.VMEM((tok, LANES), F32),
                pltpu.VMEM((tok, LANES), F32),
                pltpu.VMEM((slots, d_model), BF16),
                pltpu.VMEM((n_half, tok, WIDE), F32),
                pltpu.VMEM((ROW_BLOCKS, n_half, r_rows, WIDE), F32),
                pltpu.VMEM((ROW_BLOCKS, n_half, r_rows, WIDE), F32),
                pltpu.VMEM((SUBS, pack_buf, sub_cols), F32),
                pltpu.VMEM((SUBS, pack_buf, sub_cols), F32),
                pltpu.VMEM((SUBS, pack, sub_cols), F32),
                pltpu.VMEM((SUBS, ep_size, pack, sub_cols), BF16),
                pltpu.VMEM((SUBS, tok, sub_cols), BF16),
                pltpu.VMEM((tok, half), BF16),
                pltpu.VMEM((experts, d_model), F32),
                dma((ROW_BLOCKS + 2,)), dma((3,)), dma((3,)), dma((1,)), dma((1,)), dma((X_CHUNKS,)), dma((X_CHUNKS,)), dma((X_CHUNKS,)), dma((X_CHUNKS,)),
                dma((ROW_BLOCKS, n_half)), dma((ROW_BLOCKS, n_half)), per_ret, per_ret, per_ret, per_ret, per_ret, per_ret, per_ret, per_ret,
                dma((SUBS,)), dma((SUBS,)), dma((SUBS,)),
            ],
            compiler_params=pltpu.CompilerParams(collective_id=0, has_side_effects=True, vmem_limit_bytes=67043328),
        )(normed, residual, w_router.T, ws_gate, ws_up, ws_down, jnp.swapaxes(we_gate, 1, 2), jnp.swapaxes(we_up, 1, 2), we_down,
          first_id.reshape(1, tok), alt_id.reshape(1, tok))
        return pl.pallas_call(
            copy_kernel,
            out_shape=jax.ShapeDtypeStruct((tok, d_model), BF16),
            in_specs=[any_spec],
            out_specs=any_spec,
            scratch_shapes=[pltpu.VMEM((tok, d_model), BF16), dma((COPY_CHUNKS,)), dma((COPY_CHUNKS,))],
        )(out)

    return jax.shard_map(device_step, mesh=mesh, in_specs=(tok_spec, tok_spec, P(None, None), P(None, 'tp'), P(None, 'tp'), P('tp', None), P('ep', None, 'tp'), P('ep', None, 'tp'), P('ep', 'tp', None), id_spec, id_spec), out_specs=tok_spec, check_vma=False)
```

```python
import functools

import jax
import jax.numpy as jnp
from jax import lax
from jax.experimental import pallas as pl
from jax.experimental.pallas import tpu as pltpu
from jax.sharding import PartitionSpec as P

MESH = pl.DeviceIdType.MESH
F32 = jnp.float32
BF16 = jnp.bfloat16
LANES = 128
RANK_BLOCK = 256
X_SPLIT = (0, 320, 448, 512)
X_CHUNKS = 3
WIDE = 512
COPY_CHUNKS = 4
ROW_BLOCKS = 2
COL = 256
SUBS = 2
EARLY_GROUPS = 3
SHARED_BUFS = 3


def dot(a, b):
    return jnp.dot(a, b, preferred_element_type=F32)


def dot_bt(a, b):
    return lax.dot_general(a, b, (((1,), (1,)), ((), ())), preferred_element_type=F32)


def dot_at(a, b):
    return lax.dot_general(a, b, (((0,), (0,)), ((), ())), preferred_element_type=F32)


def moe_kernel(dims, x_hbm, res_hbm, wr_hbm, wsg_hbm, wsu_hbm, wsd_hbm, weg_hbm, weu_hbm, wed_hbm, first_ref, alt_ref, o_hbm,
               x_near, x_far, ids_all, code_rows, code_col, gate_col, slot_x, sh_own, sh_send, sh_recv, ex_own, ex_send, ex_recv, ret, out_half, res_half, wr,
               ld_sem, id_send, id_recv, sib_send, sib_recv, xp_send, xp_recv, fw_send, fw_recv,
               ysh_send, ysh_recv, yex_send, yex_recv, rs_send, rs_recv, rx_send, rx_recv, rf_send, rf_recv, yo_send, yo_recv, lo_sem):
    experts, capacity, window, pack, bounds, local_experts, ep_size = dims
    groups = len(bounds) - 1
    last_expert = [-(-min(b, local_experts * capacity) // capacity) - 1 for b in bounds[1:]]
    tok, d_model = x_hbm.shape
    half = d_model // 2
    slots = local_experts * window
    spare = pack - local_experts * capacity
    ff_shared = wsg_hbm.shape[1]
    ff_expert = weg_hbm.shape[1]
    dp = lax.axis_index("dp")
    t = lax.axis_index("tp")
    me = lax.axis_index("ep")
    core = lax.rem(me, 2)
    sib = me + 1 - 2 * core
    xp = lax.rem(me + 2, ep_size)
    diag = lax.rem(sib + 2, ep_size)
    y_peer = (dp, 1 - t, me)
    sib_dev = (dp, t, sib)
    xp_dev = (dp, t, xp)
    diag_dev = (dp, t, diag)
    own_off = pl.multiple_of(t * half, half)
    peer_off = pl.multiple_of((1 - t) * half, half)
    x_cuts = [tok * v // X_SPLIT[-1] for v in X_SPLIT]
    r_rows = tok // ROW_BLOCKS
    n_wide, tail = ff_shared // WIDE, ff_shared % WIDE
    n_chunks = n_wide + (tail > 0)
    n_half = half // WIDE
    sub_cols = half // SUBS
    sub_blocks = sub_cols // WIDE
    sent = -(-local_experts * capacity // 8) * 8

    barrier = pltpu.get_barrier_semaphore()
    for dev in (y_peer, sib_dev, xp_dev, diag_dev):
        pl.semaphore_signal(barrier, inc=1, device_id=dev, device_id_type=MESH)

    def remote(src, dst, s_sem, r_sem, dev):
        return pltpu.make_async_remote_copy(src_ref=src, dst_ref=dst, send_sem=s_sem, recv_sem=r_sem, device_id=dev, device_id_type=MESH)

    id_copies = [remote(ids_all.at[me], ids_all.at[me], id_send.at[i], id_recv.at[i], dev) for i, dev in enumerate((sib_dev, xp_dev, diag_dev))]
    def far_rows(c, i):
        n = x_cuts[c + 1] - x_cuts[c]
        return pl.ds(2 * x_cuts[c] + i * n, n)

    xp_copies = [remote(x_near.at[0, pl.ds(x_cuts[c], x_cuts[c + 1] - x_cuts[c])], x_far.at[far_rows(c, 0)], xp_send.at[c], xp_recv.at[c], xp_dev) for c in range(X_CHUNKS)]
    sib_copy = remote(x_near.at[0], x_near.at[1], sib_send.at[0], sib_recv.at[0], sib_dev)
    fw_copies = [remote(x_far.at[far_rows(c, 0)], x_far.at[far_rows(c, 1)], fw_send.at[c], fw_recv.at[c], sib_dev) for c in range(X_CHUNKS)]
    own_x = [pltpu.make_async_copy(x_hbm.at[pl.ds(r * r_rows, r_rows)], x_near.at[0, pl.ds(r * r_rows, r_rows)], ld_sem.at[r]) for r in range(ROW_BLOCKS)]
    res_load = pltpu.make_async_copy(res_hbm.at[:, pl.ds(own_off, half)], res_half, ld_sem.at[ROW_BLOCKS])
    wr_load = pltpu.make_async_copy(wr_hbm, wr, ld_sem.at[ROW_BLOCKS + 1])

    def ysh_copy(r, j):
        if r == 0:
            return remote(sh_send.at[r, j], sh_recv.at[r, j], ysh_send.at[r, j], ysh_recv.at[r, j], y_peer)
        return remote(sh_send.at[r], sh_recv.at[r], ysh_send.at[r, 0], ysh_recv.at[r, 0], y_peer)

    def shared_phase(act, wg, wu, wd, g_sem, u_sem, d_sem):
        def weight_copies(c, slot, width):
            cols = pl.ds(pl.multiple_of(c * WIDE, WIDE), width)
            dst = pl.ds(0, width)
            return (pltpu.make_async_copy(wsg_hbm.at[:, cols], wg.at[slot, :, dst], g_sem.at[slot]),
                    pltpu.make_async_copy(wsu_hbm.at[:, cols], wu.at[slot, :, dst], u_sem.at[slot]))

        def start_weights(k, slot):
            c = lax.rem(k, n_chunks)

            @pl.when(c < n_wide)
            def _():
                for copy in weight_copies(c, slot, WIDE):
                    copy.start()

            if tail:
                @pl.when(c == n_wide)
                def _():
                    for copy in weight_copies(c, slot, tail):
                        copy.start()

        def down_copy(k, slot):
            j = lax.rem(k, 2 * n_half)
            col = jnp.where(j < n_half, peer_off + j * WIDE, own_off + (j - n_half) * WIDE)
            return pltpu.make_async_copy(wsd_hbm.at[:, pl.ds(pl.multiple_of(col, WIDE), WIDE)], wd.at[slot], d_sem.at[slot])

        own_x[0].start()
        start_weights(jnp.int32(0), 0)
        for copy in own_x[1:]:
            copy.start()
        for slot in range(1, SHARED_BUFS):
            start_weights(jnp.int32(slot), slot)
        ids_all[pl.ds(me, 1), 0:1, :] = first_ref[...].reshape(1, 1, tok)
        ids_all[pl.ds(me, 1), 1:2, :] = alt_ref[...].reshape(1, 1, tok)
        def exchange():
            pl.semaphore_wait(barrier, 4)
            for copy in id_copies + xp_copies:
                copy.start()
            sib_copy.start()

        for copy in own_x:
            copy.wait()

        for r in range(ROW_BLOCKS):
            def gateup(c, width):
                k = c + r * n_chunks
                slot = lax.rem(k, SHARED_BUFS)
                for copy in weight_copies(c, slot, width):
                    copy.wait()
                x = x_near[0, r * r_rows:(r + 1) * r_rows, :]
                for lo in range(0, width, COL):
                    g = dot(x, wg[slot, :, lo:lo + COL])
                    u = dot(x, wu[slot, :, lo:lo + COL])
                    act[:, pl.ds(pl.multiple_of(c * WIDE + lo, COL), COL)] = (jax.nn.silu(g) * u).astype(BF16)

                @pl.when(k + SHARED_BUFS < ROW_BLOCKS * n_chunks)
                def _():
                    start_weights(k + SHARED_BUFS, slot)

            with jax.named_scope(f"gateup{r}"):
                @pl.loop(0, n_wide)
                def _(c):
                    gateup(c, WIDE)

                    if r == 0:
                        @pl.when(c == 0)
                        def _():
                            exchange()

                    if r == 0:
                        @pl.when((c == 1) | (c == 3))
                        def _():
                            slot = lax.div(c, 2)
                            down_copy(slot, slot).start()

                if tail:
                    gateup(jnp.int32(n_wide), tail)

            def down(j, base, store):
                k = j + r * 2 * n_half + base
                slot = lax.rem(k, 2)
                down_copy(k, slot).wait()
                store(dot(act[...], wd[slot]))

                @pl.when(k + 2 < ROW_BLOCKS * 2 * n_half)
                def _():
                    down_copy(k + 2, slot).start()

            with jax.named_scope(f"downpeer{r}"):
                @pl.loop(0, n_half)
                def _(j):
                    def store(value):
                        sh_send[r, j] = value
                        if r == 0:
                            ysh_copy(r, j).start()

                    down(j, 0, store)

                if r > 0:
                    ysh_copy(r, 0).start()

            if r == 0:
                wr_load.start()
            with jax.named_scope(f"downown{r}"):
                @pl.loop(0, n_half)
                def _(j):
                    def store(value):
                        sh_own[j, r * r_rows:(r + 1) * r_rows, :] = value

                    down(j, n_half, store)

    shared_sems = [pltpu.SemaphoreType.DMA((SHARED_BUFS,))] * 3
    pl.run_scoped(shared_phase, pltpu.VMEM((r_rows, ff_shared), BF16), pltpu.VMEM((SHARED_BUFS, d_model, WIDE), BF16), pltpu.VMEM((SHARED_BUFS, d_model, WIDE), BF16),
                  pltpu.VMEM((2, ff_shared, WIDE), BF16), *shared_sems)

    def yex_copy(sub, i):
        rows = pl.ds(bounds[i], min(bounds[i + 1], sent) - bounds[i])
        return remote(ex_send.at[sub, rows], ex_recv.at[sub, rows], yex_send.at[sub, i], yex_recv.at[sub, i], y_peer)

    def ret_copy(sub, i, who, s_sem, r_sem, dev):
        ref = ret.at[sub, who, pl.ds(bounds[i], bounds[i + 1] - bounds[i])]
        return remote(ref, ref, s_sem.at[sub, i], r_sem.at[sub, i], dev)

    def give(sub, i):
        yex_copy(sub, i).wait()
        rows = slice(bounds[i], bounds[i + 1])
        ret[sub, pl.ds(me, 1), rows, :] = (ex_own[sub, rows, :] + ex_recv[sub, rows, :]).astype(BF16).reshape(1, bounds[i + 1] - bounds[i], sub_cols)
        ret_copy(sub, i, me, rx_send, rx_recv, xp_dev).start()
        ret_copy(sub, i, me, rs_send, rs_recv, sib_dev).start()

    def forward(sub, i):
        ret_copy(sub, i, me, rx_send, rx_recv, xp_dev).wait()
        ret_copy(sub, i, xp, rf_send, rf_recv, sib_dev).start()

    def expert_base(ids):
        owner = sum((ids >= q * local_experts).astype(jnp.int32) for q in range(1, ep_size))
        return (ids * capacity + owner * spare).astype(F32)

    def routed_phase(sel_near, sel_far, wg, wu, wd, g_sem, u_sem, d_sem):
        def gate_copy(e, slot):
            return pltpu.make_async_copy(weg_hbm.at[e], wg.at[slot], g_sem.at[slot])

        def up_copy(e, slot):
            return pltpu.make_async_copy(weu_hbm.at[e], wu.at[slot], u_sem.at[slot])

        def down_copy(e, slot):
            return pltpu.make_async_copy(wed_hbm.at[e], wd.at[slot], d_sem.at[slot])

        for slot in range(2):
            gate_copy(slot, slot).start()
            up_copy(slot, slot).start()
            down_copy(slot, slot).start()

        res_load.start()
        with jax.named_scope("routing"):
            for copy in id_copies:
                copy.wait()
            e_pad = -(-experts // 8) * 8
            e_iota = lax.broadcasted_iota(jnp.int32, (e_pad, RANK_BLOCK), 0)
            row_i = lax.broadcasted_iota(jnp.int32, (RANK_BLOCK, RANK_BLOCK), 0)
            col_i = lax.broadcasted_iota(jnp.int32, (RANK_BLOCK, RANK_BLOCK), 1)
            upper = (row_i <= col_i).astype(F32).astype(BF16)
            blocks = [(q, b * RANK_BLOCK) for q in range(ep_size) for b in range(tok // RANK_BLOCK)]
            cap = jnp.float32(capacity)
            total = jnp.zeros((e_pad, 1), F32)
            rank_first = []
            for q, lo in blocks:
                first = ids_all[q, 0:1, lo:lo + RANK_BLOCK]
                hot = (e_iota == first).astype(F32)
                cum = dot(hot.astype(BF16), upper) + total
                rank_first.append(jnp.sum(cum * hot, axis=0, keepdims=True) - 1.0)
                total = total + jnp.sum(hot, axis=1, keepdims=True)
            load = jnp.minimum(total, cap)
            room = cap - load
            total = jnp.zeros((e_pad, 1), F32)
            for i, (q, lo) in enumerate(blocks):
                first = ids_all[q, 0:1, lo:lo + RANK_BLOCK]
                alt = ids_all[q, 1:2, lo:lo + RANK_BLOCK]
                kept = rank_first[i] < cap
                over = jnp.where(kept, 0.0, 1.0)
                hot = (e_iota == alt).astype(F32) * over
                cum = dot(hot.astype(BF16), upper) + total
                rank_alt = jnp.sum(cum * hot, axis=0, keepdims=True) - 1.0
                total = total + jnp.sum(hot, axis=1, keepdims=True)
                room_tok = jnp.sum(hot * room, axis=0, keepdims=True)
                load_tok = jnp.sum(hot * load, axis=0, keepdims=True)
                code_first = expert_base(first) + rank_first[i]
                code_alt = jnp.where(rank_alt < room_tok, expert_base(alt) + load_tok + rank_alt, -1.0)
                code = jnp.where(kept, code_first, code_alt)
                code_rows[q, :, lo:lo + RANK_BLOCK] = jnp.broadcast_to(code, (8, RANK_BLOCK))

            pos = lax.broadcasted_iota(jnp.int32, (slots, LANES), 0)
            slot_expert = sum((pos >= e * window).astype(jnp.int32) for e in range(1, local_experts))
            first_row = slot_expert * capacity
            row = (first_row // 8) * 8 + (pos - slot_expert * window)
            slot_code = jnp.where((row >= first_row) & (row < first_row + capacity), row + me * pack, -2).astype(F32)
            def pick_rows(codes):
                return (jnp.broadcast_to(slot_code[:, 0:1], (slots, codes.shape[1])) == codes).astype(F32).astype(BF16)

            for i, q in enumerate((me, sib)):
                codes = code_rows[q]
                for lo in range(0, tok, LANES):
                    sel_near[:, i * tok + lo:i * tok + lo + LANES] = pick_rows(codes[0:1, lo:lo + LANES])
            codes_xp, codes_diag = code_rows[xp][0:1, :], code_rows[diag][0:1, :]
            for c in range(X_CHUNKS):
                both = jnp.concatenate([codes_xp[:, x_cuts[c]:x_cuts[c + 1]], codes_diag[:, x_cuts[c]:x_cuts[c + 1]]], axis=1)
                for lo in range(0, 2 * (x_cuts[c + 1] - x_cuts[c]), LANES):
                    dst = 2 * x_cuts[c] + lo
                    sel_far[:, dst:dst + LANES] = pick_rows(both[:, lo:lo + LANES])

            code_t = jnp.broadcast_to(code_rows[me][0:1, :], (LANES, tok)).T
            code_col[...] = code_t

        with jax.named_scope("router"):
            wr_load.wait()
            x = x_near[0]
            w = wr[...]
            w_hi = w.astype(BF16)
            w_rest = w - w_hi.astype(F32)
            w_mid = w_rest.astype(BF16)
            w_lo = (w_rest - w_mid.astype(F32)).astype(BF16)
            logits = dot_bt(x, w_hi) + (dot_bt(x, w_mid) + dot_bt(x, w_lo))
            top = jnp.max(logits, axis=1, keepdims=True)
            prob = jnp.exp(logits - top)
            denom = jnp.sum(prob, axis=1, keepdims=True)
            lane_lo = expert_base(lax.broadcasted_iota(jnp.int32, (tok, experts), 1))
            code_e = code_t[:, 0:experts]
            picked = (code_e >= lane_lo) & (code_e < lane_lo + cap)
            gate = jnp.sum(jnp.where(picked, prob, 0.0), axis=1, keepdims=True) / denom
            gate_col[...] = jnp.broadcast_to(gate, (tok, LANES))

        nc = 512
        with jax.named_scope("near"):
            sib_copy.wait()

            @pl.loop(0, d_model // nc)
            def _(n):
                cols = pl.ds(pl.multiple_of(n * nc, nc), nc)
                slot_x[:, cols] = dot(sel_near[...], x_near[:, :, cols].reshape(2 * tok, nc)).astype(BF16)

        with jax.named_scope("far"):
            xp_copies[0].wait_recv()
            fw_copies[0].start()
            for c in range(X_CHUNKS):
                if c + 1 < X_CHUNKS:
                    xp_copies[c + 1].wait_recv()
                    fw_copies[c + 1].start()
                fw_copies[c].wait_recv()

                @pl.loop(0, d_model // nc)
                def _(n):
                    cols = pl.ds(pl.multiple_of(n * nc, nc), nc)
                    span = slice(2 * x_cuts[c], 2 * x_cuts[c + 1])
                    slot_x[:, cols] += dot(sel_far[:, span], x_far[span, cols]).astype(BF16)

        loop_steps = [(5, give, 0, 0), (6, give, 1, 0), (7, give, 0, 1), (8, forward, 0, 0), (8, give, 1, 1), (9, forward, 1, 0), (10, forward, 0, 1), (11, forward, 1, 1), (12, give, 0, 2)]
        if sent < pack:
            for sub in range(SUBS):
                ex_recv[sub, sent:pack, :] = jnp.zeros((pack - sent, sub_cols), F32)

        with jax.named_scope("experts"):
            for sub in range(SUBS):
                ex_send[sub, 0:8, :] = jnp.zeros((8, sub_cols), F32)
                ex_own[sub, 0:8, :] = jnp.zeros((8, sub_cols), F32)

            @pl.loop(0, local_experts)
            def _(e):
                slot = lax.rem(e, 2)
                gate_copy(e, slot).wait()
                up_copy(e, slot).wait()
                rows = slot_x[pl.ds(pl.multiple_of(e * window, window), window), :]
                g = dot_bt(wg[slot], rows)
                u = dot_bt(wu[slot], rows)
                hidden = (jax.nn.silu(g) * u).astype(BF16)

                @pl.when(e + 2 < local_experts)
                def _():
                    gate_copy(e + 2, slot).start()
                    up_copy(e + 2, slot).start()

                down_copy(e, slot).wait()
                row = pl.multiple_of((e * capacity) // 8 * 8, 8)
                for buf, off in ((ex_send, peer_off), (ex_own, own_off)):
                    value = dot_at(hidden, wd[slot, :, pl.ds(off, half)])
                    for sub in range(SUBS):
                        part = value[:, sub * sub_cols:(sub + 1) * sub_cols]
                        buf[sub, pl.ds(row, 8), :] += part[0:8]
                        buf[sub, pl.ds(row + 8, window - 8), :] = part[8:]

                @pl.when(e + 2 < local_experts)
                def _():
                    down_copy(e + 2, slot).start()

                for i in range(groups):
                    @pl.when(e == last_expert[i])
                    def _():
                        yex_copy(0, i).start()
                        if i < EARLY_GROUPS:
                            yex_copy(1, i).start()

                for when, action, sub, i in loop_steps:
                    @pl.when(e == when)
                    def _():
                        action(sub, i)

            for i in range(EARLY_GROUPS, groups):
                yex_copy(1, i).start()

    pl.run_scoped(routed_phase, pltpu.VMEM((slots, 2 * tok), BF16), pltpu.VMEM((slots, 2 * tok), BF16),
                  pltpu.VMEM((2, ff_expert, d_model), BF16), pltpu.VMEM((2, ff_expert, d_model), BF16),
                  pltpu.VMEM((2, ff_expert, d_model), BF16), pltpu.SemaphoreType.DMA((2,)), pltpu.SemaphoreType.DMA((2,)), pltpu.SemaphoreType.DMA((2,)))

    with jax.named_scope("fin_shared"):
        for copy in xp_copies + fw_copies:
            copy.wait_send()
        res_load.wait()
        for r in range(ROW_BLOCKS):
            if r > 0:
                ysh_copy(r, 0).wait()

            @pl.loop(0, n_half)
            def _(j):
                if r == 0:
                    ysh_copy(r, j).wait()
                cols = pl.ds(pl.multiple_of(j * WIDE, WIDE), WIDE)
                rows = slice(r * r_rows, (r + 1) * r_rows)
                sh_own[j, rows, :] = res_half[rows, cols].astype(F32) + (sh_own[j, rows, :] + sh_recv[r, j])

    def combine(pick, sub, i):
        n = bounds[i + 1] - bounds[i]
        lanes = slice(ep_size * bounds[i], ep_size * bounds[i + 1])
        if sub == 0:
            lane = lax.broadcasted_iota(jnp.int32, (tok, ep_size * n), 1)
            owner = sum((lane >= q * n).astype(jnp.int32) for q in range(1, ep_size))
            lane_code = (lane + owner * (pack - n) + bounds[i]).astype(F32)
            pick[:, lanes] = (code_col[:, 0:1] == lane_code).astype(F32).astype(BF16)
        ret_copy(sub, i, me, rs_send, rs_recv, sib_dev).wait()
        ret_copy(sub, i, xp, rf_send, rf_recv, sib_dev).wait()
        rows = ret[sub, :, bounds[i]:bounds[i + 1], :].reshape(ep_size * n, sub_cols)
        gate = gate_col[:, 0:1]
        for j in range(sub_blocks):
            jj = sub * sub_blocks + j
            sh_own[jj] = sh_own[jj] + gate * dot(pick[:, lanes], rows[:, j * WIDE:(j + 1) * WIDE])

    def out_copies(sub):
        src = out_half.at[sub]
        dst = o_hbm.at[:, pl.ds(pl.multiple_of(own_off + sub * sub_cols, sub_cols), sub_cols)]
        return remote(src, dst, yo_send.at[sub], yo_recv.at[sub], y_peer), pltpu.make_async_copy(src, dst, lo_sem.at[sub])

    def emit(sub):
        for j in range(sub_blocks):
            out_half[sub, :, j * WIDE:(j + 1) * WIDE] = sh_own[sub * sub_blocks + j].astype(BF16)

    def start_out(sub):
        for copy in out_copies(sub):
            copy.start()

    def return_phase(pick):
        steps = [(give, 1, 2), (forward, 0, 2), (combine, 0, 0), (combine, 1, 0), (combine, 0, 1), (combine, 1, 1), (give, 0, 3), (forward, 1, 2), (combine, 0, 2),
                 (forward, 0, 3), (combine, 1, 2), (give, 0, 4), (combine, 0, 3), (forward, 0, 4), (combine, 0, 4), (emit, 0), (start_out, 0),
                 (give, 1, 3), (forward, 1, 3), (give, 1, 4), (combine, 1, 3), (forward, 1, 4), (combine, 1, 4), (emit, 1), (start_out, 1)]
        for step in steps:
            with jax.named_scope(step[0].__name__ + "".join(str(a) for a in step[1:])):
                if step[0] is combine:
                    combine(pick, *step[1:])
                else:
                    step[0](*step[1:])

    pl.run_scoped(return_phase, pltpu.VMEM((tok, ep_size * pack), BF16))

    with jax.named_scope("out"):
        for sub in range(SUBS):
            for copy in out_copies(sub):
                copy.wait()


def copy_kernel(src, dst, buf, in_sem, out_sem):
    n = src.shape[0] // COPY_CHUNKS
    reads = [pltpu.make_async_copy(src.at[pl.ds(c * n, n)], buf.at[pl.ds(c * n, n)], in_sem.at[c]) for c in range(COPY_CHUNKS)]
    writes = [pltpu.make_async_copy(buf.at[pl.ds(c * n, n)], dst.at[pl.ds(c * n, n)], out_sem.at[c]) for c in range(COPY_CHUNKS)]
    for copy in reads:
        copy.start()
    for read, write in zip(reads, writes):
        read.wait()
        write.start()
    for copy in writes:
        copy.wait()


def solution(mesh):
    ep_size = mesh.shape["ep"]
    tok_spec = P(("dp", "ep"), None)
    id_spec = P(("dp", "ep"))

    def device_step(normed, residual, w_router, ws_gate, ws_up, ws_down, we_gate, we_up, we_down, first_id, alt_id):
        tok, d_model = normed.shape
        local_experts, _, ff_expert = we_gate.shape
        experts = local_experts * ep_size
        capacity = (5 * tok * ep_size + 4 * experts - 1) // (4 * experts)
        window = -(-(capacity + 7) // 16) * 16
        pack = -(-local_experts * capacity // 16) * 16
        pack_buf = max(pack, (local_experts - 1) * capacity // 8 * 8 + window)
        bounds = [0] + [int(pack * f) // 32 * 32 for f in (0.13, 0.255, 0.45, 0.76)] + [pack]
        half = d_model // 2
        slots = local_experts * window
        n_half = half // WIDE
        r_rows = tok // ROW_BLOCKS
        sub_cols = half // SUBS
        dma = pltpu.SemaphoreType.DMA
        any_spec = pl.BlockSpec(memory_space=pl.ANY)
        vmem_spec = pl.BlockSpec(memory_space=pltpu.VMEM)
        per_ret = dma((SUBS, len(bounds) - 1))
        out = pl.pallas_call(
            functools.partial(moe_kernel, (experts, capacity, window, pack, bounds, local_experts, ep_size)),
            out_shape=jax.ShapeDtypeStruct((tok, d_model), BF16),
            in_specs=[any_spec] * 9 + [vmem_spec] * 2,
            out_specs=any_spec,
            scratch_shapes=[
                pltpu.VMEM((2, tok, d_model), BF16),
                pltpu.VMEM((2 * tok, d_model), BF16),
                pltpu.VMEM((ep_size, 8, tok), jnp.int32),
                pltpu.VMEM((ep_size, 8, tok), F32),
                pltpu.VMEM((tok, LANES), F32),
                pltpu.VMEM((tok, LANES), F32),
                pltpu.VMEM((slots, d_model), BF16),
                pltpu.VMEM((n_half, tok, WIDE), F32),
                pltpu.VMEM((ROW_BLOCKS, n_half, r_rows, WIDE), F32),
                pltpu.VMEM((ROW_BLOCKS, n_half, r_rows, WIDE), F32),
                pltpu.VMEM((SUBS, pack_buf, sub_cols), F32),
                pltpu.VMEM((SUBS, pack_buf, sub_cols), F32),
                pltpu.VMEM((SUBS, pack, sub_cols), F32),
                pltpu.VMEM((SUBS, ep_size, pack, sub_cols), BF16),
                pltpu.VMEM((SUBS, tok, sub_cols), BF16),
                pltpu.VMEM((tok, half), BF16),
                pltpu.VMEM((experts, d_model), F32),
                dma((ROW_BLOCKS + 2,)), dma((3,)), dma((3,)), dma((1,)), dma((1,)), dma((X_CHUNKS,)), dma((X_CHUNKS,)), dma((X_CHUNKS,)), dma((X_CHUNKS,)),
                dma((ROW_BLOCKS, n_half)), dma((ROW_BLOCKS, n_half)), per_ret, per_ret, per_ret, per_ret, per_ret, per_ret, per_ret, per_ret,
                dma((SUBS,)), dma((SUBS,)), dma((SUBS,)),
            ],
            compiler_params=pltpu.CompilerParams(collective_id=0, has_side_effects=True, vmem_limit_bytes=67043328),
        )(normed, residual, w_router.T, ws_gate, ws_up, ws_down, jnp.swapaxes(we_gate, 1, 2), jnp.swapaxes(we_up, 1, 2), we_down,
          first_id.reshape(1, tok), alt_id.reshape(1, tok))
        return pl.pallas_call(
            copy_kernel,
            out_shape=jax.ShapeDtypeStruct((tok, d_model), BF16),
            in_specs=[any_spec],
            out_specs=any_spec,
            scratch_shapes=[pltpu.VMEM((tok, d_model), BF16), dma((COPY_CHUNKS,)), dma((COPY_CHUNKS,))],
        )(out)

    return jax.shard_map(device_step, mesh=mesh, in_specs=(tok_spec, tok_spec, P(None, None), P(None, 'tp'), P(None, 'tp'), P('tp', None), P('ep', None, 'tp'), P('ep', None, 'tp'), P('ep', 'tp', None), id_spec, id_spec), out_specs=tok_spec, check_vma=False)
```

```python
import functools

import jax
import jax.numpy as jnp
from jax import lax
from jax.experimental import pallas as pl
from jax.experimental.pallas import tpu as pltpu
from jax.sharding import PartitionSpec as P

MESH = pl.DeviceIdType.MESH
F32 = jnp.float32
BF16 = jnp.bfloat16
LANES = 128
RANK_BLOCK = 256
X_SPLIT = (0, 192, 384, 512)
X_CHUNKS = 3
WIDE = 512
COPY_CHUNKS = 4
ROW_BLOCKS = 2
COL = 256
SUBS = 2
EARLY_GROUPS = 3
SHARED_BUFS = 3


def dot(a, b):
    return jnp.dot(a, b, preferred_element_type=F32)


def dot_bt(a, b):
    return lax.dot_general(a, b, (((1,), (1,)), ((), ())), preferred_element_type=F32)


def dot_at(a, b):
    return lax.dot_general(a, b, (((0,), (0,)), ((), ())), preferred_element_type=F32)


def moe_kernel(dims, x_hbm, res_hbm, wr_hbm, wsg_hbm, wsu_hbm, wsd_hbm, weg_hbm, weu_hbm, wed_hbm, first_ref, alt_ref, o_hbm,
               x_near, x_far, x_sorted, ids_all, code_rows, code_col, gate_col, slot_x, sh_own, sh_send, sh_recv, ex_own, ex_send, ex_recv, ret, out_half, res_half, wr,
               ld_sem, id_send, id_recv, sib_send, sib_recv, xp_send, xp_recv, fw_send, fw_recv,
               ysh_send, ysh_recv, yex_send, yex_recv, rs_send, rs_recv, rx_send, rx_recv, rf_send, rf_recv, yo_send, yo_recv, lo_sem):
    experts, capacity, window, pack, bounds, local_experts, ep_size = dims
    groups = len(bounds) - 1
    last_expert = [-(-min(b, local_experts * capacity) // capacity) - 1 for b in bounds[1:]]
    tok, d_model = x_hbm.shape
    half = d_model // 2
    slots = local_experts * window
    spare = pack - local_experts * capacity
    ff_shared = wsg_hbm.shape[1]
    ff_expert = weg_hbm.shape[1]
    dp = lax.axis_index("dp")
    t = lax.axis_index("tp")
    me = lax.axis_index("ep")
    core = lax.rem(me, 2)
    sib = me + 1 - 2 * core
    xp = lax.rem(me + 2, ep_size)
    diag = lax.rem(sib + 2, ep_size)
    y_peer = (dp, 1 - t, me)
    sib_dev = (dp, t, sib)
    xp_dev = (dp, t, xp)
    diag_dev = (dp, t, diag)
    own_off = pl.multiple_of(t * half, half)
    peer_off = pl.multiple_of((1 - t) * half, half)
    x_cuts = [tok * v // X_SPLIT[-1] for v in X_SPLIT]
    r_rows = tok // ROW_BLOCKS
    n_wide, tail = ff_shared // WIDE, ff_shared % WIDE
    n_chunks = n_wide + (tail > 0)
    n_half = half // WIDE
    sub_cols = half // SUBS
    sub_blocks = sub_cols // WIDE
    sent = -(-local_experts * capacity // 8) * 8

    barrier = pltpu.get_barrier_semaphore()
    for dev in (y_peer, sib_dev, xp_dev, diag_dev):
        pl.semaphore_signal(barrier, inc=1, device_id=dev, device_id_type=MESH)

    def remote(src, dst, s_sem, r_sem, dev):
        return pltpu.make_async_remote_copy(src_ref=src, dst_ref=dst, send_sem=s_sem, recv_sem=r_sem, device_id=dev, device_id_type=MESH)

    id_copies = [remote(ids_all.at[me], ids_all.at[me], id_send.at[i], id_recv.at[i], dev) for i, dev in enumerate((sib_dev, xp_dev, diag_dev))]
    def far_rows(c, i):
        n = x_cuts[c + 1] - x_cuts[c]
        return pl.ds(2 * x_cuts[c] + i * n, n)

    xp_copies = [remote(x_sorted.at[pl.ds(x_cuts[c], x_cuts[c + 1] - x_cuts[c])], x_far.at[far_rows(c, 0)], xp_send.at[c], xp_recv.at[c], xp_dev) for c in range(X_CHUNKS)]
    sib_copy = remote(x_near.at[0], x_near.at[1], sib_send.at[0], sib_recv.at[0], sib_dev)
    fw_copies = [remote(x_far.at[far_rows(c, 0)], x_far.at[far_rows(c, 1)], fw_send.at[c], fw_recv.at[c], sib_dev) for c in range(X_CHUNKS)]
    own_x = [pltpu.make_async_copy(x_hbm.at[pl.ds(r * r_rows, r_rows)], x_near.at[0, pl.ds(r * r_rows, r_rows)], ld_sem.at[r]) for r in range(ROW_BLOCKS)]
    res_load = pltpu.make_async_copy(res_hbm.at[:, pl.ds(own_off, half)], res_half, ld_sem.at[ROW_BLOCKS])
    wr_load = pltpu.make_async_copy(wr_hbm, wr, ld_sem.at[ROW_BLOCKS + 1])

    cap = jnp.float32(capacity)

    def expert_base(ids):
        owner = sum((ids >= q * local_experts).astype(jnp.int32) for q in range(1, ep_size))
        return (ids * capacity + owner * spare).astype(F32)

    def route():
        for copy in id_copies:
            copy.wait()
        e_pad = -(-experts // 8) * 8
        e_iota = lax.broadcasted_iota(jnp.int32, (e_pad, RANK_BLOCK), 0)
        row_i = lax.broadcasted_iota(jnp.int32, (RANK_BLOCK, RANK_BLOCK), 0)
        col_i = lax.broadcasted_iota(jnp.int32, (RANK_BLOCK, RANK_BLOCK), 1)
        upper = (row_i <= col_i).astype(F32).astype(BF16)
        blocks = [(q, b * RANK_BLOCK) for q in range(ep_size) for b in range(tok // RANK_BLOCK)]
        total = jnp.zeros((e_pad, 1), F32)
        rank_first = []
        for q, lo in blocks:
            first = ids_all[q, 0:1, lo:lo + RANK_BLOCK]
            hot = (e_iota == first).astype(F32)
            cum = dot(hot.astype(BF16), upper) + total
            rank_first.append(jnp.sum(cum * hot, axis=0, keepdims=True) - 1.0)
            total = total + jnp.sum(hot, axis=1, keepdims=True)
        load = jnp.minimum(total, cap)
        room = cap - load
        total = jnp.zeros((e_pad, 1), F32)
        for i, (q, lo) in enumerate(blocks):
            first = ids_all[q, 0:1, lo:lo + RANK_BLOCK]
            alt = ids_all[q, 1:2, lo:lo + RANK_BLOCK]
            kept = rank_first[i] < cap
            over = jnp.where(kept, 0.0, 1.0)
            hot = (e_iota == alt).astype(F32) * over
            cum = dot(hot.astype(BF16), upper) + total
            rank_alt = jnp.sum(cum * hot, axis=0, keepdims=True) - 1.0
            total = total + jnp.sum(hot, axis=1, keepdims=True)
            room_tok = jnp.sum(hot * room, axis=0, keepdims=True)
            load_tok = jnp.sum(hot * load, axis=0, keepdims=True)
            code_first = expert_base(first) + rank_first[i]
            code_alt = jnp.where(rank_alt < room_tok, expert_base(alt) + load_tok + rank_alt, -1.0)
            code = jnp.where(kept, code_first, code_alt)
            code_rows[q, :, lo:lo + RANK_BLOCK] = jnp.broadcast_to(code, (8, RANK_BLOCK))

    def sort_block(q):
        code_t = jnp.broadcast_to(code_rows[q][0:1, :], (LANES, tok)).T[:, 0:1]
        shift = ((1 - lax.div(q, 2)) * (2 * pack)).astype(F32)

        def key_of(code):
            rel = code - shift
            local = jnp.where(rel >= pack, rel - pack, rel)
            return jnp.where((rel >= 0.0) & (rel < 2.0 * pack), local, 8192.0)

        key_t = key_of(code_t)
        key = key_of(code_rows[q][0:1, :])
        lane = lax.broadcasted_iota(jnp.int32, (tok, tok), 1)
        line = lax.broadcasted_iota(jnp.int32, (tok, tok), 0)
        ahead = (key < key_t) | ((key == key_t) & (lane < line))
        position = jnp.sum(jnp.where(ahead, 1.0, 0.0), axis=1, keepdims=True)
        return position == lane.astype(F32), code_t

    def dispatch():
        route()
        hit, _ = sort_block(me)
        order = hit.astype(F32).astype(BF16)
        for lo in range(0, d_model, WIDE):
            x_sorted[:, lo:lo + WIDE] = dot_at(order, x_near[0, :, lo:lo + WIDE]).astype(BF16)
        for copy in xp_copies:
            copy.start()

    def ysh_copy(r, j):
        if r == 0:
            return remote(sh_send.at[r, j], sh_recv.at[r, j], ysh_send.at[r, j], ysh_recv.at[r, j], y_peer)
        return remote(sh_send.at[r], sh_recv.at[r], ysh_send.at[r, 0], ysh_recv.at[r, 0], y_peer)

    def shared_phase(act, wg, wu, wd, g_sem, u_sem, d_sem):
        def weight_copies(c, slot, width):
            cols = pl.ds(pl.multiple_of(c * WIDE, WIDE), width)
            dst = pl.ds(0, width)
            return (pltpu.make_async_copy(wsg_hbm.at[:, cols], wg.at[slot, :, dst], g_sem.at[slot]),
                    pltpu.make_async_copy(wsu_hbm.at[:, cols], wu.at[slot, :, dst], u_sem.at[slot]))

        def start_weights(k, slot):
            c = lax.rem(k, n_chunks)

            @pl.when(c < n_wide)
            def _():
                for copy in weight_copies(c, slot, WIDE):
                    copy.start()

            if tail:
                @pl.when(c == n_wide)
                def _():
                    for copy in weight_copies(c, slot, tail):
                        copy.start()

        def down_copy(k, slot):
            j = lax.rem(k, 2 * n_half)
            col = jnp.where(j < n_half, peer_off + j * WIDE, own_off + (j - n_half) * WIDE)
            return pltpu.make_async_copy(wsd_hbm.at[:, pl.ds(pl.multiple_of(col, WIDE), WIDE)], wd.at[slot], d_sem.at[slot])

        own_x[0].start()
        start_weights(jnp.int32(0), 0)
        for copy in own_x[1:]:
            copy.start()
        for slot in range(1, SHARED_BUFS):
            start_weights(jnp.int32(slot), slot)
        ids_all[pl.ds(me, 1), 0:1, :] = first_ref[...].reshape(1, 1, tok)
        ids_all[pl.ds(me, 1), 1:2, :] = alt_ref[...].reshape(1, 1, tok)
        def exchange():
            pl.semaphore_wait(barrier, 4)
            for copy in id_copies:
                copy.start()
            sib_copy.start()

        for copy in own_x:
            copy.wait()

        for r in range(ROW_BLOCKS):
            def gateup(c, width):
                k = c + r * n_chunks
                slot = lax.rem(k, SHARED_BUFS)
                for copy in weight_copies(c, slot, width):
                    copy.wait()
                x = x_near[0, r * r_rows:(r + 1) * r_rows, :]
                for lo in range(0, width, COL):
                    g = dot(x, wg[slot, :, lo:lo + COL])
                    u = dot(x, wu[slot, :, lo:lo + COL])
                    act[:, pl.ds(pl.multiple_of(c * WIDE + lo, COL), COL)] = (jax.nn.silu(g) * u).astype(BF16)

                @pl.when(k + SHARED_BUFS < ROW_BLOCKS * n_chunks)
                def _():
                    start_weights(k + SHARED_BUFS, slot)

            with jax.named_scope(f"gateup{r}"):
                @pl.loop(0, n_wide)
                def _(c):
                    gateup(c, WIDE)

                    if r == 0:
                        @pl.when(c == 0)
                        def _():
                            exchange()

                    if r == 0:
                        @pl.when((c == 1) | (c == 3))
                        def _():
                            slot = lax.div(c, 2)
                            down_copy(slot, slot).start()

                if tail:
                    gateup(jnp.int32(n_wide), tail)

            def down(j, base, store):
                k = j + r * 2 * n_half + base
                slot = lax.rem(k, 2)
                down_copy(k, slot).wait()
                store(dot(act[...], wd[slot]))

                @pl.when(k + 2 < ROW_BLOCKS * 2 * n_half)
                def _():
                    down_copy(k + 2, slot).start()

            with jax.named_scope(f"downpeer{r}"):
                @pl.loop(0, n_half)
                def _(j):
                    def store(value):
                        sh_send[r, j] = value
                        if r == 0:
                            ysh_copy(r, j).start()

                    down(j, 0, store)

                if r > 0:
                    ysh_copy(r, 0).start()

            if r == 0:
                wr_load.start()
                with jax.named_scope("dispatch"):
                    dispatch()
            with jax.named_scope(f"downown{r}"):
                @pl.loop(0, n_half)
                def _(j):
                    def store(value):
                        sh_own[j, r * r_rows:(r + 1) * r_rows, :] = value

                    down(j, n_half, store)

    shared_sems = [pltpu.SemaphoreType.DMA((SHARED_BUFS,))] * 3
    pl.run_scoped(shared_phase, pltpu.VMEM((r_rows, ff_shared), BF16), pltpu.VMEM((SHARED_BUFS, d_model, WIDE), BF16), pltpu.VMEM((SHARED_BUFS, d_model, WIDE), BF16),
                  pltpu.VMEM((2, ff_shared, WIDE), BF16), *shared_sems)

    def yex_copy(sub, i):
        rows = pl.ds(bounds[i], min(bounds[i + 1], sent) - bounds[i])
        return remote(ex_send.at[sub, rows], ex_recv.at[sub, rows], yex_send.at[sub, i], yex_recv.at[sub, i], y_peer)

    def ret_copy(sub, i, who, s_sem, r_sem, dev):
        ref = ret.at[sub, who, pl.ds(bounds[i], bounds[i + 1] - bounds[i])]
        return remote(ref, ref, s_sem.at[sub, i], r_sem.at[sub, i], dev)

    def give(sub, i):
        yex_copy(sub, i).wait()
        rows = slice(bounds[i], bounds[i + 1])
        ret[sub, pl.ds(me, 1), rows, :] = (ex_own[sub, rows, :] + ex_recv[sub, rows, :]).astype(BF16).reshape(1, bounds[i + 1] - bounds[i], sub_cols)
        ret_copy(sub, i, me, rx_send, rx_recv, xp_dev).start()
        ret_copy(sub, i, me, rs_send, rs_recv, sib_dev).start()

    def forward(sub, i):
        ret_copy(sub, i, me, rx_send, rx_recv, xp_dev).wait()
        ret_copy(sub, i, xp, rf_send, rf_recv, sib_dev).start()

    def routed_phase(sel_near, sel_far, wg, wu, wd, g_sem, u_sem, d_sem):
        def gate_copy(e, slot):
            return pltpu.make_async_copy(weg_hbm.at[e], wg.at[slot], g_sem.at[slot])

        def up_copy(e, slot):
            return pltpu.make_async_copy(weu_hbm.at[e], wu.at[slot], u_sem.at[slot])

        def down_copy(e, slot):
            return pltpu.make_async_copy(wed_hbm.at[e], wd.at[slot], d_sem.at[slot])

        for slot in range(2):
            gate_copy(slot, slot).start()
            up_copy(slot, slot).start()
            down_copy(slot, slot).start()

        res_load.start()
        with jax.named_scope("routing"):
            pos = lax.broadcasted_iota(jnp.int32, (slots, LANES), 0)
            slot_expert = sum((pos >= e * window).astype(jnp.int32) for e in range(1, local_experts))
            first_row = slot_expert * capacity
            row = (first_row // 8) * 8 + (pos - slot_expert * window)
            slot_code = jnp.where((row >= first_row) & (row < first_row + capacity), row + me * pack, -2).astype(F32)
            def pick_rows(codes):
                return (jnp.broadcast_to(slot_code[:, 0:1], (slots, codes.shape[1])) == codes).astype(F32).astype(BF16)

            for i, q in enumerate((me, sib)):
                codes = code_rows[q]
                for lo in range(0, tok, LANES):
                    sel_near[:, i * tok + lo:i * tok + lo + LANES] = pick_rows(codes[0:1, lo:lo + LANES])
            def sorted_codes(q):
                hit, code_t = sort_block(q)
                return jnp.sum(jnp.where(hit, code_t, 0.0), axis=0, keepdims=True)

            codes_xp, codes_diag = sorted_codes(xp), sorted_codes(diag)
            for c in range(X_CHUNKS):
                both = jnp.concatenate([codes_xp[:, x_cuts[c]:x_cuts[c + 1]], codes_diag[:, x_cuts[c]:x_cuts[c + 1]]], axis=1)
                for lo in range(0, 2 * (x_cuts[c + 1] - x_cuts[c]), LANES):
                    dst = 2 * x_cuts[c] + lo
                    sel_far[:, dst:dst + LANES] = pick_rows(both[:, lo:lo + LANES])

            code_t = jnp.broadcast_to(code_rows[me][0:1, :], (LANES, tok)).T
            code_col[...] = code_t

        with jax.named_scope("router"):
            wr_load.wait()
            x = x_near[0]
            w = wr[...]
            w_hi = w.astype(BF16)
            w_rest = w - w_hi.astype(F32)
            w_mid = w_rest.astype(BF16)
            w_lo = (w_rest - w_mid.astype(F32)).astype(BF16)
            logits = dot_bt(x, w_hi) + (dot_bt(x, w_mid) + dot_bt(x, w_lo))
            top = jnp.max(logits, axis=1, keepdims=True)
            prob = jnp.exp(logits - top)
            denom = jnp.sum(prob, axis=1, keepdims=True)
            lane_lo = expert_base(lax.broadcasted_iota(jnp.int32, (tok, experts), 1))
            code_e = code_t[:, 0:experts]
            picked = (code_e >= lane_lo) & (code_e < lane_lo + cap)
            gate = jnp.sum(jnp.where(picked, prob, 0.0), axis=1, keepdims=True) / denom
            gate_col[...] = jnp.broadcast_to(gate, (tok, LANES))

        nc = 512
        with jax.named_scope("near"):
            sib_copy.wait()

            @pl.loop(0, d_model // nc)
            def _(n):
                cols = pl.ds(pl.multiple_of(n * nc, nc), nc)
                slot_x[:, cols] = dot(sel_near[...], x_near[:, :, cols].reshape(2 * tok, nc)).astype(BF16)

        def far(c):
            xp_copies[c].wait_recv()
            fw_copies[c].start()
            fw_copies[c].wait_recv()

            @pl.loop(0, d_model // nc)
            def _(n):
                cols = pl.ds(pl.multiple_of(n * nc, nc), nc)
                span = slice(2 * x_cuts[c], 2 * x_cuts[c + 1])
                slot_x[:, cols] += dot(sel_far[:, span], x_far[span, cols]).astype(BF16)

        loop_steps = [(5, give, 0, 0), (6, give, 1, 0), (7, give, 0, 1), (8, forward, 0, 0), (8, give, 1, 1), (9, forward, 1, 0), (10, forward, 0, 1), (11, forward, 1, 1), (12, give, 0, 2)]
        far_at = [x_cuts[c] // (2 * capacity) for c in range(X_CHUNKS)]
        if sent < pack:
            for sub in range(SUBS):
                ex_recv[sub, sent:pack, :] = jnp.zeros((pack - sent, sub_cols), F32)

        with jax.named_scope("experts"):
            for sub in range(SUBS):
                ex_send[sub, 0:8, :] = jnp.zeros((8, sub_cols), F32)
                ex_own[sub, 0:8, :] = jnp.zeros((8, sub_cols), F32)

            @pl.loop(0, local_experts)
            def _(e):
                slot = lax.rem(e, 2)
                for c in range(X_CHUNKS):
                    @pl.when(e == far_at[c])
                    def _():
                        with jax.named_scope(f"far{c}"):
                            far(c)

                gate_copy(e, slot).wait()
                up_copy(e, slot).wait()
                rows = slot_x[pl.ds(pl.multiple_of(e * window, window), window), :]
                g = dot_bt(wg[slot], rows)
                u = dot_bt(wu[slot], rows)
                hidden = (jax.nn.silu(g) * u).astype(BF16)

                @pl.when(e + 2 < local_experts)
                def _():
                    gate_copy(e + 2, slot).start()
                    up_copy(e + 2, slot).start()

                down_copy(e, slot).wait()
                row = pl.multiple_of((e * capacity) // 8 * 8, 8)
                for buf, off in ((ex_send, peer_off), (ex_own, own_off)):
                    value = dot_at(hidden, wd[slot, :, pl.ds(off, half)])
                    for sub in range(SUBS):
                        part = value[:, sub * sub_cols:(sub + 1) * sub_cols]
                        buf[sub, pl.ds(row, 8), :] += part[0:8]
                        buf[sub, pl.ds(row + 8, window - 8), :] = part[8:]

                @pl.when(e + 2 < local_experts)
                def _():
                    down_copy(e + 2, slot).start()

                for i in range(groups):
                    @pl.when(e == last_expert[i])
                    def _():
                        yex_copy(0, i).start()
                        if i < EARLY_GROUPS:
                            yex_copy(1, i).start()

                for when, action, sub, i in loop_steps:
                    @pl.when(e == when)
                    def _():
                        action(sub, i)

            for i in range(EARLY_GROUPS, groups):
                yex_copy(1, i).start()

    pl.run_scoped(routed_phase, pltpu.VMEM((slots, 2 * tok), BF16), pltpu.VMEM((slots, 2 * tok), BF16),
                  pltpu.VMEM((2, ff_expert, d_model), BF16), pltpu.VMEM((2, ff_expert, d_model), BF16),
                  pltpu.VMEM((2, ff_expert, d_model), BF16), pltpu.SemaphoreType.DMA((2,)), pltpu.SemaphoreType.DMA((2,)), pltpu.SemaphoreType.DMA((2,)))

    with jax.named_scope("fin_shared"):
        for copy in xp_copies + fw_copies:
            copy.wait_send()
        res_load.wait()
        for r in range(ROW_BLOCKS):
            if r > 0:
                ysh_copy(r, 0).wait()

            @pl.loop(0, n_half)
            def _(j):
                if r == 0:
                    ysh_copy(r, j).wait()
                cols = pl.ds(pl.multiple_of(j * WIDE, WIDE), WIDE)
                rows = slice(r * r_rows, (r + 1) * r_rows)
                sh_own[j, rows, :] = res_half[rows, cols].astype(F32) + (sh_own[j, rows, :] + sh_recv[r, j])

    def combine(pick, sub, i):
        n = bounds[i + 1] - bounds[i]
        lanes = slice(ep_size * bounds[i], ep_size * bounds[i + 1])
        if sub == 0:
            lane = lax.broadcasted_iota(jnp.int32, (tok, ep_size * n), 1)
            owner = sum((lane >= q * n).astype(jnp.int32) for q in range(1, ep_size))
            lane_code = (lane + owner * (pack - n) + bounds[i]).astype(F32)
            pick[:, lanes] = (code_col[:, 0:1] == lane_code).astype(F32).astype(BF16)
        ret_copy(sub, i, me, rs_send, rs_recv, sib_dev).wait()
        ret_copy(sub, i, xp, rf_send, rf_recv, sib_dev).wait()
        rows = ret[sub, :, bounds[i]:bounds[i + 1], :].reshape(ep_size * n, sub_cols)
        gate = gate_col[:, 0:1]
        for j in range(sub_blocks):
            jj = sub * sub_blocks + j
            sh_own[jj] = sh_own[jj] + gate * dot(pick[:, lanes], rows[:, j * WIDE:(j + 1) * WIDE])

    def out_copies(sub):
        src = out_half.at[sub]
        dst = o_hbm.at[:, pl.ds(pl.multiple_of(own_off + sub * sub_cols, sub_cols), sub_cols)]
        return remote(src, dst, yo_send.at[sub], yo_recv.at[sub], y_peer), pltpu.make_async_copy(src, dst, lo_sem.at[sub])

    def emit(sub):
        for j in range(sub_blocks):
            out_half[sub, :, j * WIDE:(j + 1) * WIDE] = sh_own[sub * sub_blocks + j].astype(BF16)

    def start_out(sub):
        for copy in out_copies(sub):
            copy.start()

    def return_phase(pick):
        steps = [(give, 1, 2), (forward, 0, 2), (combine, 0, 0), (combine, 1, 0), (combine, 0, 1), (combine, 1, 1), (give, 0, 3), (forward, 1, 2), (combine, 0, 2),
                 (forward, 0, 3), (combine, 1, 2), (give, 0, 4), (combine, 0, 3), (forward, 0, 4), (combine, 0, 4), (emit, 0), (start_out, 0),
                 (give, 1, 3), (forward, 1, 3), (give, 1, 4), (combine, 1, 3), (forward, 1, 4), (combine, 1, 4), (emit, 1), (start_out, 1)]
        for step in steps:
            with jax.named_scope(step[0].__name__ + "".join(str(a) for a in step[1:])):
                if step[0] is combine:
                    combine(pick, *step[1:])
                else:
                    step[0](*step[1:])

    pl.run_scoped(return_phase, pltpu.VMEM((tok, ep_size * pack), BF16))

    with jax.named_scope("out"):
        for sub in range(SUBS):
            for copy in out_copies(sub):
                copy.wait()


def copy_kernel(src, dst, buf, in_sem, out_sem):
    n = src.shape[0] // COPY_CHUNKS
    reads = [pltpu.make_async_copy(src.at[pl.ds(c * n, n)], buf.at[pl.ds(c * n, n)], in_sem.at[c]) for c in range(COPY_CHUNKS)]
    writes = [pltpu.make_async_copy(buf.at[pl.ds(c * n, n)], dst.at[pl.ds(c * n, n)], out_sem.at[c]) for c in range(COPY_CHUNKS)]
    for copy in reads:
        copy.start()
    for read, write in zip(reads, writes):
        read.wait()
        write.start()
    for copy in writes:
        copy.wait()


def solution(mesh):
    ep_size = mesh.shape["ep"]
    tok_spec = P(("dp", "ep"), None)
    id_spec = P(("dp", "ep"))

    def device_step(normed, residual, w_router, ws_gate, ws_up, ws_down, we_gate, we_up, we_down, first_id, alt_id):
        tok, d_model = normed.shape
        local_experts, _, ff_expert = we_gate.shape
        experts = local_experts * ep_size
        capacity = (5 * tok * ep_size + 4 * experts - 1) // (4 * experts)
        window = -(-(capacity + 7) // 16) * 16
        pack = -(-local_experts * capacity // 16) * 16
        pack_buf = max(pack, (local_experts - 1) * capacity // 8 * 8 + window)
        bounds = [0] + [int(pack * f) // 32 * 32 for f in (0.13, 0.255, 0.45, 0.76)] + [pack]
        half = d_model // 2
        slots = local_experts * window
        n_half = half // WIDE
        r_rows = tok // ROW_BLOCKS
        sub_cols = half // SUBS
        dma = pltpu.SemaphoreType.DMA
        any_spec = pl.BlockSpec(memory_space=pl.ANY)
        vmem_spec = pl.BlockSpec(memory_space=pltpu.VMEM)
        per_ret = dma((SUBS, len(bounds) - 1))
        out = pl.pallas_call(
            functools.partial(moe_kernel, (experts, capacity, window, pack, bounds, local_experts, ep_size)),
            out_shape=jax.ShapeDtypeStruct((tok, d_model), BF16),
            in_specs=[any_spec] * 9 + [vmem_spec] * 2,
            out_specs=any_spec,
            scratch_shapes=[
                pltpu.VMEM((2, tok, d_model), BF16),
                pltpu.VMEM((2 * tok, d_model), BF16),
                pltpu.VMEM((tok, d_model), BF16),
                pltpu.VMEM((ep_size, 8, tok), jnp.int32),
                pltpu.VMEM((ep_size, 8, tok), F32),
                pltpu.VMEM((tok, LANES), F32),
                pltpu.VMEM((tok, LANES), F32),
                pltpu.VMEM((slots, d_model), BF16),
                pltpu.VMEM((n_half, tok, WIDE), F32),
                pltpu.VMEM((ROW_BLOCKS, n_half, r_rows, WIDE), F32),
                pltpu.VMEM((ROW_BLOCKS, n_half, r_rows, WIDE), F32),
                pltpu.VMEM((SUBS, pack_buf, sub_cols), F32),
                pltpu.VMEM((SUBS, pack_buf, sub_cols), F32),
                pltpu.VMEM((SUBS, pack, sub_cols), F32),
                pltpu.VMEM((SUBS, ep_size, pack, sub_cols), BF16),
                pltpu.VMEM((SUBS, tok, sub_cols), BF16),
                pltpu.VMEM((tok, half), BF16),
                pltpu.VMEM((experts, d_model), F32),
                dma((ROW_BLOCKS + 2,)), dma((3,)), dma((3,)), dma((1,)), dma((1,)), dma((X_CHUNKS,)), dma((X_CHUNKS,)), dma((X_CHUNKS,)), dma((X_CHUNKS,)),
                dma((ROW_BLOCKS, n_half)), dma((ROW_BLOCKS, n_half)), per_ret, per_ret, per_ret, per_ret, per_ret, per_ret, per_ret, per_ret,
                dma((SUBS,)), dma((SUBS,)), dma((SUBS,)),
            ],
            compiler_params=pltpu.CompilerParams(collective_id=0, has_side_effects=True, vmem_limit_bytes=67043328),
        )(normed, residual, w_router.T, ws_gate, ws_up, ws_down, jnp.swapaxes(we_gate, 1, 2), jnp.swapaxes(we_up, 1, 2), we_down,
          first_id.reshape(1, tok), alt_id.reshape(1, tok))
        return pl.pallas_call(
            copy_kernel,
            out_shape=jax.ShapeDtypeStruct((tok, d_model), BF16),
            in_specs=[any_spec],
            out_specs=any_spec,
            scratch_shapes=[pltpu.VMEM((tok, d_model), BF16), dma((COPY_CHUNKS,)), dma((COPY_CHUNKS,))],
        )(out)

    return jax.shard_map(device_step, mesh=mesh, in_specs=(tok_spec, tok_spec, P(None, None), P(None, 'tp'), P(None, 'tp'), P('tp', None), P('ep', None, 'tp'), P('ep', None, 'tp'), P('ep', 'tp', None), id_spec, id_spec), out_specs=tok_spec, check_vma=False)
```

```python
import functools

import jax
import jax.numpy as jnp
from jax import lax
from jax.experimental import pallas as pl
from jax.experimental.pallas import tpu as pltpu
from jax.sharding import PartitionSpec as P

MESH = pl.DeviceIdType.MESH
F32 = jnp.float32
BF16 = jnp.bfloat16
LANES = 128
RANK_BLOCK = 256
X_SPLIT = (0, 192, 384, 512)
X_CHUNKS = 3
WIDE = 512
COPY_CHUNKS = 4
ROW_BLOCKS = 2
COL = 256
SUBS = 2
EARLY_GROUPS = 3
SHARED_BUFS = 4


def dot(a, b):
    return jnp.dot(a, b, preferred_element_type=F32)


def dot_bt(a, b):
    return lax.dot_general(a, b, (((1,), (1,)), ((), ())), preferred_element_type=F32)


def dot_at(a, b):
    return lax.dot_general(a, b, (((0,), (0,)), ((), ())), preferred_element_type=F32)


def moe_kernel(dims, x_hbm, res_hbm, wr_hbm, wsg_hbm, wsu_hbm, wsd_hbm, weg_hbm, weu_hbm, wed_hbm, first_ref, alt_ref, o_hbm,
               x_near, x_far, x_sorted, ids_all, code_rows, code_col, gate_col, slot_x, sh_own, sh_send, sh_recv, ex_own, ex_send, ex_recv, ret, out_half, res_half, wr,
               ld_sem, id_send, id_recv, sib_send, sib_recv, xp_send, xp_recv, fw_send, fw_recv,
               ysh_send, ysh_recv, yex_send, yex_recv, rs_send, rs_recv, rx_send, rx_recv, rf_send, rf_recv, yo_send, yo_recv, lo_sem):
    experts, capacity, window, pack, bounds, local_experts, ep_size = dims
    groups = len(bounds) - 1
    last_expert = [-(-min(b, local_experts * capacity) // capacity) - 1 for b in bounds[1:]]
    tok, d_model = x_hbm.shape
    half = d_model // 2
    slots = local_experts * window
    spare = pack - local_experts * capacity
    ff_shared = wsg_hbm.shape[1]
    ff_expert = weg_hbm.shape[1]
    dp = lax.axis_index("dp")
    t = lax.axis_index("tp")
    me = lax.axis_index("ep")
    core = lax.rem(me, 2)
    sib = me + 1 - 2 * core
    xp = lax.rem(me + 2, ep_size)
    diag = lax.rem(sib + 2, ep_size)
    y_peer = (dp, 1 - t, me)
    sib_dev = (dp, t, sib)
    xp_dev = (dp, t, xp)
    diag_dev = (dp, t, diag)
    own_off = pl.multiple_of(t * half, half)
    peer_off = pl.multiple_of((1 - t) * half, half)
    x_cuts = [tok * v // X_SPLIT[-1] for v in X_SPLIT]
    r_rows = tok // ROW_BLOCKS
    n_wide, tail = ff_shared // WIDE, ff_shared % WIDE
    n_chunks = n_wide + (tail > 0)
    n_half = half // WIDE
    sub_cols = half // SUBS
    sub_blocks = sub_cols // WIDE
    sent = -(-local_experts * capacity // 8) * 8

    barrier = pltpu.get_barrier_semaphore()
    for dev in (y_peer, sib_dev, xp_dev, diag_dev):
        pl.semaphore_signal(barrier, inc=1, device_id=dev, device_id_type=MESH)

    def remote(src, dst, s_sem, r_sem, dev):
        return pltpu.make_async_remote_copy(src_ref=src, dst_ref=dst, send_sem=s_sem, recv_sem=r_sem, device_id=dev, device_id_type=MESH)

    id_copies = [remote(ids_all.at[me], ids_all.at[me], id_send.at[i], id_recv.at[i], dev) for i, dev in enumerate((sib_dev, xp_dev, diag_dev))]
    def far_rows(c, i):
        n = x_cuts[c + 1] - x_cuts[c]
        return pl.ds(2 * x_cuts[c] + i * n, n)

    xp_copies = [remote(x_sorted.at[pl.ds(x_cuts[c], x_cuts[c + 1] - x_cuts[c])], x_far.at[far_rows(c, 0)], xp_send.at[c], xp_recv.at[c], xp_dev) for c in range(X_CHUNKS)]
    sib_copy = remote(x_near.at[0], x_near.at[1], sib_send.at[0], sib_recv.at[0], sib_dev)
    fw_copies = [remote(x_far.at[far_rows(c, 0)], x_far.at[far_rows(c, 1)], fw_send.at[c], fw_recv.at[c], sib_dev) for c in range(X_CHUNKS)]
    own_x = [pltpu.make_async_copy(x_hbm.at[pl.ds(r * r_rows, r_rows)], x_near.at[0, pl.ds(r * r_rows, r_rows)], ld_sem.at[r]) for r in range(ROW_BLOCKS)]
    res_load = pltpu.make_async_copy(res_hbm.at[:, pl.ds(own_off, half)], res_half, ld_sem.at[ROW_BLOCKS])
    wr_load = pltpu.make_async_copy(wr_hbm, wr, ld_sem.at[ROW_BLOCKS + 1])

    cap = jnp.float32(capacity)

    def expert_base(ids):
        owner = sum((ids >= q * local_experts).astype(jnp.int32) for q in range(1, ep_size))
        return (ids * capacity + owner * spare).astype(F32)

    def route():
        for copy in id_copies:
            copy.wait()
        e_pad = -(-experts // 8) * 8
        e_iota = lax.broadcasted_iota(jnp.int32, (e_pad, RANK_BLOCK), 0)
        row_i = lax.broadcasted_iota(jnp.int32, (RANK_BLOCK, RANK_BLOCK), 0)
        col_i = lax.broadcasted_iota(jnp.int32, (RANK_BLOCK, RANK_BLOCK), 1)
        upper = (row_i <= col_i).astype(F32).astype(BF16)
        blocks = [(q, b * RANK_BLOCK) for q in range(ep_size) for b in range(tok // RANK_BLOCK)]
        total = jnp.zeros((e_pad, 1), F32)
        rank_first = []
        for q, lo in blocks:
            first = ids_all[q, 0:1, lo:lo + RANK_BLOCK]
            hot = (e_iota == first).astype(F32)
            cum = dot(hot.astype(BF16), upper) + total
            rank_first.append(jnp.sum(cum * hot, axis=0, keepdims=True) - 1.0)
            total = total + jnp.sum(hot, axis=1, keepdims=True)
        load = jnp.minimum(total, cap)
        room = cap - load
        total = jnp.zeros((e_pad, 1), F32)
        for i, (q, lo) in enumerate(blocks):
            first = ids_all[q, 0:1, lo:lo + RANK_BLOCK]
            alt = ids_all[q, 1:2, lo:lo + RANK_BLOCK]
            kept = rank_first[i] < cap
            over = jnp.where(kept, 0.0, 1.0)
            hot = (e_iota == alt).astype(F32) * over
            cum = dot(hot.astype(BF16), upper) + total
            rank_alt = jnp.sum(cum * hot, axis=0, keepdims=True) - 1.0
            total = total + jnp.sum(hot, axis=1, keepdims=True)
            room_tok = jnp.sum(hot * room, axis=0, keepdims=True)
            load_tok = jnp.sum(hot * load, axis=0, keepdims=True)
            code_first = expert_base(first) + rank_first[i]
            code_alt = jnp.where(rank_alt < room_tok, expert_base(alt) + load_tok + rank_alt, -1.0)
            code = jnp.where(kept, code_first, code_alt)
            code_rows[q, :, lo:lo + RANK_BLOCK] = jnp.broadcast_to(code, (8, RANK_BLOCK))

    def sort_block(q):
        code_t = jnp.broadcast_to(code_rows[q][0:1, :], (LANES, tok)).T[:, 0:1]
        shift = ((1 - lax.div(q, 2)) * (2 * pack)).astype(F32)

        def key_of(code):
            rel = code - shift
            local = jnp.where(rel >= pack, rel - pack, rel)
            return jnp.where((rel >= 0.0) & (rel < 2.0 * pack), local, 8192.0)

        key_t = key_of(code_t)
        key = key_of(code_rows[q][0:1, :])
        lane = lax.broadcasted_iota(jnp.int32, (tok, tok), 1)
        line = lax.broadcasted_iota(jnp.int32, (tok, tok), 0)
        ahead = (key < key_t) | ((key == key_t) & (lane < line))
        position = jnp.sum(jnp.where(ahead, 1.0, 0.0), axis=1, keepdims=True)
        return position == lane.astype(F32), code_t

    def dispatch():
        route()
        hit, _ = sort_block(me)
        order = hit.astype(F32).astype(BF16)
        for lo in range(0, d_model, WIDE):
            x_sorted[:, lo:lo + WIDE] = dot_at(order, x_near[0, :, lo:lo + WIDE]).astype(BF16)
        xp_copies[0].start()

    def ysh_copy(r, j):
        if r == 0:
            return remote(sh_send.at[r, j], sh_recv.at[r, j], ysh_send.at[r, j], ysh_recv.at[r, j], y_peer)
        return remote(sh_send.at[r], sh_recv.at[r], ysh_send.at[r, 0], ysh_recv.at[r, 0], y_peer)

    def shared_phase(act, wg, wu, wd, g_sem, u_sem, d_sem):
        def weight_copies(c, slot, width):
            cols = pl.ds(pl.multiple_of(c * WIDE, WIDE), width)
            dst = pl.ds(0, width)
            return (pltpu.make_async_copy(wsg_hbm.at[:, cols], wg.at[slot, :, dst], g_sem.at[slot]),
                    pltpu.make_async_copy(wsu_hbm.at[:, cols], wu.at[slot, :, dst], u_sem.at[slot]))

        def start_weights(k, slot):
            c = lax.rem(k, n_chunks)

            @pl.when(c < n_wide)
            def _():
                for copy in weight_copies(c, slot, WIDE):
                    copy.start()

            if tail:
                @pl.when(c == n_wide)
                def _():
                    for copy in weight_copies(c, slot, tail):
                        copy.start()

        def down_copy(k, slot):
            j = lax.rem(k, 2 * n_half)
            col = jnp.where(j < n_half, peer_off + j * WIDE, own_off + (j - n_half) * WIDE)
            return pltpu.make_async_copy(wsd_hbm.at[:, pl.ds(pl.multiple_of(col, WIDE), WIDE)], wd.at[slot], d_sem.at[slot])

        own_x[0].start()
        start_weights(jnp.int32(0), 0)
        for copy in own_x[1:]:
            copy.start()
        for slot in range(1, SHARED_BUFS):
            start_weights(jnp.int32(slot), slot)
        ids_all[pl.ds(me, 1), 0:1, :] = first_ref[...].reshape(1, 1, tok)
        ids_all[pl.ds(me, 1), 1:2, :] = alt_ref[...].reshape(1, 1, tok)
        def exchange():
            for copy in own_x[1:]:
                copy.wait()
            pl.semaphore_wait(barrier, 4)
            for copy in id_copies:
                copy.start()
            sib_copy.start()

        for r in range(ROW_BLOCKS):
            if r == 0:
                own_x[0].wait()
            def gateup(c, width):
                k = c + r * n_chunks
                slot = lax.rem(k, SHARED_BUFS)
                for copy in weight_copies(c, slot, width):
                    copy.wait()
                x = x_near[0, r * r_rows:(r + 1) * r_rows, :]
                for lo in range(0, width, COL):
                    g = dot(x, wg[slot, :, lo:lo + COL])
                    u = dot(x, wu[slot, :, lo:lo + COL])
                    act[:, pl.ds(pl.multiple_of(c * WIDE + lo, COL), COL)] = (jax.nn.silu(g) * u).astype(BF16)

                @pl.when(k + SHARED_BUFS < ROW_BLOCKS * n_chunks)
                def _():
                    start_weights(k + SHARED_BUFS, slot)

            with jax.named_scope(f"gateup{r}"):
                @pl.loop(0, n_wide)
                def _(c):
                    gateup(c, WIDE)

                    if r == 0:
                        @pl.when(c == 0)
                        def _():
                            exchange()

                    if r == 0:
                        @pl.when((c == 1) | (c == 3))
                        def _():
                            slot = lax.div(c, 2)
                            down_copy(slot, slot).start()

                if tail:
                    gateup(jnp.int32(n_wide), tail)

            def down(j, base, store):
                k = j + r * 2 * n_half + base
                slot = lax.rem(k, 2)
                down_copy(k, slot).wait()
                store(dot(act[...], wd[slot]))

                @pl.when(k + 2 < ROW_BLOCKS * 2 * n_half)
                def _():
                    down_copy(k + 2, slot).start()

            with jax.named_scope(f"downpeer{r}"):
                @pl.loop(0, n_half)
                def _(j):
                    def store(value):
                        sh_send[r, j] = value
                        if r == 0:
                            ysh_copy(r, j).start()

                    down(j, 0, store)

                if r > 0:
                    ysh_copy(r, 0).start()

            if r == 0:
                wr_load.start()
                with jax.named_scope("dispatch"):
                    dispatch()
            with jax.named_scope(f"downown{r}"):
                @pl.loop(0, n_half)
                def _(j):
                    def store(value):
                        sh_own[j, r * r_rows:(r + 1) * r_rows, :] = value

                    down(j, n_half, store)

    shared_sems = [pltpu.SemaphoreType.DMA((SHARED_BUFS,))] * 3
    pl.run_scoped(shared_phase, pltpu.VMEM((r_rows, ff_shared), BF16), pltpu.VMEM((SHARED_BUFS, d_model, WIDE), BF16), pltpu.VMEM((SHARED_BUFS, d_model, WIDE), BF16),
                  pltpu.VMEM((2, ff_shared, WIDE), BF16), *shared_sems)

    def yex_copy(sub, i):
        rows = pl.ds(bounds[i], min(bounds[i + 1], sent) - bounds[i])
        return remote(ex_send.at[sub, rows], ex_recv.at[sub, rows], yex_send.at[sub, i], yex_recv.at[sub, i], y_peer)

    def ret_copy(sub, i, who, s_sem, r_sem, dev):
        ref = ret.at[sub, who, pl.ds(bounds[i], bounds[i + 1] - bounds[i])]
        return remote(ref, ref, s_sem.at[sub, i], r_sem.at[sub, i], dev)

    def give(sub, i):
        yex_copy(sub, i).wait()
        rows = slice(bounds[i], bounds[i + 1])
        ret[sub, pl.ds(me, 1), rows, :] = (ex_own[sub, rows, :] + ex_recv[sub, rows, :]).astype(BF16).reshape(1, bounds[i + 1] - bounds[i], sub_cols)
        ret_copy(sub, i, me, rx_send, rx_recv, xp_dev).start()
        ret_copy(sub, i, me, rs_send, rs_recv, sib_dev).start()

    def forward(sub, i):
        ret_copy(sub, i, me, rx_send, rx_recv, xp_dev).wait()
        ret_copy(sub, i, xp, rf_send, rf_recv, sib_dev).start()

    def routed_phase(sel_near, sel_far, wg, wu, wd, g_sem, u_sem, d_sem):
        def gate_copy(e, slot):
            return pltpu.make_async_copy(weg_hbm.at[e], wg.at[slot], g_sem.at[slot])

        def up_copy(e, slot):
            return pltpu.make_async_copy(weu_hbm.at[e], wu.at[slot], u_sem.at[slot])

        def down_copy(e, slot):
            return pltpu.make_async_copy(wed_hbm.at[e], wd.at[slot], d_sem.at[slot])

        for slot in range(2):
            gate_copy(slot, slot).start()
            up_copy(slot, slot).start()
            down_copy(slot, slot).start()

        res_load.start()
        xp_copies[1].start()
        with jax.named_scope("routing"):
            pos = lax.broadcasted_iota(jnp.int32, (slots, LANES), 0)
            slot_expert = sum((pos >= e * window).astype(jnp.int32) for e in range(1, local_experts))
            first_row = slot_expert * capacity
            row = (first_row // 8) * 8 + (pos - slot_expert * window)
            slot_code = jnp.where((row >= first_row) & (row < first_row + capacity), row + me * pack, -2).astype(F32)
            def pick_rows(codes):
                return (jnp.broadcast_to(slot_code[:, 0:1], (slots, codes.shape[1])) == codes).astype(F32).astype(BF16)

            for i, q in enumerate((me, sib)):
                codes = code_rows[q]
                for lo in range(0, tok, LANES):
                    sel_near[:, i * tok + lo:i * tok + lo + LANES] = pick_rows(codes[0:1, lo:lo + LANES])
            def sorted_codes(q):
                hit, code_t = sort_block(q)
                return jnp.sum(jnp.where(hit, code_t, 0.0), axis=0, keepdims=True)

            codes_xp, codes_diag = sorted_codes(xp), sorted_codes(diag)
            for c in range(X_CHUNKS):
                both = jnp.concatenate([codes_xp[:, x_cuts[c]:x_cuts[c + 1]], codes_diag[:, x_cuts[c]:x_cuts[c + 1]]], axis=1)
                for lo in range(0, 2 * (x_cuts[c + 1] - x_cuts[c]), LANES):
                    dst = 2 * x_cuts[c] + lo
                    sel_far[:, dst:dst + LANES] = pick_rows(both[:, lo:lo + LANES])

            code_t = jnp.broadcast_to(code_rows[me][0:1, :], (LANES, tok)).T
            code_col[...] = code_t

        with jax.named_scope("router"):
            wr_load.wait()
            x = x_near[0]
            w = wr[...]
            w_hi = w.astype(BF16)
            w_rest = w - w_hi.astype(F32)
            w_mid = w_rest.astype(BF16)
            w_lo = (w_rest - w_mid.astype(F32)).astype(BF16)
            logits = dot_bt(x, w_hi) + (dot_bt(x, w_mid) + dot_bt(x, w_lo))
            top = jnp.max(logits, axis=1, keepdims=True)
            prob = jnp.exp(logits - top)
            denom = jnp.sum(prob, axis=1, keepdims=True)
            lane_lo = expert_base(lax.broadcasted_iota(jnp.int32, (tok, experts), 1))
            code_e = code_t[:, 0:experts]
            picked = (code_e >= lane_lo) & (code_e < lane_lo + cap)
            gate = jnp.sum(jnp.where(picked, prob, 0.0), axis=1, keepdims=True) / denom
            gate_col[...] = jnp.broadcast_to(gate, (tok, LANES))

        nc = 512
        with jax.named_scope("near"):
            sib_copy.wait()

            @pl.loop(0, d_model // nc)
            def _(n):
                cols = pl.ds(pl.multiple_of(n * nc, nc), nc)
                slot_x[:, cols] = dot(sel_near[...], x_near[:, :, cols].reshape(2 * tok, nc)).astype(BF16)

        def far(c):
            if 0 < c < X_CHUNKS - 1:
                xp_copies[c].wait_send()
                xp_copies[c + 1].start()
            xp_copies[c].wait_recv()
            fw_copies[c].start()
            fw_copies[c].wait_recv()

            @pl.loop(0, d_model // nc)
            def _(n):
                cols = pl.ds(pl.multiple_of(n * nc, nc), nc)
                span = slice(2 * x_cuts[c], 2 * x_cuts[c + 1])
                slot_x[:, cols] += dot(sel_far[:, span], x_far[span, cols]).astype(BF16)

        loop_steps = [(5, give, 0, 0), (6, give, 1, 0), (7, give, 0, 1), (8, forward, 0, 0), (8, give, 1, 1), (9, forward, 1, 0), (10, forward, 0, 1), (11, forward, 1, 1), (12, give, 0, 2)]
        far_at = [x_cuts[c] // (2 * capacity) for c in range(X_CHUNKS)]
        if sent < pack:
            for sub in range(SUBS):
                ex_recv[sub, sent:pack, :] = jnp.zeros((pack - sent, sub_cols), F32)

        with jax.named_scope("experts"):
            for sub in range(SUBS):
                ex_send[sub, 0:8, :] = jnp.zeros((8, sub_cols), F32)
                ex_own[sub, 0:8, :] = jnp.zeros((8, sub_cols), F32)

            @pl.loop(0, local_experts)
            def _(e):
                slot = lax.rem(e, 2)
                for c in range(X_CHUNKS):
                    @pl.when(e == far_at[c])
                    def _():
                        with jax.named_scope(f"far{c}"):
                            far(c)

                gate_copy(e, slot).wait()
                up_copy(e, slot).wait()
                rows = slot_x[pl.ds(pl.multiple_of(e * window, window), window), :]
                g = dot_bt(wg[slot], rows)
                u = dot_bt(wu[slot], rows)
                hidden = (jax.nn.silu(g) * u).astype(BF16)

                @pl.when(e + 2 < local_experts)
                def _():
                    gate_copy(e + 2, slot).start()
                    up_copy(e + 2, slot).start()

                down_copy(e, slot).wait()
                row = pl.multiple_of((e * capacity) // 8 * 8, 8)
                for buf, off in ((ex_send, peer_off), (ex_own, own_off)):
                    value = dot_at(hidden, wd[slot, :, pl.ds(off, half)])
                    for sub in range(SUBS):
                        part = value[:, sub * sub_cols:(sub + 1) * sub_cols]
                        buf[sub, pl.ds(row, 8), :] += part[0:8]
                        buf[sub, pl.ds(row + 8, window - 8), :] = part[8:]

                @pl.when(e + 2 < local_experts)
                def _():
                    down_copy(e + 2, slot).start()

                for i in range(groups):
                    @pl.when(e == last_expert[i])
                    def _():
                        yex_copy(0, i).start()
                        if i < EARLY_GROUPS:
                            yex_copy(1, i).start()

                for when, action, sub, i in loop_steps:
                    @pl.when(e == when)
                    def _():
                        action(sub, i)

            for i in range(EARLY_GROUPS, groups):
                yex_copy(1, i).start()

    pl.run_scoped(routed_phase, pltpu.VMEM((slots, 2 * tok), BF16), pltpu.VMEM((slots, 2 * tok), BF16),
                  pltpu.VMEM((2, ff_expert, d_model), BF16), pltpu.VMEM((2, ff_expert, d_model), BF16),
                  pltpu.VMEM((2, ff_expert, d_model), BF16), pltpu.SemaphoreType.DMA((2,)), pltpu.SemaphoreType.DMA((2,)), pltpu.SemaphoreType.DMA((2,)))

    with jax.named_scope("fin_shared"):
        for copy in xp_copies[:1] + xp_copies[-1:] + fw_copies:
            copy.wait_send()
        res_load.wait()
        for r in range(ROW_BLOCKS):
            if r > 0:
                ysh_copy(r, 0).wait()

            @pl.loop(0, n_half)
            def _(j):
                if r == 0:
                    ysh_copy(r, j).wait()
                cols = pl.ds(pl.multiple_of(j * WIDE, WIDE), WIDE)
                rows = slice(r * r_rows, (r + 1) * r_rows)
                sh_own[j, rows, :] = res_half[rows, cols].astype(F32) + (sh_own[j, rows, :] + sh_recv[r, j])

    def combine(pick, sub, i):
        n = bounds[i + 1] - bounds[i]
        lanes = slice(ep_size * bounds[i], ep_size * bounds[i + 1])
        if sub == 0:
            lane = lax.broadcasted_iota(jnp.int32, (tok, ep_size * n), 1)
            owner = sum((lane >= q * n).astype(jnp.int32) for q in range(1, ep_size))
            lane_code = (lane + owner * (pack - n) + bounds[i]).astype(F32)
            pick[:, lanes] = (code_col[:, 0:1] == lane_code).astype(F32).astype(BF16)
        ret_copy(sub, i, me, rs_send, rs_recv, sib_dev).wait()
        ret_copy(sub, i, xp, rf_send, rf_recv, sib_dev).wait()
        rows = ret[sub, :, bounds[i]:bounds[i + 1], :].reshape(ep_size * n, sub_cols)
        gate = gate_col[:, 0:1]
        for j in range(sub_blocks):
            jj = sub * sub_blocks + j
            sh_own[jj] = sh_own[jj] + gate * dot(pick[:, lanes], rows[:, j * WIDE:(j + 1) * WIDE])

    def out_copies(sub):
        src = out_half.at[sub]
        dst = o_hbm.at[:, pl.ds(pl.multiple_of(own_off + sub * sub_cols, sub_cols), sub_cols)]
        return remote(src, dst, yo_send.at[sub], yo_recv.at[sub], y_peer), pltpu.make_async_copy(src, dst, lo_sem.at[sub])

    def emit(sub):
        for j in range(sub_blocks):
            out_half[sub, :, j * WIDE:(j + 1) * WIDE] = sh_own[sub * sub_blocks + j].astype(BF16)

    def start_out(sub):
        for copy in out_copies(sub):
            copy.start()

    def return_phase(pick):
        steps = [(give, 1, 2), (forward, 0, 2), (combine, 0, 0), (combine, 1, 0), (combine, 0, 1), (combine, 1, 1), (give, 0, 3), (forward, 1, 2), (combine, 0, 2),
                 (forward, 0, 3), (combine, 1, 2), (give, 0, 4), (combine, 0, 3), (forward, 0, 4), (combine, 0, 4), (emit, 0), (start_out, 0),
                 (give, 1, 3), (forward, 1, 3), (give, 1, 4), (combine, 1, 3), (forward, 1, 4), (combine, 1, 4), (emit, 1), (start_out, 1)]
        for step in steps:
            with jax.named_scope(step[0].__name__ + "".join(str(a) for a in step[1:])):
                if step[0] is combine:
                    combine(pick, *step[1:])
                else:
                    step[0](*step[1:])

    pl.run_scoped(return_phase, pltpu.VMEM((tok, ep_size * pack), BF16))

    with jax.named_scope("out"):
        for sub in range(SUBS):
            for copy in out_copies(sub):
                copy.wait()


def copy_kernel(src, dst, buf, in_sem, out_sem):
    n = src.shape[0] // COPY_CHUNKS
    reads = [pltpu.make_async_copy(src.at[pl.ds(c * n, n)], buf.at[pl.ds(c * n, n)], in_sem.at[c]) for c in range(COPY_CHUNKS)]
    writes = [pltpu.make_async_copy(buf.at[pl.ds(c * n, n)], dst.at[pl.ds(c * n, n)], out_sem.at[c]) for c in range(COPY_CHUNKS)]
    for copy in reads:
        copy.start()
    for read, write in zip(reads, writes):
        read.wait()
        write.start()
    for copy in writes:
        copy.wait()


def solution(mesh):
    ep_size = mesh.shape["ep"]
    tok_spec = P(("dp", "ep"), None)
    id_spec = P(("dp", "ep"))

    def device_step(normed, residual, w_router, ws_gate, ws_up, ws_down, we_gate, we_up, we_down, first_id, alt_id):
        tok, d_model = normed.shape
        local_experts, _, ff_expert = we_gate.shape
        experts = local_experts * ep_size
        capacity = (5 * tok * ep_size + 4 * experts - 1) // (4 * experts)
        window = -(-(capacity + 7) // 16) * 16
        pack = -(-local_experts * capacity // 16) * 16
        pack_buf = max(pack, (local_experts - 1) * capacity // 8 * 8 + window)
        bounds = [0] + [int(pack * f) // 32 * 32 for f in (0.13, 0.255, 0.45, 0.76)] + [pack]
        half = d_model // 2
        slots = local_experts * window
        n_half = half // WIDE
        r_rows = tok // ROW_BLOCKS
        sub_cols = half // SUBS
        dma = pltpu.SemaphoreType.DMA
        any_spec = pl.BlockSpec(memory_space=pl.ANY)
        vmem_spec = pl.BlockSpec(memory_space=pltpu.VMEM)
        per_ret = dma((SUBS, len(bounds) - 1))
        out = pl.pallas_call(
            functools.partial(moe_kernel, (experts, capacity, window, pack, bounds, local_experts, ep_size)),
            out_shape=jax.ShapeDtypeStruct((tok, d_model), BF16),
            in_specs=[any_spec] * 9 + [vmem_spec] * 2,
            out_specs=any_spec,
            scratch_shapes=[
                pltpu.VMEM((2, tok, d_model), BF16),
                pltpu.VMEM((2 * tok, d_model), BF16),
                pltpu.VMEM((tok, d_model), BF16),
                pltpu.VMEM((ep_size, 8, tok), jnp.int32),
                pltpu.VMEM((ep_size, 8, tok), F32),
                pltpu.VMEM((tok, LANES), F32),
                pltpu.VMEM((tok, LANES), F32),
                pltpu.VMEM((slots, d_model), BF16),
                pltpu.VMEM((n_half, tok, WIDE), F32),
                pltpu.VMEM((ROW_BLOCKS, n_half, r_rows, WIDE), F32),
                pltpu.VMEM((ROW_BLOCKS, n_half, r_rows, WIDE), F32),
                pltpu.VMEM((SUBS, pack_buf, sub_cols), F32),
                pltpu.VMEM((SUBS, pack_buf, sub_cols), F32),
                pltpu.VMEM((SUBS, pack, sub_cols), F32),
                pltpu.VMEM((SUBS, ep_size, pack, sub_cols), BF16),
                pltpu.VMEM((SUBS, tok, sub_cols), BF16),
                pltpu.VMEM((tok, half), BF16),
                pltpu.VMEM((experts, d_model), F32),
                dma((ROW_BLOCKS + 2,)), dma((3,)), dma((3,)), dma((1,)), dma((1,)), dma((X_CHUNKS,)), dma((X_CHUNKS,)), dma((X_CHUNKS,)), dma((X_CHUNKS,)),
                dma((ROW_BLOCKS, n_half)), dma((ROW_BLOCKS, n_half)), per_ret, per_ret, per_ret, per_ret, per_ret, per_ret, per_ret, per_ret,
                dma((SUBS,)), dma((SUBS,)), dma((SUBS,)),
            ],
            compiler_params=pltpu.CompilerParams(collective_id=0, has_side_effects=True, vmem_limit_bytes=67043328),
        )(normed, residual, w_router.T, ws_gate, ws_up, ws_down, jnp.swapaxes(we_gate, 1, 2), jnp.swapaxes(we_up, 1, 2), we_down,
          first_id.reshape(1, tok), alt_id.reshape(1, tok))
        return pl.pallas_call(
            copy_kernel,
            out_shape=jax.ShapeDtypeStruct((tok, d_model), BF16),
            in_specs=[any_spec],
            out_specs=any_spec,
            scratch_shapes=[pltpu.VMEM((tok, d_model), BF16), dma((COPY_CHUNKS,)), dma((COPY_CHUNKS,))],
        )(out)

    return jax.shard_map(device_step, mesh=mesh, in_specs=(tok_spec, tok_spec, P(None, None), P(None, 'tp'), P(None, 'tp'), P('tp', None), P('ep', None, 'tp'), P('ep', None, 'tp'), P('ep', 'tp', None), id_spec, id_spec), out_specs=tok_spec, check_vma=False)
```

```python
import functools

import jax
import jax.numpy as jnp
from jax import lax
from jax.experimental import pallas as pl
from jax.experimental.pallas import tpu as pltpu
from jax.sharding import PartitionSpec as P

MESH = pl.DeviceIdType.MESH
F32 = jnp.float32
BF16 = jnp.bfloat16
LANES = 128
RANK_BLOCK = 256
X_SPLIT = (0, 192, 320, 448, 512)
X_CHUNKS = 4
WIDE = 512
COPY_CHUNKS = 4
ROW_BLOCKS = 2
COL = 256
SUBS = 2
EARLY_GROUPS = 3
SHARED_BUFS = 4


def dot(a, b):
    return jnp.dot(a, b, preferred_element_type=F32)


def dot_bt(a, b):
    return lax.dot_general(a, b, (((1,), (1,)), ((), ())), preferred_element_type=F32)


def dot_at(a, b):
    return lax.dot_general(a, b, (((0,), (0,)), ((), ())), preferred_element_type=F32)


def moe_kernel(dims, x_hbm, res_hbm, wr_hbm, wsg_hbm, wsu_hbm, wsd_hbm, weg_hbm, weu_hbm, wed_hbm, first_ref, alt_ref, o_hbm,
               x_near, x_far, x_sorted, ids_all, code_rows, code_col, gate_col, slot_x, sh_own, sh_send, sh_recv, ex_own, ex_send, ex_recv, ret, out_half, res_half, wr,
               ld_sem, id_send, id_recv, sib_send, sib_recv, xp_send, xp_recv, fw_send, fw_recv,
               ysh_send, ysh_recv, yex_send, yex_recv, rs_send, rs_recv, rx_send, rx_recv, rf_send, rf_recv, yo_send, yo_recv, lo_sem):
    experts, capacity, window, pack, bounds, local_experts, ep_size = dims
    groups = len(bounds) - 1
    last_expert = [-(-min(b, local_experts * capacity) // capacity) - 1 for b in bounds[1:]]
    tok, d_model = x_hbm.shape
    half = d_model // 2
    slots = local_experts * window
    spare = pack - local_experts * capacity
    ff_shared = wsg_hbm.shape[1]
    ff_expert = weg_hbm.shape[1]
    dp = lax.axis_index("dp")
    t = lax.axis_index("tp")
    me = lax.axis_index("ep")
    core = lax.rem(me, 2)
    sib = me + 1 - 2 * core
    xp = lax.rem(me + 2, ep_size)
    diag = lax.rem(sib + 2, ep_size)
    y_peer = (dp, 1 - t, me)
    sib_dev = (dp, t, sib)
    xp_dev = (dp, t, xp)
    diag_dev = (dp, t, diag)
    own_off = pl.multiple_of(t * half, half)
    peer_off = pl.multiple_of((1 - t) * half, half)
    x_cuts = [tok * v // X_SPLIT[-1] for v in X_SPLIT]
    r_rows = tok // ROW_BLOCKS
    n_wide, tail = ff_shared // WIDE, ff_shared % WIDE
    n_chunks = n_wide + (tail > 0)
    n_half = half // WIDE
    sub_cols = half // SUBS
    sub_blocks = sub_cols // WIDE
    sent = -(-local_experts * capacity // 8) * 8

    barrier = pltpu.get_barrier_semaphore()
    for dev in (y_peer, sib_dev, xp_dev, diag_dev):
        pl.semaphore_signal(barrier, inc=1, device_id=dev, device_id_type=MESH)

    def remote(src, dst, s_sem, r_sem, dev):
        return pltpu.make_async_remote_copy(src_ref=src, dst_ref=dst, send_sem=s_sem, recv_sem=r_sem, device_id=dev, device_id_type=MESH)

    id_copies = [remote(ids_all.at[me], ids_all.at[me], id_send.at[i], id_recv.at[i], dev) for i, dev in enumerate((sib_dev, xp_dev, diag_dev))]
    def far_rows(c, i):
        n = x_cuts[c + 1] - x_cuts[c]
        return pl.ds(2 * x_cuts[c] + i * n, n)

    xp_copies = [remote(x_sorted.at[pl.ds(x_cuts[c], x_cuts[c + 1] - x_cuts[c])], x_far.at[far_rows(c, 0)], xp_send.at[c], xp_recv.at[c], xp_dev) for c in range(X_CHUNKS)]
    sib_copy = remote(x_near.at[0], x_near.at[1], sib_send.at[0], sib_recv.at[0], sib_dev)
    fw_copies = [remote(x_far.at[far_rows(c, 0)], x_far.at[far_rows(c, 1)], fw_send.at[c], fw_recv.at[c], sib_dev) for c in range(X_CHUNKS)]
    own_x = [pltpu.make_async_copy(x_hbm.at[pl.ds(r * r_rows, r_rows)], x_near.at[0, pl.ds(r * r_rows, r_rows)], ld_sem.at[r]) for r in range(ROW_BLOCKS)]
    res_load = pltpu.make_async_copy(res_hbm.at[:, pl.ds(own_off, half)], res_half, ld_sem.at[ROW_BLOCKS])
    wr_load = pltpu.make_async_copy(wr_hbm, wr, ld_sem.at[ROW_BLOCKS + 1])

    cap = jnp.float32(capacity)

    def expert_base(ids):
        owner = sum((ids >= q * local_experts).astype(jnp.int32) for q in range(1, ep_size))
        return (ids * capacity + owner * spare).astype(F32)

    def route():
        for copy in id_copies:
            copy.wait()
        e_pad = -(-experts // 8) * 8
        e_iota = lax.broadcasted_iota(jnp.int32, (e_pad, RANK_BLOCK), 0)
        row_i = lax.broadcasted_iota(jnp.int32, (RANK_BLOCK, RANK_BLOCK), 0)
        col_i = lax.broadcasted_iota(jnp.int32, (RANK_BLOCK, RANK_BLOCK), 1)
        upper = (row_i <= col_i).astype(F32).astype(BF16)
        blocks = [(q, b * RANK_BLOCK) for q in range(ep_size) for b in range(tok // RANK_BLOCK)]
        total = jnp.zeros((e_pad, 1), F32)
        rank_first = []
        for q, lo in blocks:
            first = ids_all[q, 0:1, lo:lo + RANK_BLOCK]
            hot = (e_iota == first).astype(F32)
            cum = dot(hot.astype(BF16), upper) + total
            rank_first.append(jnp.sum(cum * hot, axis=0, keepdims=True) - 1.0)
            total = total + jnp.sum(hot, axis=1, keepdims=True)
        load = jnp.minimum(total, cap)
        room = cap - load
        total = jnp.zeros((e_pad, 1), F32)
        for i, (q, lo) in enumerate(blocks):
            first = ids_all[q, 0:1, lo:lo + RANK_BLOCK]
            alt = ids_all[q, 1:2, lo:lo + RANK_BLOCK]
            kept = rank_first[i] < cap
            over = jnp.where(kept, 0.0, 1.0)
            hot = (e_iota == alt).astype(F32) * over
            cum = dot(hot.astype(BF16), upper) + total
            rank_alt = jnp.sum(cum * hot, axis=0, keepdims=True) - 1.0
            total = total + jnp.sum(hot, axis=1, keepdims=True)
            room_tok = jnp.sum(hot * room, axis=0, keepdims=True)
            load_tok = jnp.sum(hot * load, axis=0, keepdims=True)
            code_first = expert_base(first) + rank_first[i]
            code_alt = jnp.where(rank_alt < room_tok, expert_base(alt) + load_tok + rank_alt, -1.0)
            code = jnp.where(kept, code_first, code_alt)
            code_rows[q, :, lo:lo + RANK_BLOCK] = jnp.broadcast_to(code, (8, RANK_BLOCK))

    def sort_block(q):
        code_t = jnp.broadcast_to(code_rows[q][0:1, :], (LANES, tok)).T[:, 0:1]
        shift = ((1 - lax.div(q, 2)) * (2 * pack)).astype(F32)

        def key_of(code):
            rel = code - shift
            local = jnp.where(rel >= pack, rel - pack, rel)
            return jnp.where((rel >= 0.0) & (rel < 2.0 * pack), local, 8192.0)

        key_t = key_of(code_t)
        key = key_of(code_rows[q][0:1, :])
        lane = lax.broadcasted_iota(jnp.int32, (tok, tok), 1)
        line = lax.broadcasted_iota(jnp.int32, (tok, tok), 0)
        ahead = (key < key_t) | ((key == key_t) & (lane < line))
        position = jnp.sum(jnp.where(ahead, 1.0, 0.0), axis=1, keepdims=True)
        return position == lane.astype(F32), code_t

    def dispatch():
        route()
        hit, _ = sort_block(me)
        order = hit.astype(F32).astype(BF16)
        for lo in range(0, d_model, WIDE):
            x_sorted[:, lo:lo + WIDE] = dot_at(order, x_near[0, :, lo:lo + WIDE]).astype(BF16)
        xp_copies[0].start()

    def ysh_copy(r, j):
        if r == 0:
            return remote(sh_send.at[r, j], sh_recv.at[r, j], ysh_send.at[r, j], ysh_recv.at[r, j], y_peer)
        return remote(sh_send.at[r], sh_recv.at[r], ysh_send.at[r, 0], ysh_recv.at[r, 0], y_peer)

    def shared_phase(act, wg, wu, wd, g_sem, u_sem, d_sem):
        def weight_copies(c, slot, width):
            cols = pl.ds(pl.multiple_of(c * WIDE, WIDE), width)
            dst = pl.ds(0, width)
            return (pltpu.make_async_copy(wsg_hbm.at[:, cols], wg.at[slot, :, dst], g_sem.at[slot]),
                    pltpu.make_async_copy(wsu_hbm.at[:, cols], wu.at[slot, :, dst], u_sem.at[slot]))

        def start_weights(k, slot):
            c = lax.rem(k, n_chunks)

            @pl.when(c < n_wide)
            def _():
                for copy in weight_copies(c, slot, WIDE):
                    copy.start()

            if tail:
                @pl.when(c == n_wide)
                def _():
                    for copy in weight_copies(c, slot, tail):
                        copy.start()

        def down_copy(k, slot):
            j = lax.rem(k, 2 * n_half)
            col = jnp.where(j < n_half, peer_off + j * WIDE, own_off + (j - n_half) * WIDE)
            return pltpu.make_async_copy(wsd_hbm.at[:, pl.ds(pl.multiple_of(col, WIDE), WIDE)], wd.at[slot], d_sem.at[slot])

        own_x[0].start()
        start_weights(jnp.int32(0), 0)
        for copy in own_x[1:]:
            copy.start()
        for slot in range(1, SHARED_BUFS):
            start_weights(jnp.int32(slot), slot)
        ids_all[pl.ds(me, 1), 0:1, :] = first_ref[...].reshape(1, 1, tok)
        ids_all[pl.ds(me, 1), 1:2, :] = alt_ref[...].reshape(1, 1, tok)
        def exchange():
            for copy in own_x[1:]:
                copy.wait()
            pl.semaphore_wait(barrier, 4)
            for copy in id_copies:
                copy.start()
            sib_copy.start()

        for r in range(ROW_BLOCKS):
            if r == 0:
                own_x[0].wait()
            def gateup(c, width):
                k = c + r * n_chunks
                slot = lax.rem(k, SHARED_BUFS)
                for copy in weight_copies(c, slot, width):
                    copy.wait()
                x = x_near[0, r * r_rows:(r + 1) * r_rows, :]
                for lo in range(0, width, COL):
                    g = dot(x, wg[slot, :, lo:lo + COL])
                    u = dot(x, wu[slot, :, lo:lo + COL])
                    act[:, pl.ds(pl.multiple_of(c * WIDE + lo, COL), COL)] = (jax.nn.silu(g) * u).astype(BF16)

                @pl.when(k + SHARED_BUFS < (r + 1) * n_chunks)
                def _():
                    start_weights(k + SHARED_BUFS, slot)

            with jax.named_scope(f"gateup{r}"):
                @pl.loop(0, n_wide)
                def _(c):
                    gateup(c, WIDE)

                    if r == 0:
                        @pl.when(c == 0)
                        def _():
                            exchange()

                    if r == 0:
                        @pl.when((c == 1) | (c == 3))
                        def _():
                            slot = lax.div(c, 2)
                            down_copy(slot, slot).start()

                if tail:
                    gateup(jnp.int32(n_wide), tail)

            if r + 1 < ROW_BLOCKS:
                for i in range(SHARED_BUFS):
                    k = (r + 1) * n_chunks + i
                    start_weights(jnp.int32(k), k % SHARED_BUFS)

            def down(j, base, store):
                k = j + r * 2 * n_half + base
                slot = lax.rem(k, 2)
                down_copy(k, slot).wait()
                store(dot(act[...], wd[slot]))

                @pl.when(k + 2 < ROW_BLOCKS * 2 * n_half)
                def _():
                    down_copy(k + 2, slot).start()

            with jax.named_scope(f"downpeer{r}"):
                @pl.loop(0, n_half)
                def _(j):
                    def store(value):
                        sh_send[r, j] = value
                        if r == 0:
                            ysh_copy(r, j).start()

                    down(j, 0, store)

                if r > 0:
                    ysh_copy(r, 0).start()

            if r == 0:
                wr_load.start()
                with jax.named_scope("dispatch"):
                    dispatch()
            with jax.named_scope(f"downown{r}"):
                @pl.loop(0, n_half)
                def _(j):
                    def store(value):
                        sh_own[j, r * r_rows:(r + 1) * r_rows, :] = value

                    down(j, n_half, store)

    shared_sems = [pltpu.SemaphoreType.DMA((SHARED_BUFS,))] * 3
    pl.run_scoped(shared_phase, pltpu.VMEM((r_rows, ff_shared), BF16), pltpu.VMEM((SHARED_BUFS, d_model, WIDE), BF16), pltpu.VMEM((SHARED_BUFS, d_model, WIDE), BF16),
                  pltpu.VMEM((2, ff_shared, WIDE), BF16), *shared_sems)

    def yex_copy(sub, i):
        rows = pl.ds(bounds[i], min(bounds[i + 1], sent) - bounds[i])
        return remote(ex_send.at[sub, rows], ex_recv.at[sub, rows], yex_send.at[sub, i], yex_recv.at[sub, i], y_peer)

    def ret_copy(sub, i, who, s_sem, r_sem, dev):
        ref = ret.at[sub, who, pl.ds(bounds[i], bounds[i + 1] - bounds[i])]
        return remote(ref, ref, s_sem.at[sub, i], r_sem.at[sub, i], dev)

    def give(sub, i):
        yex_copy(sub, i).wait()
        rows = slice(bounds[i], bounds[i + 1])
        ret[sub, pl.ds(me, 1), rows, :] = (ex_own[sub, rows, :] + ex_recv[sub, rows, :]).astype(BF16).reshape(1, bounds[i + 1] - bounds[i], sub_cols)
        ret_copy(sub, i, me, rx_send, rx_recv, xp_dev).start()
        ret_copy(sub, i, me, rs_send, rs_recv, sib_dev).start()

    def forward(sub, i):
        ret_copy(sub, i, me, rx_send, rx_recv, xp_dev).wait()
        ret_copy(sub, i, xp, rf_send, rf_recv, sib_dev).start()

    def routed_phase(sel_near, sel_far, wg, wu, wd, g_sem, u_sem, d_sem):
        def gate_copy(e, slot):
            return pltpu.make_async_copy(weg_hbm.at[e], wg.at[slot], g_sem.at[slot])

        def up_copy(e, slot):
            return pltpu.make_async_copy(weu_hbm.at[e], wu.at[slot], u_sem.at[slot])

        def down_copy(e, slot):
            return pltpu.make_async_copy(wed_hbm.at[e], wd.at[slot], d_sem.at[slot])

        for slot in range(2):
            gate_copy(slot, slot).start()
            up_copy(slot, slot).start()
            down_copy(slot, slot).start()

        res_load.start()
        xp_copies[1].start()
        with jax.named_scope("routing"):
            pos = lax.broadcasted_iota(jnp.int32, (slots, LANES), 0)
            slot_expert = sum((pos >= e * window).astype(jnp.int32) for e in range(1, local_experts))
            first_row = slot_expert * capacity
            row = (first_row // 8) * 8 + (pos - slot_expert * window)
            slot_code = jnp.where((row >= first_row) & (row < first_row + capacity), row + me * pack, -2).astype(F32)
            def pick_rows(codes):
                return (jnp.broadcast_to(slot_code[:, 0:1], (slots, codes.shape[1])) == codes).astype(F32).astype(BF16)

            for i, q in enumerate((me, sib)):
                codes = code_rows[q]
                for lo in range(0, tok, LANES):
                    sel_near[:, i * tok + lo:i * tok + lo + LANES] = pick_rows(codes[0:1, lo:lo + LANES])
            def sorted_codes(q):
                hit, code_t = sort_block(q)
                return jnp.sum(jnp.where(hit, code_t, 0.0), axis=0, keepdims=True)

            codes_xp, codes_diag = sorted_codes(xp), sorted_codes(diag)
            for c in range(X_CHUNKS):
                both = jnp.concatenate([codes_xp[:, x_cuts[c]:x_cuts[c + 1]], codes_diag[:, x_cuts[c]:x_cuts[c + 1]]], axis=1)
                for lo in range(0, 2 * (x_cuts[c + 1] - x_cuts[c]), LANES):
                    dst = 2 * x_cuts[c] + lo
                    sel_far[:, dst:dst + LANES] = pick_rows(both[:, lo:lo + LANES])

            code_t = jnp.broadcast_to(code_rows[me][0:1, :], (LANES, tok)).T
            code_col[...] = code_t

        nc = 512
        with jax.named_scope("near"):
            sib_copy.wait()

            @pl.loop(0, d_model // nc)
            def _(n):
                cols = pl.ds(pl.multiple_of(n * nc, nc), nc)
                slot_x[:, cols] = dot(sel_near[...], x_near[:, :, cols].reshape(2 * tok, nc)).astype(BF16)

        def pass_on(c):
            if c == X_CHUNKS - 2:
                xp_copies[c].wait_send()
                xp_copies[c + 1].start()
            xp_copies[c].wait_recv()
            fw_copies[c].start()

        def gather(c):
            fw_copies[c].wait_recv()

            @pl.loop(0, d_model // nc)
            def _(n):
                cols = pl.ds(pl.multiple_of(n * nc, nc), nc)
                span = slice(2 * x_cuts[c], 2 * x_cuts[c + 1])
                slot_x[:, cols] += dot(sel_far[:, span], x_far[span, cols]).astype(BF16)

        pass_on(0)
        with jax.named_scope("router"):
            wr_load.wait()
            x = x_near[0]
            w = wr[...]
            w_hi = w.astype(BF16)
            w_rest = w - w_hi.astype(F32)
            w_mid = w_rest.astype(BF16)
            w_lo = (w_rest - w_mid.astype(F32)).astype(BF16)
            logits = dot_bt(x, w_hi) + (dot_bt(x, w_mid) + dot_bt(x, w_lo))
            top = jnp.max(logits, axis=1, keepdims=True)
            prob = jnp.exp(logits - top)
            denom = jnp.sum(prob, axis=1, keepdims=True)
            lane_lo = expert_base(lax.broadcasted_iota(jnp.int32, (tok, experts), 1))
            code_e = code_col[:, 0:experts]
            picked = (code_e >= lane_lo) & (code_e < lane_lo + cap)
            gate = jnp.sum(jnp.where(picked, prob, 0.0), axis=1, keepdims=True) / denom
            gate_col[...] = jnp.broadcast_to(gate, (tok, LANES))

        xp_copies[2].start()
        with jax.named_scope("far0"):
            gather(0)

        pass_at = [0, 1, 3, 4]
        loop_steps = [(5, give, 0, 0), (6, give, 1, 0), (7, give, 0, 1), (8, forward, 0, 0), (8, give, 1, 1), (9, forward, 1, 0), (10, forward, 0, 1), (11, forward, 1, 1), (12, give, 0, 2)]
        far_at = [x_cuts[c] // (2 * capacity) for c in range(X_CHUNKS)]
        if sent < pack:
            for sub in range(SUBS):
                ex_recv[sub, sent:pack, :] = jnp.zeros((pack - sent, sub_cols), F32)

        with jax.named_scope("experts"):
            for sub in range(SUBS):
                ex_send[sub, 0:8, :] = jnp.zeros((8, sub_cols), F32)
                ex_own[sub, 0:8, :] = jnp.zeros((8, sub_cols), F32)

            @pl.loop(0, local_experts)
            def _(e):
                slot = lax.rem(e, 2)
                for c in range(1, X_CHUNKS):
                    @pl.when(e == pass_at[c])
                    def _():
                        pass_on(c)

                    @pl.when(e == far_at[c])
                    def _():
                        with jax.named_scope(f"far{c}"):
                            gather(c)

                gate_copy(e, slot).wait()
                up_copy(e, slot).wait()
                rows = slot_x[pl.ds(pl.multiple_of(e * window, window), window), :]
                g = dot_bt(wg[slot], rows)
                u = dot_bt(wu[slot], rows)
                hidden = (jax.nn.silu(g) * u).astype(BF16)

                @pl.when(e + 2 < local_experts)
                def _():
                    gate_copy(e + 2, slot).start()
                    up_copy(e + 2, slot).start()

                down_copy(e, slot).wait()
                row = pl.multiple_of((e * capacity) // 8 * 8, 8)
                for buf, off in ((ex_send, peer_off), (ex_own, own_off)):
                    value = dot_at(hidden, wd[slot, :, pl.ds(off, half)])
                    for sub in range(SUBS):
                        part = value[:, sub * sub_cols:(sub + 1) * sub_cols]
                        buf[sub, pl.ds(row, 8), :] += part[0:8]
                        buf[sub, pl.ds(row + 8, window - 8), :] = part[8:]

                @pl.when(e + 2 < local_experts)
                def _():
                    down_copy(e + 2, slot).start()

                for i in range(groups):
                    @pl.when(e == last_expert[i])
                    def _():
                        yex_copy(0, i).start()
                        if i < EARLY_GROUPS:
                            yex_copy(1, i).start()

                for when, action, sub, i in loop_steps:
                    @pl.when(e == when)
                    def _():
                        action(sub, i)

            for i in range(EARLY_GROUPS, groups):
                yex_copy(1, i).start()

    pl.run_scoped(routed_phase, pltpu.VMEM((slots, 2 * tok), BF16), pltpu.VMEM((slots, 2 * tok), BF16),
                  pltpu.VMEM((2, ff_expert, d_model), BF16), pltpu.VMEM((2, ff_expert, d_model), BF16),
                  pltpu.VMEM((2, ff_expert, d_model), BF16), pltpu.SemaphoreType.DMA((2,)), pltpu.SemaphoreType.DMA((2,)), pltpu.SemaphoreType.DMA((2,)))

    with jax.named_scope("fin_shared"):
        for copy in xp_copies[:-2] + xp_copies[-1:] + fw_copies:
            copy.wait_send()
        res_load.wait()
        for r in range(ROW_BLOCKS):
            if r > 0:
                ysh_copy(r, 0).wait()

            @pl.loop(0, n_half)
            def _(j):
                if r == 0:
                    ysh_copy(r, j).wait()
                cols = pl.ds(pl.multiple_of(j * WIDE, WIDE), WIDE)
                rows = slice(r * r_rows, (r + 1) * r_rows)
                sh_own[j, rows, :] = res_half[rows, cols].astype(F32) + (sh_own[j, rows, :] + sh_recv[r, j])

    def combine(pick, sub, i):
        n = bounds[i + 1] - bounds[i]
        lanes = slice(ep_size * bounds[i], ep_size * bounds[i + 1])
        if sub == 0:
            lane = lax.broadcasted_iota(jnp.int32, (tok, ep_size * n), 1)
            owner = sum((lane >= q * n).astype(jnp.int32) for q in range(1, ep_size))
            lane_code = (lane + owner * (pack - n) + bounds[i]).astype(F32)
            pick[:, lanes] = (code_col[:, 0:1] == lane_code).astype(F32).astype(BF16)
        ret_copy(sub, i, me, rs_send, rs_recv, sib_dev).wait()
        ret_copy(sub, i, xp, rf_send, rf_recv, sib_dev).wait()
        rows = ret[sub, :, bounds[i]:bounds[i + 1], :].reshape(ep_size * n, sub_cols)
        gate = gate_col[:, 0:1]
        for j in range(sub_blocks):
            jj = sub * sub_blocks + j
            sh_own[jj] = sh_own[jj] + gate * dot(pick[:, lanes], rows[:, j * WIDE:(j + 1) * WIDE])

    def out_copies(sub):
        src = out_half.at[sub]
        dst = o_hbm.at[:, pl.ds(pl.multiple_of(own_off + sub * sub_cols, sub_cols), sub_cols)]
        return remote(src, dst, yo_send.at[sub], yo_recv.at[sub], y_peer), pltpu.make_async_copy(src, dst, lo_sem.at[sub])

    def emit(sub):
        for j in range(sub_blocks):
            out_half[sub, :, j * WIDE:(j + 1) * WIDE] = sh_own[sub * sub_blocks + j].astype(BF16)

    def start_out(sub):
        for copy in out_copies(sub):
            copy.start()

    def return_phase(pick):
        steps = [(give, 1, 2), (forward, 0, 2), (combine, 0, 0), (combine, 1, 0), (combine, 0, 1), (combine, 1, 1), (give, 0, 3), (forward, 1, 2), (combine, 0, 2),
                 (forward, 0, 3), (combine, 1, 2), (give, 0, 4), (combine, 0, 3), (forward, 0, 4), (combine, 0, 4), (emit, 0), (start_out, 0),
                 (give, 1, 3), (forward, 1, 3), (give, 1, 4), (combine, 1, 3), (forward, 1, 4), (combine, 1, 4), (emit, 1), (start_out, 1)]
        for step in steps:
            with jax.named_scope(step[0].__name__ + "".join(str(a) for a in step[1:])):
                if step[0] is combine:
                    combine(pick, *step[1:])
                else:
                    step[0](*step[1:])

    pl.run_scoped(return_phase, pltpu.VMEM((tok, ep_size * pack), BF16))

    with jax.named_scope("out"):
        for sub in range(SUBS):
            for copy in out_copies(sub):
                copy.wait()


def copy_kernel(src, dst, buf, in_sem, out_sem):
    n = src.shape[0] // COPY_CHUNKS
    reads = [pltpu.make_async_copy(src.at[pl.ds(c * n, n)], buf.at[pl.ds(c * n, n)], in_sem.at[c]) for c in range(COPY_CHUNKS)]
    writes = [pltpu.make_async_copy(buf.at[pl.ds(c * n, n)], dst.at[pl.ds(c * n, n)], out_sem.at[c]) for c in range(COPY_CHUNKS)]
    for copy in reads:
        copy.start()
    for read, write in zip(reads, writes):
        read.wait()
        write.start()
    for copy in writes:
        copy.wait()


def solution(mesh):
    ep_size = mesh.shape["ep"]
    tok_spec = P(("dp", "ep"), None)
    id_spec = P(("dp", "ep"))

    def device_step(normed, residual, w_router, ws_gate, ws_up, ws_down, we_gate, we_up, we_down, first_id, alt_id):
        tok, d_model = normed.shape
        local_experts, _, ff_expert = we_gate.shape
        experts = local_experts * ep_size
        capacity = (5 * tok * ep_size + 4 * experts - 1) // (4 * experts)
        window = -(-(capacity + 7) // 16) * 16
        pack = -(-local_experts * capacity // 16) * 16
        pack_buf = max(pack, (local_experts - 1) * capacity // 8 * 8 + window)
        bounds = [0] + [int(pack * f) // 32 * 32 for f in (0.13, 0.255, 0.45, 0.76)] + [pack]
        half = d_model // 2
        slots = local_experts * window
        n_half = half // WIDE
        r_rows = tok // ROW_BLOCKS
        sub_cols = half // SUBS
        dma = pltpu.SemaphoreType.DMA
        any_spec = pl.BlockSpec(memory_space=pl.ANY)
        vmem_spec = pl.BlockSpec(memory_space=pltpu.VMEM)
        per_ret = dma((SUBS, len(bounds) - 1))
        out = pl.pallas_call(
            functools.partial(moe_kernel, (experts, capacity, window, pack, bounds, local_experts, ep_size)),
            out_shape=jax.ShapeDtypeStruct((tok, d_model), BF16),
            in_specs=[any_spec] * 9 + [vmem_spec] * 2,
            out_specs=any_spec,
            scratch_shapes=[
                pltpu.VMEM((2, tok, d_model), BF16),
                pltpu.VMEM((2 * tok, d_model), BF16),
                pltpu.VMEM((tok, d_model), BF16),
                pltpu.VMEM((ep_size, 8, tok), jnp.int32),
                pltpu.VMEM((ep_size, 8, tok), F32),
                pltpu.VMEM((tok, LANES), F32),
                pltpu.VMEM((tok, LANES), F32),
                pltpu.VMEM((slots, d_model), BF16),
                pltpu.VMEM((n_half, tok, WIDE), F32),
                pltpu.VMEM((ROW_BLOCKS, n_half, r_rows, WIDE), F32),
                pltpu.VMEM((ROW_BLOCKS, n_half, r_rows, WIDE), F32),
                pltpu.VMEM((SUBS, pack_buf, sub_cols), F32),
                pltpu.VMEM((SUBS, pack_buf, sub_cols), F32),
                pltpu.VMEM((SUBS, pack, sub_cols), F32),
                pltpu.VMEM((SUBS, ep_size, pack, sub_cols), BF16),
                pltpu.VMEM((SUBS, tok, sub_cols), BF16),
                pltpu.VMEM((tok, half), BF16),
                pltpu.VMEM((experts, d_model), F32),
                dma((ROW_BLOCKS + 2,)), dma((3,)), dma((3,)), dma((1,)), dma((1,)), dma((X_CHUNKS,)), dma((X_CHUNKS,)), dma((X_CHUNKS,)), dma((X_CHUNKS,)),
                dma((ROW_BLOCKS, n_half)), dma((ROW_BLOCKS, n_half)), per_ret, per_ret, per_ret, per_ret, per_ret, per_ret, per_ret, per_ret,
                dma((SUBS,)), dma((SUBS,)), dma((SUBS,)),
            ],
            compiler_params=pltpu.CompilerParams(collective_id=0, has_side_effects=True, vmem_limit_bytes=67043328),
        )(normed, residual, w_router.T, ws_gate, ws_up, ws_down, jnp.swapaxes(we_gate, 1, 2), jnp.swapaxes(we_up, 1, 2), we_down,
          first_id.reshape(1, tok), alt_id.reshape(1, tok))
        return pl.pallas_call(
            copy_kernel,
            out_shape=jax.ShapeDtypeStruct((tok, d_model), BF16),
            in_specs=[any_spec],
            out_specs=any_spec,
            scratch_shapes=[pltpu.VMEM((tok, d_model), BF16), dma((COPY_CHUNKS,)), dma((COPY_CHUNKS,))],
        )(out)

    return jax.shard_map(device_step, mesh=mesh, in_specs=(tok_spec, tok_spec, P(None, None), P(None, 'tp'), P(None, 'tp'), P('tp', None), P('ep', None, 'tp'), P('ep', None, 'tp'), P('ep', 'tp', None), id_spec, id_spec), out_specs=tok_spec, check_vma=False)
```

```python
import functools

import jax
import jax.numpy as jnp
from jax import lax
from jax.experimental import pallas as pl
from jax.experimental.pallas import tpu as pltpu
from jax.sharding import PartitionSpec as P

MESH = pl.DeviceIdType.MESH
F32 = jnp.float32
BF16 = jnp.bfloat16
LANES = 128
RANK_BLOCK = 256
X_SPLIT = (0, 192, 320, 448, 512)
X_CHUNKS = 4
WIDE = 512
COPY_CHUNKS = 4
ROW_BLOCKS = 2
COL = 256
SUBS = 2
EARLY_GROUPS = 4
SHARED_BUFS = 4


def dot(a, b):
    return jnp.dot(a, b, preferred_element_type=F32)


def dot_bt(a, b):
    return lax.dot_general(a, b, (((1,), (1,)), ((), ())), preferred_element_type=F32)


def dot_at(a, b):
    return lax.dot_general(a, b, (((0,), (0,)), ((), ())), preferred_element_type=F32)


def moe_kernel(dims, x_hbm, res_hbm, wr_hbm, wsg_hbm, wsu_hbm, wsd_hbm, weg_hbm, weu_hbm, wed_hbm, first_ref, alt_ref, o_hbm,
               x_near, x_far, x_sorted, ids_all, code_rows, code_col, gate_col, slot_x, sh_own, sh_send, sh_recv, ex_own, ex_send, ex_recv, ret, out_half, res_half, wr,
               ld_sem, id_send, id_recv, sib_send, sib_recv, xp_send, xp_recv, fw_send, fw_recv,
               ysh_send, ysh_recv, yex_send, yex_recv, rs_send, rs_recv, rx_send, rx_recv, rf_send, rf_recv, yo_send, yo_recv, lo_sem):
    experts, capacity, window, pack, bounds, local_experts, ep_size = dims
    groups = len(bounds) - 1
    last_expert = [-(-min(b, local_experts * capacity) // capacity) - 1 for b in bounds[1:]]
    tok, d_model = x_hbm.shape
    half = d_model // 2
    slots = local_experts * window
    spare = pack - local_experts * capacity
    ff_shared = wsg_hbm.shape[1]
    ff_expert = weg_hbm.shape[1]
    dp = lax.axis_index("dp")
    t = lax.axis_index("tp")
    me = lax.axis_index("ep")
    core = lax.rem(me, 2)
    sib = me + 1 - 2 * core
    xp = lax.rem(me + 2, ep_size)
    diag = lax.rem(sib + 2, ep_size)
    y_peer = (dp, 1 - t, me)
    sib_dev = (dp, t, sib)
    xp_dev = (dp, t, xp)
    diag_dev = (dp, t, diag)
    own_off = pl.multiple_of(t * half, half)
    peer_off = pl.multiple_of((1 - t) * half, half)
    x_cuts = [tok * v // X_SPLIT[-1] for v in X_SPLIT]
    r_rows = tok // ROW_BLOCKS
    n_wide, tail = ff_shared // WIDE, ff_shared % WIDE
    n_chunks = n_wide + (tail > 0)
    n_half = half // WIDE
    sub_cols = half // SUBS
    sub_blocks = sub_cols // WIDE
    sent = -(-local_experts * capacity // 8) * 8

    barrier = pltpu.get_barrier_semaphore()
    for dev in (y_peer, sib_dev, xp_dev, diag_dev):
        pl.semaphore_signal(barrier, inc=1, device_id=dev, device_id_type=MESH)

    def remote(src, dst, s_sem, r_sem, dev):
        return pltpu.make_async_remote_copy(src_ref=src, dst_ref=dst, send_sem=s_sem, recv_sem=r_sem, device_id=dev, device_id_type=MESH)

    id_copies = [remote(ids_all.at[me], ids_all.at[me], id_send.at[i], id_recv.at[i], dev) for i, dev in enumerate((sib_dev, xp_dev, diag_dev))]
    def far_rows(c, i):
        n = x_cuts[c + 1] - x_cuts[c]
        return pl.ds(2 * x_cuts[c] + i * n, n)

    xp_copies = [remote(x_sorted.at[pl.ds(x_cuts[c], x_cuts[c + 1] - x_cuts[c])], x_far.at[far_rows(c, 0)], xp_send.at[c], xp_recv.at[c], xp_dev) for c in range(X_CHUNKS)]
    sib_copy = remote(x_near.at[0], x_near.at[1], sib_send.at[0], sib_recv.at[0], sib_dev)
    fw_copies = [remote(x_far.at[far_rows(c, 0)], x_far.at[far_rows(c, 1)], fw_send.at[c], fw_recv.at[c], sib_dev) for c in range(X_CHUNKS)]
    own_x = [pltpu.make_async_copy(x_hbm.at[pl.ds(r * r_rows, r_rows)], x_near.at[0, pl.ds(r * r_rows, r_rows)], ld_sem.at[r]) for r in range(ROW_BLOCKS)]
    res_load = pltpu.make_async_copy(res_hbm.at[:, pl.ds(own_off, half)], res_half, ld_sem.at[ROW_BLOCKS])
    wr_load = pltpu.make_async_copy(wr_hbm, wr, ld_sem.at[ROW_BLOCKS + 1])

    cap = jnp.float32(capacity)

    def expert_base(ids):
        owner = sum((ids >= q * local_experts).astype(jnp.int32) for q in range(1, ep_size))
        return (ids * capacity + owner * spare).astype(F32)

    def route():
        for copy in id_copies:
            copy.wait()
        e_pad = -(-experts // 8) * 8
        e_iota = lax.broadcasted_iota(jnp.int32, (e_pad, RANK_BLOCK), 0)
        row_i = lax.broadcasted_iota(jnp.int32, (RANK_BLOCK, RANK_BLOCK), 0)
        col_i = lax.broadcasted_iota(jnp.int32, (RANK_BLOCK, RANK_BLOCK), 1)
        upper = (row_i <= col_i).astype(F32).astype(BF16)
        blocks = [(q, b * RANK_BLOCK) for q in range(ep_size) for b in range(tok // RANK_BLOCK)]
        total = jnp.zeros((e_pad, 1), F32)
        rank_first = []
        for q, lo in blocks:
            first = ids_all[q, 0:1, lo:lo + RANK_BLOCK]
            hot = (e_iota == first).astype(F32)
            cum = dot(hot.astype(BF16), upper) + total
            rank_first.append(jnp.sum(cum * hot, axis=0, keepdims=True) - 1.0)
            total = total + jnp.sum(hot, axis=1, keepdims=True)
        load = jnp.minimum(total, cap)
        room = cap - load
        total = jnp.zeros((e_pad, 1), F32)
        for i, (q, lo) in enumerate(blocks):
            first = ids_all[q, 0:1, lo:lo + RANK_BLOCK]
            alt = ids_all[q, 1:2, lo:lo + RANK_BLOCK]
            kept = rank_first[i] < cap
            over = jnp.where(kept, 0.0, 1.0)
            hot = (e_iota == alt).astype(F32) * over
            cum = dot(hot.astype(BF16), upper) + total
            rank_alt = jnp.sum(cum * hot, axis=0, keepdims=True) - 1.0
            total = total + jnp.sum(hot, axis=1, keepdims=True)
            room_tok = jnp.sum(hot * room, axis=0, keepdims=True)
            load_tok = jnp.sum(hot * load, axis=0, keepdims=True)
            code_first = expert_base(first) + rank_first[i]
            code_alt = jnp.where(rank_alt < room_tok, expert_base(alt) + load_tok + rank_alt, -1.0)
            code = jnp.where(kept, code_first, code_alt)
            code_rows[q, :, lo:lo + RANK_BLOCK] = jnp.broadcast_to(code, (8, RANK_BLOCK))

    def sort_block(q):
        code_t = jnp.broadcast_to(code_rows[q][0:1, :], (LANES, tok)).T[:, 0:1]
        shift = ((1 - lax.div(q, 2)) * (2 * pack)).astype(F32)

        def key_of(code):
            rel = code - shift
            local = jnp.where(rel >= pack, rel - pack, rel)
            return jnp.where((rel >= 0.0) & (rel < 2.0 * pack), local, 8192.0)

        key_t = key_of(code_t)
        key = key_of(code_rows[q][0:1, :])
        lane = lax.broadcasted_iota(jnp.int32, (tok, tok), 1)
        line = lax.broadcasted_iota(jnp.int32, (tok, tok), 0)
        ahead = (key < key_t) | ((key == key_t) & (lane < line))
        position = jnp.sum(jnp.where(ahead, 1.0, 0.0), axis=1, keepdims=True)
        return position == lane.astype(F32), code_t

    def dispatch():
        route()
        hit, _ = sort_block(me)
        order = hit.astype(F32).astype(BF16)
        for lo in range(0, d_model, WIDE):
            x_sorted[:, lo:lo + WIDE] = dot_at(order, x_near[0, :, lo:lo + WIDE]).astype(BF16)
        xp_copies[0].start()

    def ysh_copy(r, j):
        if r == 0:
            return remote(sh_send.at[r, j], sh_recv.at[r, j], ysh_send.at[r, j], ysh_recv.at[r, j], y_peer)
        return remote(sh_send.at[r], sh_recv.at[r], ysh_send.at[r, 0], ysh_recv.at[r, 0], y_peer)

    def shared_phase(act, wg, wu, wd, g_sem, u_sem, d_sem):
        def weight_copies(c, slot, width):
            cols = pl.ds(pl.multiple_of(c * WIDE, WIDE), width)
            dst = pl.ds(0, width)
            return (pltpu.make_async_copy(wsg_hbm.at[:, cols], wg.at[slot, :, dst], g_sem.at[slot]),
                    pltpu.make_async_copy(wsu_hbm.at[:, cols], wu.at[slot, :, dst], u_sem.at[slot]))

        def start_weights(k, slot):
            c = lax.rem(k, n_chunks)

            @pl.when(c < n_wide)
            def _():
                for copy in weight_copies(c, slot, WIDE):
                    copy.start()

            if tail:
                @pl.when(c == n_wide)
                def _():
                    for copy in weight_copies(c, slot, tail):
                        copy.start()

        def down_copy(k, slot):
            j = lax.rem(k, 2 * n_half)
            col = jnp.where(j < n_half, peer_off + j * WIDE, own_off + (j - n_half) * WIDE)
            return pltpu.make_async_copy(wsd_hbm.at[:, pl.ds(pl.multiple_of(col, WIDE), WIDE)], wd.at[slot], d_sem.at[slot])

        own_x[0].start()
        start_weights(jnp.int32(0), 0)
        for copy in own_x[1:]:
            copy.start()
        for slot in range(1, SHARED_BUFS):
            start_weights(jnp.int32(slot), slot)
        ids_all[pl.ds(me, 1), 0:1, :] = first_ref[...].reshape(1, 1, tok)
        ids_all[pl.ds(me, 1), 1:2, :] = alt_ref[...].reshape(1, 1, tok)
        def exchange():
            for copy in own_x[1:]:
                copy.wait()
            pl.semaphore_wait(barrier, 4)
            for copy in id_copies:
                copy.start()
            sib_copy.start()

        for r in range(ROW_BLOCKS):
            if r == 0:
                own_x[0].wait()
            def gateup(c, width):
                k = c + r * n_chunks
                slot = lax.rem(k, SHARED_BUFS)
                for copy in weight_copies(c, slot, width):
                    copy.wait()
                x = x_near[0, r * r_rows:(r + 1) * r_rows, :]
                for lo in range(0, width, COL):
                    g = dot(x, wg[slot, :, lo:lo + COL])
                    u = dot(x, wu[slot, :, lo:lo + COL])
                    act[:, pl.ds(pl.multiple_of(c * WIDE + lo, COL), COL)] = (jax.nn.silu(g) * u).astype(BF16)

                @pl.when(k + SHARED_BUFS < (r + 1) * n_chunks)
                def _():
                    start_weights(k + SHARED_BUFS, slot)

            with jax.named_scope(f"gateup{r}"):
                @pl.loop(0, n_wide)
                def _(c):
                    gateup(c, WIDE)

                    if r == 0:
                        @pl.when(c == 0)
                        def _():
                            exchange()

                        @pl.when(c == 2)
                        def _():
                            with jax.named_scope("dispatch"):
                                dispatch()

                    if r == 0:
                        @pl.when((c == 1) | (c == 3))
                        def _():
                            slot = lax.div(c, 2)
                            down_copy(slot, slot).start()

                if tail:
                    gateup(jnp.int32(n_wide), tail)

            if r + 1 == ROW_BLOCKS:
                xp_copies[1].start()

            if r + 1 < ROW_BLOCKS:
                for i in range(SHARED_BUFS):
                    k = (r + 1) * n_chunks + i
                    start_weights(jnp.int32(k), k % SHARED_BUFS)

            def down(j, base, store):
                k = j + r * 2 * n_half + base
                slot = lax.rem(k, 2)
                down_copy(k, slot).wait()
                store(dot(act[...], wd[slot]))

                @pl.when(k + 2 < ROW_BLOCKS * 2 * n_half)
                def _():
                    down_copy(k + 2, slot).start()

            with jax.named_scope(f"downpeer{r}"):
                @pl.loop(0, n_half)
                def _(j):
                    def store(value):
                        sh_send[r, j] = value
                        if r == 0:
                            ysh_copy(r, j).start()

                    down(j, 0, store)

                if r > 0:
                    ysh_copy(r, 0).start()

            if r == 0:
                wr_load.start()
            with jax.named_scope(f"downown{r}"):
                @pl.loop(0, n_half)
                def _(j):
                    def store(value):
                        sh_own[j, r * r_rows:(r + 1) * r_rows, :] = value

                    down(j, n_half, store)

    shared_sems = [pltpu.SemaphoreType.DMA((SHARED_BUFS,))] * 3
    pl.run_scoped(shared_phase, pltpu.VMEM((r_rows, ff_shared), BF16), pltpu.VMEM((SHARED_BUFS, d_model, WIDE), BF16), pltpu.VMEM((SHARED_BUFS, d_model, WIDE), BF16),
                  pltpu.VMEM((2, ff_shared, WIDE), BF16), *shared_sems)

    def yex_copy(sub, i):
        rows = pl.ds(bounds[i], min(bounds[i + 1], sent) - bounds[i])
        return remote(ex_send.at[sub, rows], ex_recv.at[sub, rows], yex_send.at[sub, i], yex_recv.at[sub, i], y_peer)

    def ret_copy(sub, i, who, s_sem, r_sem, dev):
        ref = ret.at[sub, who, pl.ds(bounds[i], bounds[i + 1] - bounds[i])]
        return remote(ref, ref, s_sem.at[sub, i], r_sem.at[sub, i], dev)

    def give(sub, i):
        yex_copy(sub, i).wait()
        rows = slice(bounds[i], bounds[i + 1])
        ret[sub, pl.ds(me, 1), rows, :] = (ex_own[sub, rows, :] + ex_recv[sub, rows, :]).astype(BF16).reshape(1, bounds[i + 1] - bounds[i], sub_cols)
        ret_copy(sub, i, me, rx_send, rx_recv, xp_dev).start()
        ret_copy(sub, i, me, rs_send, rs_recv, sib_dev).start()

    def forward(sub, i):
        ret_copy(sub, i, me, rx_send, rx_recv, xp_dev).wait()
        ret_copy(sub, i, xp, rf_send, rf_recv, sib_dev).start()

    def routed_phase(sel_near, sel_far, wg, wu, wd, g_sem, u_sem, d_sem):
        def gate_copy(e, slot):
            return pltpu.make_async_copy(weg_hbm.at[e], wg.at[slot], g_sem.at[slot])

        def up_copy(e, slot):
            return pltpu.make_async_copy(weu_hbm.at[e], wu.at[slot], u_sem.at[slot])

        def down_copy(e, slot):
            return pltpu.make_async_copy(wed_hbm.at[e], wd.at[slot], d_sem.at[slot])

        for slot in range(2):
            gate_copy(slot, slot).start()
            up_copy(slot, slot).start()
            down_copy(slot, slot).start()

        res_load.start()
        xp_copies[0].wait_recv()
        fw_copies[0].start()
        with jax.named_scope("routing"):
            pos = lax.broadcasted_iota(jnp.int32, (slots, LANES), 0)
            slot_expert = sum((pos >= e * window).astype(jnp.int32) for e in range(1, local_experts))
            first_row = slot_expert * capacity
            row = (first_row // 8) * 8 + (pos - slot_expert * window)
            slot_code = jnp.where((row >= first_row) & (row < first_row + capacity), row + me * pack, -2).astype(F32)
            def pick_rows(codes):
                return (jnp.broadcast_to(slot_code[:, 0:1], (slots, codes.shape[1])) == codes).astype(F32).astype(BF16)

            for i, q in enumerate((me, sib)):
                codes = code_rows[q]
                for lo in range(0, tok, LANES):
                    sel_near[:, i * tok + lo:i * tok + lo + LANES] = pick_rows(codes[0:1, lo:lo + LANES])
            def sorted_codes(q):
                hit, code_t = sort_block(q)
                return jnp.sum(jnp.where(hit, code_t, 0.0), axis=0, keepdims=True)

            codes_xp, codes_diag = sorted_codes(xp), sorted_codes(diag)
            for c in range(X_CHUNKS):
                both = jnp.concatenate([codes_xp[:, x_cuts[c]:x_cuts[c + 1]], codes_diag[:, x_cuts[c]:x_cuts[c + 1]]], axis=1)
                for lo in range(0, 2 * (x_cuts[c + 1] - x_cuts[c]), LANES):
                    dst = 2 * x_cuts[c] + lo
                    sel_far[:, dst:dst + LANES] = pick_rows(both[:, lo:lo + LANES])

            code_t = jnp.broadcast_to(code_rows[me][0:1, :], (LANES, tok)).T
            code_col[...] = code_t

        nc = 512
        with jax.named_scope("near"):
            sib_copy.wait()

            @pl.loop(0, d_model // nc)
            def _(n):
                cols = pl.ds(pl.multiple_of(n * nc, nc), nc)
                slot_x[:, cols] = dot(sel_near[...], x_near[:, :, cols].reshape(2 * tok, nc)).astype(BF16)

        def pass_on(c):
            xp_copies[c].wait_recv()
            fw_copies[c].start()

        def gather(c):
            fw_copies[c].wait_recv()

            @pl.loop(0, d_model // nc)
            def _(n):
                cols = pl.ds(pl.multiple_of(n * nc, nc), nc)
                span = slice(2 * x_cuts[c], 2 * x_cuts[c + 1])
                slot_x[:, cols] += dot(sel_far[:, span], x_far[span, cols]).astype(BF16)

        xp_copies[2].start()
        with jax.named_scope("router"):
            wr_load.wait()
            x = x_near[0]
            w = wr[...]
            w_hi = w.astype(BF16)
            w_rest = w - w_hi.astype(F32)
            w_mid = w_rest.astype(BF16)
            w_lo = (w_rest - w_mid.astype(F32)).astype(BF16)
            logits = dot_bt(x, w_hi) + (dot_bt(x, w_mid) + dot_bt(x, w_lo))
            top = jnp.max(logits, axis=1, keepdims=True)
            prob = jnp.exp(logits - top)
            denom = jnp.sum(prob, axis=1, keepdims=True)
            lane_lo = expert_base(lax.broadcasted_iota(jnp.int32, (tok, experts), 1))
            code_e = code_col[:, 0:experts]
            picked = (code_e >= lane_lo) & (code_e < lane_lo + cap)
            gate = jnp.sum(jnp.where(picked, prob, 0.0), axis=1, keepdims=True) / denom
            gate_col[...] = jnp.broadcast_to(gate, (tok, LANES))

        with jax.named_scope("far0"):
            gather(0)

        pass_at = [0, 1, 3, 4]
        loop_steps = [(5, give, 0, 0), (6, give, 1, 0), (7, forward, 0, 0), (8, give, 0, 1), (8, forward, 1, 0), (9, give, 1, 1), (10, forward, 0, 1), (11, forward, 1, 1),
                      (11, give, 0, 2), (13, forward, 0, 2), (13, give, 1, 2)]
        far_at = [x_cuts[c] // (2 * capacity) for c in range(X_CHUNKS)]
        if sent < pack:
            for sub in range(SUBS):
                ex_recv[sub, sent:pack, :] = jnp.zeros((pack - sent, sub_cols), F32)

        with jax.named_scope("experts"):
            for sub in range(SUBS):
                ex_send[sub, 0:8, :] = jnp.zeros((8, sub_cols), F32)
                ex_own[sub, 0:8, :] = jnp.zeros((8, sub_cols), F32)

            @pl.loop(0, local_experts)
            def _(e):
                slot = lax.rem(e, 2)
                @pl.when(e == 2)
                def _():
                    xp_copies[2].wait_send()
                    xp_copies[3].start()

                for c in range(1, X_CHUNKS):
                    @pl.when(e == pass_at[c])
                    def _():
                        pass_on(c)

                    @pl.when(e == far_at[c])
                    def _():
                        with jax.named_scope(f"far{c}"):
                            gather(c)

                gate_copy(e, slot).wait()
                up_copy(e, slot).wait()
                rows = slot_x[pl.ds(pl.multiple_of(e * window, window), window), :]
                g = dot_bt(wg[slot], rows)
                u = dot_bt(wu[slot], rows)
                hidden = (jax.nn.silu(g) * u).astype(BF16)

                @pl.when(e + 2 < local_experts)
                def _():
                    gate_copy(e + 2, slot).start()
                    up_copy(e + 2, slot).start()

                down_copy(e, slot).wait()
                row = pl.multiple_of((e * capacity) // 8 * 8, 8)
                for buf, off in ((ex_send, peer_off), (ex_own, own_off)):
                    value = dot_at(hidden, wd[slot, :, pl.ds(off, half)])
                    for sub in range(SUBS):
                        part = value[:, sub * sub_cols:(sub + 1) * sub_cols]
                        buf[sub, pl.ds(row, 8), :] += part[0:8]
                        buf[sub, pl.ds(row + 8, window - 8), :] = part[8:]

                @pl.when(e + 2 < local_experts)
                def _():
                    down_copy(e + 2, slot).start()

                for i in range(groups):
                    @pl.when(e == last_expert[i])
                    def _():
                        yex_copy(0, i).start()
                        if i < EARLY_GROUPS:
                            yex_copy(1, i).start()

                for when, action, sub, i in loop_steps:
                    @pl.when(e == when)
                    def _():
                        action(sub, i)

            for i in range(EARLY_GROUPS, groups):
                yex_copy(1, i).start()

    pl.run_scoped(routed_phase, pltpu.VMEM((slots, 2 * tok), BF16), pltpu.VMEM((slots, 2 * tok), BF16),
                  pltpu.VMEM((2, ff_expert, d_model), BF16), pltpu.VMEM((2, ff_expert, d_model), BF16),
                  pltpu.VMEM((2, ff_expert, d_model), BF16), pltpu.SemaphoreType.DMA((2,)), pltpu.SemaphoreType.DMA((2,)), pltpu.SemaphoreType.DMA((2,)))

    with jax.named_scope("fin_shared"):
        for copy in xp_copies[:-2] + xp_copies[-1:] + fw_copies:
            copy.wait_send()
        res_load.wait()
        for r in range(ROW_BLOCKS):
            if r > 0:
                ysh_copy(r, 0).wait()

            @pl.loop(0, n_half)
            def _(j):
                if r == 0:
                    ysh_copy(r, j).wait()
                cols = pl.ds(pl.multiple_of(j * WIDE, WIDE), WIDE)
                rows = slice(r * r_rows, (r + 1) * r_rows)
                sh_own[j, rows, :] = res_half[rows, cols].astype(F32) + (sh_own[j, rows, :] + sh_recv[r, j])

    def combine(pick, sub, i):
        n = bounds[i + 1] - bounds[i]
        lanes = slice(ep_size * bounds[i], ep_size * bounds[i + 1])
        if sub == 0:
            lane = lax.broadcasted_iota(jnp.int32, (tok, ep_size * n), 1)
            owner = sum((lane >= q * n).astype(jnp.int32) for q in range(1, ep_size))
            lane_code = (lane + owner * (pack - n) + bounds[i]).astype(F32)
            pick[:, lanes] = (code_col[:, 0:1] == lane_code).astype(F32).astype(BF16)
        ret_copy(sub, i, me, rs_send, rs_recv, sib_dev).wait()
        ret_copy(sub, i, xp, rf_send, rf_recv, sib_dev).wait()
        rows = ret[sub, :, bounds[i]:bounds[i + 1], :].reshape(ep_size * n, sub_cols)
        gate = gate_col[:, 0:1]
        for j in range(sub_blocks):
            jj = sub * sub_blocks + j
            sh_own[jj] = sh_own[jj] + gate * dot(pick[:, lanes], rows[:, j * WIDE:(j + 1) * WIDE])

    def out_copies(sub):
        src = out_half.at[sub]
        dst = o_hbm.at[:, pl.ds(pl.multiple_of(own_off + sub * sub_cols, sub_cols), sub_cols)]
        return remote(src, dst, yo_send.at[sub], yo_recv.at[sub], y_peer), pltpu.make_async_copy(src, dst, lo_sem.at[sub])

    def emit(sub):
        for j in range(sub_blocks):
            out_half[sub, :, j * WIDE:(j + 1) * WIDE] = sh_own[sub * sub_blocks + j].astype(BF16)

    def start_out(sub):
        for copy in out_copies(sub):
            copy.start()

    def return_phase(pick):
        steps = [(forward, 1, 2), (combine, 0, 0), (combine, 1, 0), (combine, 0, 1), (combine, 1, 1), (combine, 0, 2), (give, 0, 3), (combine, 1, 2), (forward, 0, 3),
                 (combine, 0, 3), (give, 1, 3), (forward, 1, 3), (give, 0, 4), (combine, 1, 3), (forward, 0, 4), (give, 0, 5), (combine, 0, 4), (forward, 0, 5),
                 (combine, 0, 5), (emit, 0), (start_out, 0), (give, 1, 4), (forward, 1, 4), (give, 1, 5), (combine, 1, 4), (forward, 1, 5), (combine, 1, 5), (emit, 1), (start_out, 1)]
        for step in steps:
            with jax.named_scope(step[0].__name__ + "".join(str(a) for a in step[1:])):
                if step[0] is combine:
                    combine(pick, *step[1:])
                else:
                    step[0](*step[1:])

    pl.run_scoped(return_phase, pltpu.VMEM((tok, ep_size * pack), BF16))

    with jax.named_scope("out"):
        for sub in range(SUBS):
            for copy in out_copies(sub):
                copy.wait()


def copy_kernel(src, dst, buf, in_sem, out_sem):
    n = src.shape[0] // COPY_CHUNKS
    reads = [pltpu.make_async_copy(src.at[pl.ds(c * n, n)], buf.at[pl.ds(c * n, n)], in_sem.at[c]) for c in range(COPY_CHUNKS)]
    writes = [pltpu.make_async_copy(buf.at[pl.ds(c * n, n)], dst.at[pl.ds(c * n, n)], out_sem.at[c]) for c in range(COPY_CHUNKS)]
    for copy in reads:
        copy.start()
    for read, write in zip(reads, writes):
        read.wait()
        write.start()
    for copy in writes:
        copy.wait()


def solution(mesh):
    ep_size = mesh.shape["ep"]
    tok_spec = P(("dp", "ep"), None)
    id_spec = P(("dp", "ep"))

    def device_step(normed, residual, w_router, ws_gate, ws_up, ws_down, we_gate, we_up, we_down, first_id, alt_id):
        tok, d_model = normed.shape
        local_experts, _, ff_expert = we_gate.shape
        experts = local_experts * ep_size
        capacity = (5 * tok * ep_size + 4 * experts - 1) // (4 * experts)
        window = -(-(capacity + 7) // 16) * 16
        pack = -(-local_experts * capacity // 16) * 16
        pack_buf = max(pack, (local_experts - 1) * capacity // 8 * 8 + window)
        bounds = [0] + [int(pack * f) // 32 * 32 for f in (0.13, 0.255, 0.4, 0.64, 0.84)] + [pack]
        half = d_model // 2
        slots = local_experts * window
        n_half = half // WIDE
        r_rows = tok // ROW_BLOCKS
        sub_cols = half // SUBS
        dma = pltpu.SemaphoreType.DMA
        any_spec = pl.BlockSpec(memory_space=pl.ANY)
        vmem_spec = pl.BlockSpec(memory_space=pltpu.VMEM)
        per_ret = dma((SUBS, len(bounds) - 1))
        out = pl.pallas_call(
            functools.partial(moe_kernel, (experts, capacity, window, pack, bounds, local_experts, ep_size)),
            out_shape=jax.ShapeDtypeStruct((tok, d_model), BF16),
            in_specs=[any_spec] * 9 + [vmem_spec] * 2,
            out_specs=any_spec,
            scratch_shapes=[
                pltpu.VMEM((2, tok, d_model), BF16),
                pltpu.VMEM((2 * tok, d_model), BF16),
                pltpu.VMEM((tok, d_model), BF16),
                pltpu.VMEM((ep_size, 8, tok), jnp.int32),
                pltpu.VMEM((ep_size, 8, tok), F32),
                pltpu.VMEM((tok, LANES), F32),
                pltpu.VMEM((tok, LANES), F32),
                pltpu.VMEM((slots, d_model), BF16),
                pltpu.VMEM((n_half, tok, WIDE), F32),
                pltpu.VMEM((ROW_BLOCKS, n_half, r_rows, WIDE), F32),
                pltpu.VMEM((ROW_BLOCKS, n_half, r_rows, WIDE), F32),
                pltpu.VMEM((SUBS, pack_buf, sub_cols), F32),
                pltpu.VMEM((SUBS, pack_buf, sub_cols), F32),
                pltpu.VMEM((SUBS, pack, sub_cols), F32),
                pltpu.VMEM((SUBS, ep_size, pack, sub_cols), BF16),
                pltpu.VMEM((SUBS, tok, sub_cols), BF16),
                pltpu.VMEM((tok, half), BF16),
                pltpu.VMEM((experts, d_model), F32),
                dma((ROW_BLOCKS + 2,)), dma((3,)), dma((3,)), dma((1,)), dma((1,)), dma((X_CHUNKS,)), dma((X_CHUNKS,)), dma((X_CHUNKS,)), dma((X_CHUNKS,)),
                dma((ROW_BLOCKS, n_half)), dma((ROW_BLOCKS, n_half)), per_ret, per_ret, per_ret, per_ret, per_ret, per_ret, per_ret, per_ret,
                dma((SUBS,)), dma((SUBS,)), dma((SUBS,)),
            ],
            compiler_params=pltpu.CompilerParams(collective_id=0, has_side_effects=True, vmem_limit_bytes=67043328),
        )(normed, residual, w_router.T, ws_gate, ws_up, ws_down, jnp.swapaxes(we_gate, 1, 2), jnp.swapaxes(we_up, 1, 2), we_down,
          first_id.reshape(1, tok), alt_id.reshape(1, tok))
        return pl.pallas_call(
            copy_kernel,
            out_shape=jax.ShapeDtypeStruct((tok, d_model), BF16),
            in_specs=[any_spec],
            out_specs=any_spec,
            scratch_shapes=[pltpu.VMEM((tok, d_model), BF16), dma((COPY_CHUNKS,)), dma((COPY_CHUNKS,))],
        )(out)

    return jax.shard_map(device_step, mesh=mesh, in_specs=(tok_spec, tok_spec, P(None, None), P(None, 'tp'), P(None, 'tp'), P('tp', None), P('ep', None, 'tp'), P('ep', None, 'tp'), P('ep', 'tp', None), id_spec, id_spec), out_specs=tok_spec, check_vma=False)
```

```python
import functools

import jax
import jax.numpy as jnp
from jax import lax
from jax.experimental import pallas as pl
from jax.experimental.pallas import tpu as pltpu
from jax.sharding import PartitionSpec as P

MESH = pl.DeviceIdType.MESH
F32 = jnp.float32
BF16 = jnp.bfloat16
LANES = 128
RANK_BLOCK = 256
X_SPLIT = (0, 192, 320, 448, 512)
X_CHUNKS = 4
WIDE = 512
COPY_CHUNKS = 4
ROW_BLOCKS = 2
COL = 256
SUBS = 2
EARLY_GROUPS = 4
SHARED_BUFS = 4


def dot(a, b):
    return jnp.dot(a, b, preferred_element_type=F32)


def dot_bt(a, b):
    return lax.dot_general(a, b, (((1,), (1,)), ((), ())), preferred_element_type=F32)


def dot_at(a, b):
    return lax.dot_general(a, b, (((0,), (0,)), ((), ())), preferred_element_type=F32)


def moe_kernel(dims, x_hbm, res_hbm, wr_hbm, wsg_hbm, wsu_hbm, wsd_hbm, weg_hbm, weu_hbm, wed_hbm, first_ref, alt_ref, o_hbm,
               x_near, x_far, x_sorted, ids_all, code_rows, code_col, gate_col, slot_x, sh_own, sh_send, sh_recv, ex_own, ex_send, ex_recv, ret, out_half, res_half, wr,
               ld_sem, id_send, id_recv, sib_send, sib_recv, xp_send, xp_recv, fw_send, fw_recv,
               ysh_send, ysh_recv, yex_send, yex_recv, rs_send, rs_recv, rx_send, rx_recv, rf_send, rf_recv, yo_send, yo_recv, lo_sem):
    experts, capacity, window, pack, bounds, local_experts, ep_size = dims
    groups = len(bounds) - 1
    last_expert = [-(-min(b, local_experts * capacity) // capacity) - 1 for b in bounds[1:]]
    tok, d_model = x_hbm.shape
    half = d_model // 2
    slots = local_experts * window
    spare = pack - local_experts * capacity
    ff_shared = wsg_hbm.shape[1]
    ff_expert = weg_hbm.shape[1]
    dp = lax.axis_index("dp")
    t = lax.axis_index("tp")
    me = lax.axis_index("ep")
    core = lax.rem(me, 2)
    sib = me + 1 - 2 * core
    xp = lax.rem(me + 2, ep_size)
    diag = lax.rem(sib + 2, ep_size)
    y_peer = (dp, 1 - t, me)
    sib_dev = (dp, t, sib)
    xp_dev = (dp, t, xp)
    diag_dev = (dp, t, diag)
    own_off = pl.multiple_of(t * half, half)
    peer_off = pl.multiple_of((1 - t) * half, half)
    x_cuts = [tok * v // X_SPLIT[-1] for v in X_SPLIT]
    r_rows = tok // ROW_BLOCKS
    n_wide, tail = ff_shared // WIDE, ff_shared % WIDE
    n_chunks = n_wide + (tail > 0)
    n_half = half // WIDE
    sub_cols = half // SUBS
    sub_blocks = sub_cols // WIDE
    sent = -(-local_experts * capacity // 8) * 8

    barrier = pltpu.get_barrier_semaphore()
    for dev in (y_peer, sib_dev, xp_dev, diag_dev):
        pl.semaphore_signal(barrier, inc=1, device_id=dev, device_id_type=MESH)

    def remote(src, dst, s_sem, r_sem, dev):
        return pltpu.make_async_remote_copy(src_ref=src, dst_ref=dst, send_sem=s_sem, recv_sem=r_sem, device_id=dev, device_id_type=MESH)

    id_copies = [remote(ids_all.at[me], ids_all.at[me], id_send.at[i], id_recv.at[i], dev) for i, dev in enumerate((sib_dev, xp_dev, diag_dev))]
    def far_rows(c, i):
        n = x_cuts[c + 1] - x_cuts[c]
        return pl.ds(2 * x_cuts[c] + i * n, n)

    xp_copies = [remote(x_sorted.at[pl.ds(x_cuts[c], x_cuts[c + 1] - x_cuts[c])], x_far.at[far_rows(c, 0)], xp_send.at[c], xp_recv.at[c], xp_dev) for c in range(X_CHUNKS)]
    sib_copy = remote(x_near.at[0], x_near.at[1], sib_send.at[0], sib_recv.at[0], sib_dev)
    fw_copies = [remote(x_far.at[far_rows(c, 0)], x_far.at[far_rows(c, 1)], fw_send.at[c], fw_recv.at[c], sib_dev) for c in range(X_CHUNKS)]
    own_x = [pltpu.make_async_copy(x_hbm.at[pl.ds(r * r_rows, r_rows)], x_near.at[0, pl.ds(r * r_rows, r_rows)], ld_sem.at[r]) for r in range(ROW_BLOCKS)]
    res_load = pltpu.make_async_copy(res_hbm.at[:, pl.ds(own_off, half)], res_half, ld_sem.at[ROW_BLOCKS])
    wr_load = pltpu.make_async_copy(wr_hbm, wr, ld_sem.at[ROW_BLOCKS + 1])

    cap = jnp.float32(capacity)

    def expert_base(ids):
        owner = sum((ids >= q * local_experts).astype(jnp.int32) for q in range(1, ep_size))
        return (ids * capacity + owner * spare).astype(F32)

    def route():
        for copy in id_copies:
            copy.wait()
        e_pad = -(-experts // 8) * 8
        e_iota = lax.broadcasted_iota(jnp.int32, (e_pad, RANK_BLOCK), 0)
        row_i = lax.broadcasted_iota(jnp.int32, (RANK_BLOCK, RANK_BLOCK), 0)
        col_i = lax.broadcasted_iota(jnp.int32, (RANK_BLOCK, RANK_BLOCK), 1)
        upper = (row_i <= col_i).astype(F32).astype(BF16)
        blocks = [(q, b * RANK_BLOCK) for q in range(ep_size) for b in range(tok // RANK_BLOCK)]
        total = jnp.zeros((e_pad, 1), F32)
        rank_first = []
        for q, lo in blocks:
            first = ids_all[q, 0:1, lo:lo + RANK_BLOCK]
            hot = (e_iota == first).astype(F32)
            cum = dot(hot.astype(BF16), upper) + total
            rank_first.append(jnp.sum(cum * hot, axis=0, keepdims=True) - 1.0)
            total = total + jnp.sum(hot, axis=1, keepdims=True)
        load = jnp.minimum(total, cap)
        room = cap - load
        total = jnp.zeros((e_pad, 1), F32)
        for i, (q, lo) in enumerate(blocks):
            first = ids_all[q, 0:1, lo:lo + RANK_BLOCK]
            alt = ids_all[q, 1:2, lo:lo + RANK_BLOCK]
            kept = rank_first[i] < cap
            over = jnp.where(kept, 0.0, 1.0)
            hot = (e_iota == alt).astype(F32) * over
            cum = dot(hot.astype(BF16), upper) + total
            rank_alt = jnp.sum(cum * hot, axis=0, keepdims=True) - 1.0
            total = total + jnp.sum(hot, axis=1, keepdims=True)
            room_tok = jnp.sum(hot * room, axis=0, keepdims=True)
            load_tok = jnp.sum(hot * load, axis=0, keepdims=True)
            code_first = expert_base(first) + rank_first[i]
            code_alt = jnp.where(rank_alt < room_tok, expert_base(alt) + load_tok + rank_alt, -1.0)
            code = jnp.where(kept, code_first, code_alt)
            code_rows[q, :, lo:lo + RANK_BLOCK] = jnp.broadcast_to(code, (8, RANK_BLOCK))

    def sort_block(q):
        code_t = jnp.broadcast_to(code_rows[q][0:1, :], (LANES, tok)).T[:, 0:1]
        shift = ((1 - lax.div(q, 2)) * (2 * pack)).astype(F32)

        def key_of(code):
            rel = code - shift
            local = jnp.where(rel >= pack, rel - pack, rel)
            return jnp.where((rel >= 0.0) & (rel < 2.0 * pack), local, 8192.0)

        key_t = key_of(code_t)
        key = key_of(code_rows[q][0:1, :])
        lane = lax.broadcasted_iota(jnp.int32, (tok, tok), 1)
        line = lax.broadcasted_iota(jnp.int32, (tok, tok), 0)
        ahead = (key < key_t) | ((key == key_t) & (lane < line))
        position = jnp.sum(jnp.where(ahead, 1.0, 0.0), axis=1, keepdims=True)
        return position == lane.astype(F32), code_t

    def dispatch():
        route()
        hit, _ = sort_block(me)
        order = hit.astype(F32).astype(BF16)
        for lo in range(0, d_model, WIDE):
            x_sorted[:, lo:lo + WIDE] = dot_at(order, x_near[0, :, lo:lo + WIDE]).astype(BF16)
        xp_copies[0].start()

    def ysh_copy(r, j):
        if r == 0:
            return remote(sh_send.at[r, j], sh_recv.at[r, j], ysh_send.at[r, j], ysh_recv.at[r, j], y_peer)
        return remote(sh_send.at[r], sh_recv.at[r], ysh_send.at[r, 0], ysh_recv.at[r, 0], y_peer)

    def shared_phase(act, wg, wu, wd, g_sem, u_sem, d_sem):
        def weight_copies(c, slot, width):
            cols = pl.ds(pl.multiple_of(c * WIDE, WIDE), width)
            dst = pl.ds(0, width)
            return (pltpu.make_async_copy(wsg_hbm.at[:, cols], wg.at[slot, :, dst], g_sem.at[slot]),
                    pltpu.make_async_copy(wsu_hbm.at[:, cols], wu.at[slot, :, dst], u_sem.at[slot]))

        def start_weights(k, slot):
            c = lax.rem(k, n_chunks)

            @pl.when(c < n_wide)
            def _():
                for copy in weight_copies(c, slot, WIDE):
                    copy.start()

            if tail:
                @pl.when(c == n_wide)
                def _():
                    for copy in weight_copies(c, slot, tail):
                        copy.start()

        def down_copy(k, slot):
            j = lax.rem(k, 2 * n_half)
            col = jnp.where(j < n_half, peer_off + j * WIDE, own_off + (j - n_half) * WIDE)
            return pltpu.make_async_copy(wsd_hbm.at[:, pl.ds(pl.multiple_of(col, WIDE), WIDE)], wd.at[slot], d_sem.at[slot])

        own_x[0].start()
        start_weights(jnp.int32(0), 0)
        for copy in own_x[1:]:
            copy.start()
        for slot in range(1, SHARED_BUFS):
            start_weights(jnp.int32(slot), slot)
        ids_all[pl.ds(me, 1), 0:1, :] = first_ref[...].reshape(1, 1, tok)
        ids_all[pl.ds(me, 1), 1:2, :] = alt_ref[...].reshape(1, 1, tok)
        def exchange():
            for copy in own_x[1:]:
                copy.wait()
            pl.semaphore_wait(barrier, 4)
            for copy in id_copies:
                copy.start()
            sib_copy.start()

        for r in range(ROW_BLOCKS):
            if r == 0:
                own_x[0].wait()
            def gateup(c, width):
                k = c + r * n_chunks
                slot = lax.rem(k, SHARED_BUFS)
                for copy in weight_copies(c, slot, width):
                    copy.wait()
                x = x_near[0, r * r_rows:(r + 1) * r_rows, :]
                for lo in range(0, width, COL):
                    g = dot(x, wg[slot, :, lo:lo + COL])
                    u = dot(x, wu[slot, :, lo:lo + COL])
                    act[:, pl.ds(pl.multiple_of(c * WIDE + lo, COL), COL)] = (jax.nn.silu(g) * u).astype(BF16)

                @pl.when(k + SHARED_BUFS < (r + 1) * n_chunks)
                def _():
                    start_weights(k + SHARED_BUFS, slot)

            with jax.named_scope(f"gateup{r}"):
                @pl.loop(0, n_wide)
                def _(c):
                    gateup(c, WIDE)

                    if r == 0:
                        @pl.when(c == 0)
                        def _():
                            exchange()

                    if r == 0:
                        @pl.when((c == 1) | (c == 3))
                        def _():
                            slot = lax.div(c, 2)
                            down_copy(slot, slot).start()

                if tail:
                    gateup(jnp.int32(n_wide), tail)

            if r + 1 < ROW_BLOCKS:
                for i in range(SHARED_BUFS):
                    k = (r + 1) * n_chunks + i
                    start_weights(jnp.int32(k), k % SHARED_BUFS)

            def down(j, base, store):
                k = j + r * 2 * n_half + base
                slot = lax.rem(k, 2)
                down_copy(k, slot).wait()
                store(dot(act[...], wd[slot]))

                @pl.when(k + 2 < ROW_BLOCKS * 2 * n_half)
                def _():
                    down_copy(k + 2, slot).start()

            with jax.named_scope(f"downpeer{r}"):
                @pl.loop(0, n_half)
                def _(j):
                    def store(value):
                        sh_send[r, j] = value
                        if r == 0:
                            ysh_copy(r, j).start()

                    down(j, 0, store)

                if r > 0:
                    ysh_copy(r, 0).start()

            if r == 0:
                wr_load.start()
                with jax.named_scope("dispatch"):
                    dispatch()
            with jax.named_scope(f"downown{r}"):
                @pl.loop(0, n_half)
                def _(j):
                    def store(value):
                        sh_own[j, r * r_rows:(r + 1) * r_rows, :] = value

                    down(j, n_half, store)

    shared_sems = [pltpu.SemaphoreType.DMA((SHARED_BUFS,))] * 3
    pl.run_scoped(shared_phase, pltpu.VMEM((r_rows, ff_shared), BF16), pltpu.VMEM((SHARED_BUFS, d_model, WIDE), BF16), pltpu.VMEM((SHARED_BUFS, d_model, WIDE), BF16),
                  pltpu.VMEM((2, ff_shared, WIDE), BF16), *shared_sems)

    def yex_copy(sub, i):
        rows = pl.ds(bounds[i], min(bounds[i + 1], sent) - bounds[i])
        return remote(ex_send.at[sub, rows], ex_recv.at[sub, rows], yex_send.at[sub, i], yex_recv.at[sub, i], y_peer)

    def ret_copy(sub, i, who, s_sem, r_sem, dev):
        ref = ret.at[sub, who, pl.ds(bounds[i], bounds[i + 1] - bounds[i])]
        return remote(ref, ref, s_sem.at[sub, i], r_sem.at[sub, i], dev)

    def give(sub, i):
        yex_copy(sub, i).wait()
        rows = slice(bounds[i], bounds[i + 1])
        ret[sub, pl.ds(me, 1), rows, :] = (ex_own[sub, rows, :] + ex_recv[sub, rows, :]).astype(BF16).reshape(1, bounds[i + 1] - bounds[i], sub_cols)
        ret_copy(sub, i, me, rx_send, rx_recv, xp_dev).start()
        ret_copy(sub, i, me, rs_send, rs_recv, sib_dev).start()

    def forward(sub, i):
        ret_copy(sub, i, me, rx_send, rx_recv, xp_dev).wait()
        ret_copy(sub, i, xp, rf_send, rf_recv, sib_dev).start()

    def routed_phase(sel_near, sel_far, wg, wu, wd, g_sem, u_sem, d_sem):
        def gate_copy(e, slot):
            return pltpu.make_async_copy(weg_hbm.at[e], wg.at[slot], g_sem.at[slot])

        def up_copy(e, slot):
            return pltpu.make_async_copy(weu_hbm.at[e], wu.at[slot], u_sem.at[slot])

        def down_copy(e, slot):
            return pltpu.make_async_copy(wed_hbm.at[e], wd.at[slot], d_sem.at[slot])

        for slot in range(2):
            gate_copy(slot, slot).start()
            up_copy(slot, slot).start()
            down_copy(slot, slot).start()

        res_load.start()
        xp_copies[1].start()
        with jax.named_scope("routing"):
            pos = lax.broadcasted_iota(jnp.int32, (slots, LANES), 0)
            slot_expert = sum((pos >= e * window).astype(jnp.int32) for e in range(1, local_experts))
            first_row = slot_expert * capacity
            row = (first_row // 8) * 8 + (pos - slot_expert * window)
            slot_code = jnp.where((row >= first_row) & (row < first_row + capacity), row + me * pack, -2).astype(F32)
            def pick_rows(codes):
                return (jnp.broadcast_to(slot_code[:, 0:1], (slots, codes.shape[1])) == codes).astype(F32).astype(BF16)

            for i, q in enumerate((me, sib)):
                codes = code_rows[q]
                for lo in range(0, tok, LANES):
                    sel_near[:, i * tok + lo:i * tok + lo + LANES] = pick_rows(codes[0:1, lo:lo + LANES])
            def sorted_codes(q):
                hit, code_t = sort_block(q)
                return jnp.sum(jnp.where(hit, code_t, 0.0), axis=0, keepdims=True)

            codes_xp, codes_diag = sorted_codes(xp), sorted_codes(diag)
            for c in range(X_CHUNKS):
                both = jnp.concatenate([codes_xp[:, x_cuts[c]:x_cuts[c + 1]], codes_diag[:, x_cuts[c]:x_cuts[c + 1]]], axis=1)
                for lo in range(0, 2 * (x_cuts[c + 1] - x_cuts[c]), LANES):
                    dst = 2 * x_cuts[c] + lo
                    sel_far[:, dst:dst + LANES] = pick_rows(both[:, lo:lo + LANES])

            code_t = jnp.broadcast_to(code_rows[me][0:1, :], (LANES, tok)).T
            code_col[...] = code_t

        nc = 512
        with jax.named_scope("near"):
            sib_copy.wait()

            @pl.loop(0, d_model // nc)
            def _(n):
                cols = pl.ds(pl.multiple_of(n * nc, nc), nc)
                slot_x[:, cols] = dot(sel_near[...], x_near[:, :, cols].reshape(2 * tok, nc)).astype(BF16)

        def pass_on(c):
            if c == X_CHUNKS - 2:
                xp_copies[c].wait_send()
                xp_copies[c + 1].start()
            xp_copies[c].wait_recv()
            fw_copies[c].start()

        def gather(c):
            fw_copies[c].wait_recv()

            @pl.loop(0, d_model // nc)
            def _(n):
                cols = pl.ds(pl.multiple_of(n * nc, nc), nc)
                span = slice(2 * x_cuts[c], 2 * x_cuts[c + 1])
                slot_x[:, cols] += dot(sel_far[:, span], x_far[span, cols]).astype(BF16)

        pass_on(0)
        with jax.named_scope("router"):
            wr_load.wait()
            x = x_near[0]
            w = wr[...]
            w_hi = w.astype(BF16)
            w_rest = w - w_hi.astype(F32)
            w_mid = w_rest.astype(BF16)
            w_lo = (w_rest - w_mid.astype(F32)).astype(BF16)
            logits = dot_bt(x, w_hi) + (dot_bt(x, w_mid) + dot_bt(x, w_lo))
            top = jnp.max(logits, axis=1, keepdims=True)
            prob = jnp.exp(logits - top)
            denom = jnp.sum(prob, axis=1, keepdims=True)
            lane_lo = expert_base(lax.broadcasted_iota(jnp.int32, (tok, experts), 1))
            code_e = code_col[:, 0:experts]
            picked = (code_e >= lane_lo) & (code_e < lane_lo + cap)
            gate = jnp.sum(jnp.where(picked, prob, 0.0), axis=1, keepdims=True) / denom
            gate_col[...] = jnp.broadcast_to(gate, (tok, LANES))

        with jax.named_scope("far0"):
            gather(0)

        pass_at = [0, 1, 3, 4]
        loop_steps = [(5, give, 0, 0), (5, give, 1, 0), (6, give, 0, 1), (7, forward, 0, 0), (7, give, 1, 1), (8, forward, 1, 0), (9, forward, 0, 1), (9, give, 0, 2),
                      (10, forward, 1, 1), (11, forward, 0, 2), (11, give, 1, 2), (13, forward, 1, 2), (14, give, 0, 3)]
        far_at = [x_cuts[c] // (2 * capacity) for c in range(X_CHUNKS)]
        if sent < pack:
            for sub in range(SUBS):
                ex_recv[sub, sent:pack, :] = jnp.zeros((pack - sent, sub_cols), F32)

        with jax.named_scope("experts"):
            for sub in range(SUBS):
                ex_send[sub, 0:8, :] = jnp.zeros((8, sub_cols), F32)
                ex_own[sub, 0:8, :] = jnp.zeros((8, sub_cols), F32)

            @pl.loop(0, local_experts)
            def _(e):
                slot = lax.rem(e, 2)
                @pl.when(e == 0)
                def _():
                    xp_copies[2].start()

                for c in range(1, X_CHUNKS):
                    @pl.when(e == pass_at[c])
                    def _():
                        pass_on(c)

                    @pl.when(e == far_at[c])
                    def _():
                        with jax.named_scope(f"far{c}"):
                            gather(c)

                gate_copy(e, slot).wait()
                up_copy(e, slot).wait()
                rows = slot_x[pl.ds(pl.multiple_of(e * window, window), window), :]
                g = dot_bt(wg[slot], rows)
                u = dot_bt(wu[slot], rows)
                hidden = (jax.nn.silu(g) * u).astype(BF16)

                @pl.when(e + 2 < local_experts)
                def _():
                    gate_copy(e + 2, slot).start()
                    up_copy(e + 2, slot).start()

                down_copy(e, slot).wait()
                row = pl.multiple_of((e * capacity) // 8 * 8, 8)
                for buf, off in ((ex_send, peer_off), (ex_own, own_off)):
                    value = dot_at(hidden, wd[slot, :, pl.ds(off, half)])
                    for sub in range(SUBS):
                        part = value[:, sub * sub_cols:(sub + 1) * sub_cols]
                        buf[sub, pl.ds(row, 8), :] += part[0:8]
                        buf[sub, pl.ds(row + 8, window - 8), :] = part[8:]

                @pl.when(e + 2 < local_experts)
                def _():
                    down_copy(e + 2, slot).start()

                for i in range(groups):
                    @pl.when(e == last_expert[i])
                    def _():
                        yex_copy(0, i).start()
                        if i < EARLY_GROUPS:
                            yex_copy(1, i).start()

                for when, action, sub, i in loop_steps:
                    @pl.when(e == when)
                    def _():
                        action(sub, i)

            for i in range(EARLY_GROUPS, groups):
                yex_copy(1, i).start()

    pl.run_scoped(routed_phase, pltpu.VMEM((slots, 2 * tok), BF16), pltpu.VMEM((slots, 2 * tok), BF16),
                  pltpu.VMEM((2, ff_expert, d_model), BF16), pltpu.VMEM((2, ff_expert, d_model), BF16),
                  pltpu.VMEM((2, ff_expert, d_model), BF16), pltpu.SemaphoreType.DMA((2,)), pltpu.SemaphoreType.DMA((2,)), pltpu.SemaphoreType.DMA((2,)))

    with jax.named_scope("fin_shared"):
        for copy in xp_copies[:-2] + xp_copies[-1:] + fw_copies:
            copy.wait_send()
        res_load.wait()
        for r in range(ROW_BLOCKS):
            if r > 0:
                ysh_copy(r, 0).wait()

            @pl.loop(0, n_half)
            def _(j):
                if r == 0:
                    ysh_copy(r, j).wait()
                cols = pl.ds(pl.multiple_of(j * WIDE, WIDE), WIDE)
                rows = slice(r * r_rows, (r + 1) * r_rows)
                sh_own[j, rows, :] = res_half[rows, cols].astype(F32) + (sh_own[j, rows, :] + sh_recv[r, j])

    def combine(pick, sub, i):
        n = bounds[i + 1] - bounds[i]
        lanes = slice(ep_size * bounds[i], ep_size * bounds[i + 1])
        if sub == 0:
            lane = lax.broadcasted_iota(jnp.int32, (tok, ep_size * n), 1)
            owner = sum((lane >= q * n).astype(jnp.int32) for q in range(1, ep_size))
            lane_code = (lane + owner * (pack - n) + bounds[i]).astype(F32)
            pick[:, lanes] = (code_col[:, 0:1] == lane_code).astype(F32).astype(BF16)
        ret_copy(sub, i, me, rs_send, rs_recv, sib_dev).wait()
        ret_copy(sub, i, xp, rf_send, rf_recv, sib_dev).wait()
        rows = ret[sub, :, bounds[i]:bounds[i + 1], :].reshape(ep_size * n, sub_cols)
        gate = gate_col[:, 0:1]
        for j in range(sub_blocks):
            jj = sub * sub_blocks + j
            sh_own[jj] = sh_own[jj] + gate * dot(pick[:, lanes], rows[:, j * WIDE:(j + 1) * WIDE])

    def out_copies(sub):
        src = out_half.at[sub]
        dst = o_hbm.at[:, pl.ds(pl.multiple_of(own_off + sub * sub_cols, sub_cols), sub_cols)]
        return remote(src, dst, yo_send.at[sub], yo_recv.at[sub], y_peer), pltpu.make_async_copy(src, dst, lo_sem.at[sub])

    def emit(sub):
        for j in range(sub_blocks):
            out_half[sub, :, j * WIDE:(j + 1) * WIDE] = sh_own[sub * sub_blocks + j].astype(BF16)

    def start_out(sub):
        for copy in out_copies(sub):
            copy.start()

    def return_phase(pick):
        steps = [(combine, 0, 0), (combine, 1, 0), (combine, 0, 1), (combine, 1, 1), (combine, 0, 2), (combine, 1, 2), (give, 1, 3), (forward, 0, 3),
                 (combine, 0, 3), (forward, 1, 3), (give, 0, 4), (combine, 1, 3), (forward, 0, 4), (give, 0, 5), (combine, 0, 4), (forward, 0, 5),
                 (combine, 0, 5), (emit, 0), (start_out, 0), (give, 1, 4), (forward, 1, 4), (give, 1, 5), (combine, 1, 4), (forward, 1, 5), (combine, 1, 5), (emit, 1), (start_out, 1)]
        for step in steps:
            with jax.named_scope(step[0].__name__ + "".join(str(a) for a in step[1:])):
                if step[0] is combine:
                    combine(pick, *step[1:])
                else:
                    step[0](*step[1:])

    pl.run_scoped(return_phase, pltpu.VMEM((tok, ep_size * pack), BF16))

    with jax.named_scope("out"):
        for sub in range(SUBS):
            for copy in out_copies(sub):
                copy.wait()


def copy_kernel(src, dst, buf, in_sem, out_sem):
    n = src.shape[0] // COPY_CHUNKS
    reads = [pltpu.make_async_copy(src.at[pl.ds(c * n, n)], buf.at[pl.ds(c * n, n)], in_sem.at[c]) for c in range(COPY_CHUNKS)]
    writes = [pltpu.make_async_copy(buf.at[pl.ds(c * n, n)], dst.at[pl.ds(c * n, n)], out_sem.at[c]) for c in range(COPY_CHUNKS)]
    for copy in reads:
        copy.start()
    for read, write in zip(reads, writes):
        read.wait()
        write.start()
    for copy in writes:
        copy.wait()


def solution(mesh):
    ep_size = mesh.shape["ep"]
    tok_spec = P(("dp", "ep"), None)
    id_spec = P(("dp", "ep"))

    def device_step(normed, residual, w_router, ws_gate, ws_up, ws_down, we_gate, we_up, we_down, first_id, alt_id):
        tok, d_model = normed.shape
        local_experts, _, ff_expert = we_gate.shape
        experts = local_experts * ep_size
        capacity = (5 * tok * ep_size + 4 * experts - 1) // (4 * experts)
        window = -(-(capacity + 7) // 16) * 16
        pack = -(-local_experts * capacity // 16) * 16
        pack_buf = max(pack, (local_experts - 1) * capacity // 8 * 8 + window)
        bounds = [0] + [int(pack * f) // 32 * 32 for f in (0.13, 0.255, 0.4, 0.64, 0.84)] + [pack]
        half = d_model // 2
        slots = local_experts * window
        n_half = half // WIDE
        r_rows = tok // ROW_BLOCKS
        sub_cols = half // SUBS
        dma = pltpu.SemaphoreType.DMA
        any_spec = pl.BlockSpec(memory_space=pl.ANY)
        vmem_spec = pl.BlockSpec(memory_space=pltpu.VMEM)
        per_ret = dma((SUBS, len(bounds) - 1))
        out = pl.pallas_call(
            functools.partial(moe_kernel, (experts, capacity, window, pack, bounds, local_experts, ep_size)),
            out_shape=jax.ShapeDtypeStruct((tok, d_model), BF16),
            in_specs=[any_spec] * 9 + [vmem_spec] * 2,
            out_specs=any_spec,
            scratch_shapes=[
                pltpu.VMEM((2, tok, d_model), BF16),
                pltpu.VMEM((2 * tok, d_model), BF16),
                pltpu.VMEM((tok, d_model), BF16),
                pltpu.VMEM((ep_size, 8, tok), jnp.int32),
                pltpu.VMEM((ep_size, 8, tok), F32),
                pltpu.VMEM((tok, LANES), F32),
                pltpu.VMEM((tok, LANES), F32),
                pltpu.VMEM((slots, d_model), BF16),
                pltpu.VMEM((n_half, tok, WIDE), F32),
                pltpu.VMEM((ROW_BLOCKS, n_half, r_rows, WIDE), F32),
                pltpu.VMEM((ROW_BLOCKS, n_half, r_rows, WIDE), F32),
                pltpu.VMEM((SUBS, pack_buf, sub_cols), F32),
                pltpu.VMEM((SUBS, pack_buf, sub_cols), F32),
                pltpu.VMEM((SUBS, pack, sub_cols), F32),
                pltpu.VMEM((SUBS, ep_size, pack, sub_cols), BF16),
                pltpu.VMEM((SUBS, tok, sub_cols), BF16),
                pltpu.VMEM((tok, half), BF16),
                pltpu.VMEM((experts, d_model), F32),
                dma((ROW_BLOCKS + 2,)), dma((3,)), dma((3,)), dma((1,)), dma((1,)), dma((X_CHUNKS,)), dma((X_CHUNKS,)), dma((X_CHUNKS,)), dma((X_CHUNKS,)),
                dma((ROW_BLOCKS, n_half)), dma((ROW_BLOCKS, n_half)), per_ret, per_ret, per_ret, per_ret, per_ret, per_ret, per_ret, per_ret,
                dma((SUBS,)), dma((SUBS,)), dma((SUBS,)),
            ],
            compiler_params=pltpu.CompilerParams(collective_id=0, has_side_effects=True, vmem_limit_bytes=67043328),
        )(normed, residual, w_router.T, ws_gate, ws_up, ws_down, jnp.swapaxes(we_gate, 1, 2), jnp.swapaxes(we_up, 1, 2), we_down,
          first_id.reshape(1, tok), alt_id.reshape(1, tok))
        return pl.pallas_call(
            copy_kernel,
            out_shape=jax.ShapeDtypeStruct((tok, d_model), BF16),
            in_specs=[any_spec],
            out_specs=any_spec,
            scratch_shapes=[pltpu.VMEM((tok, d_model), BF16), dma((COPY_CHUNKS,)), dma((COPY_CHUNKS,))],
        )(out)

    return jax.shard_map(device_step, mesh=mesh, in_specs=(tok_spec, tok_spec, P(None, None), P(None, 'tp'), P(None, 'tp'), P('tp', None), P('ep', None, 'tp'), P('ep', None, 'tp'), P('ep', 'tp', None), id_spec, id_spec), out_specs=tok_spec, check_vma=False)
```

```python
import functools

import jax
import jax.numpy as jnp
from jax import lax
from jax.experimental import pallas as pl
from jax.experimental.pallas import tpu as pltpu
from jax.sharding import PartitionSpec as P

MESH = pl.DeviceIdType.MESH
F32 = jnp.float32
BF16 = jnp.bfloat16
LANES = 128
RANK_BLOCK = 256
X_SPLIT = (0, 192, 320, 448, 512)
X_CHUNKS = 4
WIDE = 512
COPY_CHUNKS = 8
ROW_BLOCKS = 2
COL = 256
SUBS = 2
EARLY_GROUPS = 4
SHARED_BUFS = 4


def dot(a, b):
    return jnp.dot(a, b, preferred_element_type=F32)


def dot_bt(a, b):
    return lax.dot_general(a, b, (((1,), (1,)), ((), ())), preferred_element_type=F32)


def dot_at(a, b):
    return lax.dot_general(a, b, (((0,), (0,)), ((), ())), preferred_element_type=F32)


def moe_kernel(dims, x_hbm, res_hbm, wr_hbm, wsg_hbm, wsu_hbm, wsd_hbm, weg_hbm, weu_hbm, wed_hbm, first_ref, alt_ref, o_hbm,
               x_near, x_far, x_sorted, ids_all, code_rows, code_col, gate_col, slot_x, sh_own, sh_send, sh_recv, ex_own, ex_send, ex_recv, ret, out_half, res_half, wr,
               ld_sem, id_send, id_recv, sib_send, sib_recv, xp_send, xp_recv, fw_send, fw_recv,
               ysh_send, ysh_recv, yex_send, yex_recv, rs_send, rs_recv, rx_send, rx_recv, rf_send, rf_recv, yo_send, yo_recv, lo_sem):
    experts, capacity, window, pack, bounds, local_experts, ep_size = dims
    groups = len(bounds) - 1
    last_expert = [-(-min(b, local_experts * capacity) // capacity) - 1 for b in bounds[1:]]
    tok, d_model = x_hbm.shape
    half = d_model // 2
    slots = local_experts * window
    spare = pack - local_experts * capacity
    ff_shared = wsg_hbm.shape[1]
    ff_expert = weg_hbm.shape[1]
    dp = lax.axis_index("dp")
    t = lax.axis_index("tp")
    me = lax.axis_index("ep")
    core = lax.rem(me, 2)
    sib = me + 1 - 2 * core
    xp = lax.rem(me + 2, ep_size)
    diag = lax.rem(sib + 2, ep_size)
    y_peer = (dp, 1 - t, me)
    sib_dev = (dp, t, sib)
    xp_dev = (dp, t, xp)
    diag_dev = (dp, t, diag)
    own_off = pl.multiple_of(t * half, half)
    peer_off = pl.multiple_of((1 - t) * half, half)
    x_cuts = [tok * v // X_SPLIT[-1] for v in X_SPLIT]
    r_rows = tok // ROW_BLOCKS
    n_wide, tail = ff_shared // WIDE, ff_shared % WIDE
    n_chunks = n_wide + (tail > 0)
    n_half = half // WIDE
    sub_cols = half // SUBS
    sub_blocks = sub_cols // WIDE
    sent = -(-local_experts * capacity // 8) * 8

    barrier = pltpu.get_barrier_semaphore()
    for dev in (y_peer, sib_dev, xp_dev, diag_dev):
        pl.semaphore_signal(barrier, inc=1, device_id=dev, device_id_type=MESH)

    def remote(src, dst, s_sem, r_sem, dev):
        return pltpu.make_async_remote_copy(src_ref=src, dst_ref=dst, send_sem=s_sem, recv_sem=r_sem, device_id=dev, device_id_type=MESH)

    id_copies = [remote(ids_all.at[me], ids_all.at[me], id_send.at[i], id_recv.at[i], dev) for i, dev in enumerate((sib_dev, xp_dev, diag_dev))]
    def far_rows(c, i):
        n = x_cuts[c + 1] - x_cuts[c]
        return pl.ds(2 * x_cuts[c] + i * n, n)

    xp_copies = [remote(x_sorted.at[pl.ds(x_cuts[c], x_cuts[c + 1] - x_cuts[c])], x_far.at[far_rows(c, 0)], xp_send.at[c], xp_recv.at[c], xp_dev) for c in range(X_CHUNKS)]
    sib_copy = remote(x_near.at[0], x_near.at[1], sib_send.at[0], sib_recv.at[0], sib_dev)
    fw_copies = [remote(x_far.at[far_rows(c, 0)], x_far.at[far_rows(c, 1)], fw_send.at[c], fw_recv.at[c], sib_dev) for c in range(X_CHUNKS)]
    own_x = [pltpu.make_async_copy(x_hbm.at[pl.ds(r * r_rows, r_rows)], x_near.at[0, pl.ds(r * r_rows, r_rows)], ld_sem.at[r]) for r in range(ROW_BLOCKS)]
    res_load = pltpu.make_async_copy(res_hbm.at[:, pl.ds(own_off, half)], res_half, ld_sem.at[ROW_BLOCKS])
    wr_load = pltpu.make_async_copy(wr_hbm, wr, ld_sem.at[ROW_BLOCKS + 1])

    cap = jnp.float32(capacity)

    def expert_base(ids):
        owner = sum((ids >= q * local_experts).astype(jnp.int32) for q in range(1, ep_size))
        return (ids * capacity + owner * spare).astype(F32)

    def route():
        for copy in id_copies:
            copy.wait()
        e_pad = -(-experts // 8) * 8
        e_iota = lax.broadcasted_iota(jnp.int32, (e_pad, RANK_BLOCK), 0)
        row_i = lax.broadcasted_iota(jnp.int32, (RANK_BLOCK, RANK_BLOCK), 0)
        col_i = lax.broadcasted_iota(jnp.int32, (RANK_BLOCK, RANK_BLOCK), 1)
        upper = (row_i <= col_i).astype(F32).astype(BF16)
        blocks = [(q, b * RANK_BLOCK) for q in range(ep_size) for b in range(tok // RANK_BLOCK)]
        total = jnp.zeros((e_pad, 1), F32)
        rank_first = []
        for q, lo in blocks:
            first = ids_all[q, 0:1, lo:lo + RANK_BLOCK]
            hot = (e_iota == first).astype(F32)
            cum = dot(hot.astype(BF16), upper) + total
            rank_first.append(jnp.sum(cum * hot, axis=0, keepdims=True) - 1.0)
            total = total + jnp.sum(hot, axis=1, keepdims=True)
        load = jnp.minimum(total, cap)
        room = cap - load
        total = jnp.zeros((e_pad, 1), F32)
        for i, (q, lo) in enumerate(blocks):
            first = ids_all[q, 0:1, lo:lo + RANK_BLOCK]
            alt = ids_all[q, 1:2, lo:lo + RANK_BLOCK]
            kept = rank_first[i] < cap
            over = jnp.where(kept, 0.0, 1.0)
            hot = (e_iota == alt).astype(F32) * over
            cum = dot(hot.astype(BF16), upper) + total
            rank_alt = jnp.sum(cum * hot, axis=0, keepdims=True) - 1.0
            total = total + jnp.sum(hot, axis=1, keepdims=True)
            room_tok = jnp.sum(hot * room, axis=0, keepdims=True)
            load_tok = jnp.sum(hot * load, axis=0, keepdims=True)
            code_first = expert_base(first) + rank_first[i]
            code_alt = jnp.where(rank_alt < room_tok, expert_base(alt) + load_tok + rank_alt, -1.0)
            code = jnp.where(kept, code_first, code_alt)
            code_rows[q, :, lo:lo + RANK_BLOCK] = jnp.broadcast_to(code, (8, RANK_BLOCK))

    def sort_block(q):
        code_t = jnp.broadcast_to(code_rows[q][0:1, :], (LANES, tok)).T[:, 0:1]
        shift = ((1 - lax.div(q, 2)) * (2 * pack)).astype(F32)

        def key_of(code):
            rel = code - shift
            local = jnp.where(rel >= pack, rel - pack, rel)
            return jnp.where((rel >= 0.0) & (rel < 2.0 * pack), local, 8192.0)

        key_t = key_of(code_t)
        key = key_of(code_rows[q][0:1, :])
        lane = lax.broadcasted_iota(jnp.int32, (tok, tok), 1)
        line = lax.broadcasted_iota(jnp.int32, (tok, tok), 0)
        ahead = (key < key_t) | ((key == key_t) & (lane < line))
        position = jnp.sum(jnp.where(ahead, 1.0, 0.0), axis=1, keepdims=True)
        return position == lane.astype(F32), code_t

    def dispatch():
        route()
        hit, _ = sort_block(me)
        order = hit.astype(F32).astype(BF16)
        for lo in range(0, d_model, WIDE):
            x_sorted[:, lo:lo + WIDE] = dot_at(order, x_near[0, :, lo:lo + WIDE]).astype(BF16)
        xp_copies[0].start()

    def ysh_copy(r, j):
        if r == 0:
            return remote(sh_send.at[r, j], sh_recv.at[r, j], ysh_send.at[r, j], ysh_recv.at[r, j], y_peer)
        return remote(sh_send.at[r], sh_recv.at[r], ysh_send.at[r, 0], ysh_recv.at[r, 0], y_peer)

    def shared_phase(act, wg, wu, wd, g_sem, u_sem, d_sem):
        def weight_copies(c, slot, width):
            cols = pl.ds(pl.multiple_of(c * WIDE, WIDE), width)
            dst = pl.ds(0, width)
            return (pltpu.make_async_copy(wsg_hbm.at[:, cols], wg.at[slot, :, dst], g_sem.at[slot]),
                    pltpu.make_async_copy(wsu_hbm.at[:, cols], wu.at[slot, :, dst], u_sem.at[slot]))

        def start_weights(k, slot):
            c = lax.rem(k, n_chunks)

            @pl.when(c < n_wide)
            def _():
                for copy in weight_copies(c, slot, WIDE):
                    copy.start()

            if tail:
                @pl.when(c == n_wide)
                def _():
                    for copy in weight_copies(c, slot, tail):
                        copy.start()

        def down_copy(k, slot):
            j = lax.rem(k, 2 * n_half)
            col = jnp.where(j < n_half, peer_off + j * WIDE, own_off + (j - n_half) * WIDE)
            return pltpu.make_async_copy(wsd_hbm.at[:, pl.ds(pl.multiple_of(col, WIDE), WIDE)], wd.at[slot], d_sem.at[slot])

        own_x[0].start()
        start_weights(jnp.int32(0), 0)
        for copy in own_x[1:]:
            copy.start()
        for slot in range(1, SHARED_BUFS):
            start_weights(jnp.int32(slot), slot)
        ids_all[pl.ds(me, 1), 0:1, :] = first_ref[...].reshape(1, 1, tok)
        ids_all[pl.ds(me, 1), 1:2, :] = alt_ref[...].reshape(1, 1, tok)
        def exchange():
            for copy in own_x[1:]:
                copy.wait()
            pl.semaphore_wait(barrier, 4)
            for copy in id_copies:
                copy.start()
            sib_copy.start()

        for r in range(ROW_BLOCKS):
            if r == 0:
                own_x[0].wait()
            def gateup(c, width):
                k = c + r * n_chunks
                slot = lax.rem(k, SHARED_BUFS)
                for copy in weight_copies(c, slot, width):
                    copy.wait()
                x = x_near[0, r * r_rows:(r + 1) * r_rows, :]
                for lo in range(0, width, COL):
                    g = dot(x, wg[slot, :, lo:lo + COL])
                    u = dot(x, wu[slot, :, lo:lo + COL])
                    act[:, pl.ds(pl.multiple_of(c * WIDE + lo, COL), COL)] = (jax.nn.silu(g) * u).astype(BF16)

                @pl.when(k + SHARED_BUFS < (r + 1) * n_chunks)
                def _():
                    start_weights(k + SHARED_BUFS, slot)

            with jax.named_scope(f"gateup{r}"):
                @pl.loop(0, n_wide)
                def _(c):
                    gateup(c, WIDE)

                    if r == 0:
                        @pl.when(c == 0)
                        def _():
                            exchange()

                    if r == 0:
                        @pl.when((c == 1) | (c == 3))
                        def _():
                            slot = lax.div(c, 2)
                            down_copy(slot, slot).start()

                if tail:
                    gateup(jnp.int32(n_wide), tail)

            if r + 1 < ROW_BLOCKS:
                for i in range(SHARED_BUFS):
                    k = (r + 1) * n_chunks + i
                    start_weights(jnp.int32(k), k % SHARED_BUFS)

            def down(j, base, store):
                k = j + r * 2 * n_half + base
                slot = lax.rem(k, 2)
                down_copy(k, slot).wait()
                store(dot(act[...], wd[slot]))

                @pl.when(k + 2 < ROW_BLOCKS * 2 * n_half)
                def _():
                    down_copy(k + 2, slot).start()

            with jax.named_scope(f"downpeer{r}"):
                @pl.loop(0, n_half)
                def _(j):
                    def store(value):
                        sh_send[r, j] = value
                        if r == 0:
                            ysh_copy(r, j).start()

                    down(j, 0, store)

                if r > 0:
                    ysh_copy(r, 0).start()

            if r == 0:
                wr_load.start()
                with jax.named_scope("dispatch"):
                    dispatch()
            with jax.named_scope(f"downown{r}"):
                @pl.loop(0, n_half)
                def _(j):
                    def store(value):
                        sh_own[j, r * r_rows:(r + 1) * r_rows, :] = value

                    down(j, n_half, store)

    shared_sems = [pltpu.SemaphoreType.DMA((SHARED_BUFS,))] * 3
    pl.run_scoped(shared_phase, pltpu.VMEM((r_rows, ff_shared), BF16), pltpu.VMEM((SHARED_BUFS, d_model, WIDE), BF16), pltpu.VMEM((SHARED_BUFS, d_model, WIDE), BF16),
                  pltpu.VMEM((2, ff_shared, WIDE), BF16), *shared_sems)

    def yex_copy(sub, i):
        rows = pl.ds(bounds[i], min(bounds[i + 1], sent) - bounds[i])
        return remote(ex_send.at[sub, rows], ex_recv.at[sub, rows], yex_send.at[sub, i], yex_recv.at[sub, i], y_peer)

    def ret_copy(sub, i, who, s_sem, r_sem, dev):
        ref = ret.at[sub, who, pl.ds(bounds[i], bounds[i + 1] - bounds[i])]
        return remote(ref, ref, s_sem.at[sub, i], r_sem.at[sub, i], dev)

    def give(sub, i):
        yex_copy(sub, i).wait()
        rows = slice(bounds[i], bounds[i + 1])
        ret[sub, pl.ds(me, 1), rows, :] = (ex_own[sub, rows, :] + ex_recv[sub, rows, :]).astype(BF16).reshape(1, bounds[i + 1] - bounds[i], sub_cols)
        ret_copy(sub, i, me, rx_send, rx_recv, xp_dev).start()
        ret_copy(sub, i, me, rs_send, rs_recv, sib_dev).start()

    def forward(sub, i):
        ret_copy(sub, i, me, rx_send, rx_recv, xp_dev).wait()
        ret_copy(sub, i, xp, rf_send, rf_recv, sib_dev).start()

    def routed_phase(sel_near, sel_far, wg, wu, wd, g_sem, u_sem, d_sem):
        def gate_copy(e, slot):
            return pltpu.make_async_copy(weg_hbm.at[e], wg.at[slot], g_sem.at[slot])

        def up_copy(e, slot):
            return pltpu.make_async_copy(weu_hbm.at[e], wu.at[slot], u_sem.at[slot])

        def down_copy(e, slot):
            return pltpu.make_async_copy(wed_hbm.at[e], wd.at[slot], d_sem.at[slot])

        for slot in range(2):
            gate_copy(slot, slot).start()
            up_copy(slot, slot).start()
            down_copy(slot, slot).start()

        res_load.start()
        xp_copies[1].start()
        with jax.named_scope("routing"):
            pos = lax.broadcasted_iota(jnp.int32, (slots, LANES), 0)
            slot_expert = sum((pos >= e * window).astype(jnp.int32) for e in range(1, local_experts))
            first_row = slot_expert * capacity
            row = (first_row // 8) * 8 + (pos - slot_expert * window)
            slot_code = jnp.where((row >= first_row) & (row < first_row + capacity), row + me * pack, -2).astype(F32)
            def pick_rows(codes):
                return (jnp.broadcast_to(slot_code[:, 0:1], (slots, codes.shape[1])) == codes).astype(F32).astype(BF16)

            for i, q in enumerate((me, sib)):
                codes = code_rows[q]
                for lo in range(0, tok, LANES):
                    sel_near[:, i * tok + lo:i * tok + lo + LANES] = pick_rows(codes[0:1, lo:lo + LANES])
            def sorted_codes(q):
                hit, code_t = sort_block(q)
                return jnp.sum(jnp.where(hit, code_t, 0.0), axis=0, keepdims=True)

            codes_xp, codes_diag = sorted_codes(xp), sorted_codes(diag)
            for c in range(X_CHUNKS):
                both = jnp.concatenate([codes_xp[:, x_cuts[c]:x_cuts[c + 1]], codes_diag[:, x_cuts[c]:x_cuts[c + 1]]], axis=1)
                for lo in range(0, 2 * (x_cuts[c + 1] - x_cuts[c]), LANES):
                    dst = 2 * x_cuts[c] + lo
                    sel_far[:, dst:dst + LANES] = pick_rows(both[:, lo:lo + LANES])

            code_t = jnp.broadcast_to(code_rows[me][0:1, :], (LANES, tok)).T
            code_col[...] = code_t

        nc = 512
        with jax.named_scope("near"):
            sib_copy.wait()

            @pl.loop(0, d_model // nc)
            def _(n):
                cols = pl.ds(pl.multiple_of(n * nc, nc), nc)
                slot_x[:, cols] = dot(sel_near[...], x_near[:, :, cols].reshape(2 * tok, nc)).astype(BF16)

        def pass_on(c):
            if c == X_CHUNKS - 2:
                xp_copies[c].wait_send()
                xp_copies[c + 1].start()
            xp_copies[c].wait_recv()
            fw_copies[c].start()

        def gather(c):
            fw_copies[c].wait_recv()

            @pl.loop(0, d_model // nc)
            def _(n):
                cols = pl.ds(pl.multiple_of(n * nc, nc), nc)
                span = slice(2 * x_cuts[c], 2 * x_cuts[c + 1])
                slot_x[:, cols] += dot(sel_far[:, span], x_far[span, cols]).astype(BF16)

        pass_on(0)
        with jax.named_scope("router"):
            wr_load.wait()
            x = x_near[0]
            w = wr[...]
            w_hi = w.astype(BF16)
            w_rest = w - w_hi.astype(F32)
            w_mid = w_rest.astype(BF16)
            w_lo = (w_rest - w_mid.astype(F32)).astype(BF16)
            logits = dot_bt(x, w_hi) + (dot_bt(x, w_mid) + dot_bt(x, w_lo))
            top = jnp.max(logits, axis=1, keepdims=True)
            prob = jnp.exp(logits - top)
            denom = jnp.sum(prob, axis=1, keepdims=True)
            lane_lo = expert_base(lax.broadcasted_iota(jnp.int32, (tok, experts), 1))
            code_e = code_col[:, 0:experts]
            picked = (code_e >= lane_lo) & (code_e < lane_lo + cap)
            gate = jnp.sum(jnp.where(picked, prob, 0.0), axis=1, keepdims=True) / denom
            gate_col[...] = jnp.broadcast_to(gate, (tok, LANES))

        with jax.named_scope("far0"):
            gather(0)

        pass_at = [0, 1, 3, 4]
        loop_steps = [(5, give, 0, 0), (5, give, 1, 0), (6, give, 0, 1), (7, forward, 0, 0), (7, give, 1, 1), (8, forward, 1, 0), (9, forward, 0, 1), (9, give, 0, 2),
                      (10, forward, 1, 1), (11, forward, 0, 2), (11, give, 1, 2), (13, forward, 1, 2), (14, give, 0, 3)]
        far_at = [x_cuts[c] // (2 * capacity) for c in range(X_CHUNKS)]
        if sent < pack:
            for sub in range(SUBS):
                ex_recv[sub, sent:pack, :] = jnp.zeros((pack - sent, sub_cols), F32)

        with jax.named_scope("experts"):
            for sub in range(SUBS):
                ex_send[sub, 0:8, :] = jnp.zeros((8, sub_cols), F32)
                ex_own[sub, 0:8, :] = jnp.zeros((8, sub_cols), F32)

            @pl.loop(0, local_experts)
            def _(e):
                slot = lax.rem(e, 2)
                @pl.when(e == 0)
                def _():
                    xp_copies[2].start()

                for c in range(1, X_CHUNKS):
                    @pl.when(e == pass_at[c])
                    def _():
                        pass_on(c)

                    @pl.when(e == far_at[c])
                    def _():
                        with jax.named_scope(f"far{c}"):
                            gather(c)

                gate_copy(e, slot).wait()
                up_copy(e, slot).wait()
                rows = slot_x[pl.ds(pl.multiple_of(e * window, window), window), :]
                g = dot_bt(wg[slot], rows)
                u = dot_bt(wu[slot], rows)
                hidden = (jax.nn.silu(g) * u).astype(BF16)

                @pl.when(e + 2 < local_experts)
                def _():
                    gate_copy(e + 2, slot).start()
                    up_copy(e + 2, slot).start()

                down_copy(e, slot).wait()
                row = pl.multiple_of((e * capacity) // 8 * 8, 8)
                for buf, off in ((ex_send, peer_off), (ex_own, own_off)):
                    value = dot_at(hidden, wd[slot, :, pl.ds(off, half)])
                    for sub in range(SUBS):
                        part = value[:, sub * sub_cols:(sub + 1) * sub_cols]
                        buf[sub, pl.ds(row, 8), :] += part[0:8]
                        buf[sub, pl.ds(row + 8, window - 8), :] = part[8:]

                @pl.when(e + 2 < local_experts)
                def _():
                    down_copy(e + 2, slot).start()

                for i in range(groups):
                    @pl.when(e == last_expert[i])
                    def _():
                        yex_copy(0, i).start()
                        if i < EARLY_GROUPS:
                            yex_copy(1, i).start()

                for when, action, sub, i in loop_steps:
                    @pl.when(e == when)
                    def _():
                        action(sub, i)

            for i in range(EARLY_GROUPS, groups):
                yex_copy(1, i).start()

    pl.run_scoped(routed_phase, pltpu.VMEM((slots, 2 * tok), BF16), pltpu.VMEM((slots, 2 * tok), BF16),
                  pltpu.VMEM((2, ff_expert, d_model), BF16), pltpu.VMEM((2, ff_expert, d_model), BF16),
                  pltpu.VMEM((2, ff_expert, d_model), BF16), pltpu.SemaphoreType.DMA((2,)), pltpu.SemaphoreType.DMA((2,)), pltpu.SemaphoreType.DMA((2,)))

    with jax.named_scope("fin_shared"):
        for copy in xp_copies[:-2] + xp_copies[-1:] + fw_copies:
            copy.wait_send()
        res_load.wait()
        for r in range(ROW_BLOCKS):
            if r > 0:
                ysh_copy(r, 0).wait()

            @pl.loop(0, n_half)
            def _(j):
                if r == 0:
                    ysh_copy(r, j).wait()
                cols = pl.ds(pl.multiple_of(j * WIDE, WIDE), WIDE)
                rows = slice(r * r_rows, (r + 1) * r_rows)
                sh_own[j, rows, :] = res_half[rows, cols].astype(F32) + (sh_own[j, rows, :] + sh_recv[r, j])

    def combine(pick, sub, i):
        n = bounds[i + 1] - bounds[i]
        lanes = slice(ep_size * bounds[i], ep_size * bounds[i + 1])
        if sub == 0:
            lane = lax.broadcasted_iota(jnp.int32, (tok, ep_size * n), 1)
            owner = sum((lane >= q * n).astype(jnp.int32) for q in range(1, ep_size))
            lane_code = (lane + owner * (pack - n) + bounds[i]).astype(F32)
            pick[:, lanes] = (code_col[:, 0:1] == lane_code).astype(F32).astype(BF16)
        ret_copy(sub, i, me, rs_send, rs_recv, sib_dev).wait()
        ret_copy(sub, i, xp, rf_send, rf_recv, sib_dev).wait()
        rows = ret[sub, :, bounds[i]:bounds[i + 1], :].reshape(ep_size * n, sub_cols)
        gate = gate_col[:, 0:1]
        for j in range(sub_blocks):
            jj = sub * sub_blocks + j
            sh_own[jj] = sh_own[jj] + gate * dot(pick[:, lanes], rows[:, j * WIDE:(j + 1) * WIDE])

    def out_copies(sub):
        src = out_half.at[sub]
        dst = o_hbm.at[:, pl.ds(pl.multiple_of(own_off + sub * sub_cols, sub_cols), sub_cols)]
        return remote(src, dst, yo_send.at[sub], yo_recv.at[sub], y_peer), pltpu.make_async_copy(src, dst, lo_sem.at[sub])

    def emit(sub):
        for j in range(sub_blocks):
            out_half[sub, :, j * WIDE:(j + 1) * WIDE] = sh_own[sub * sub_blocks + j].astype(BF16)

    def start_out(sub):
        for copy in out_copies(sub):
            copy.start()

    def return_phase(pick):
        steps = [(combine, 0, 0), (combine, 1, 0), (combine, 0, 1), (combine, 1, 1), (combine, 0, 2), (combine, 1, 2), (give, 1, 3), (forward, 0, 3),
                 (combine, 0, 3), (forward, 1, 3), (give, 0, 4), (combine, 1, 3), (forward, 0, 4), (give, 0, 5), (combine, 0, 4), (forward, 0, 5),
                 (combine, 0, 5), (emit, 0), (start_out, 0), (give, 1, 4), (forward, 1, 4), (give, 1, 5), (combine, 1, 4), (forward, 1, 5), (combine, 1, 5), (emit, 1), (start_out, 1)]
        for step in steps:
            with jax.named_scope(step[0].__name__ + "".join(str(a) for a in step[1:])):
                if step[0] is combine:
                    combine(pick, *step[1:])
                else:
                    step[0](*step[1:])

    pl.run_scoped(return_phase, pltpu.VMEM((tok, ep_size * pack), BF16))

    with jax.named_scope("out"):
        for sub in range(SUBS):
            for copy in out_copies(sub):
                copy.wait()


def copy_kernel(src, dst, buf, in_sem, out_sem):
    n = src.shape[0] // COPY_CHUNKS
    reads = [pltpu.make_async_copy(src.at[pl.ds(c * n, n)], buf.at[pl.ds(c * n, n)], in_sem.at[c]) for c in range(COPY_CHUNKS)]
    writes = [pltpu.make_async_copy(buf.at[pl.ds(c * n, n)], dst.at[pl.ds(c * n, n)], out_sem.at[c]) for c in range(COPY_CHUNKS)]
    for copy in reads:
        copy.start()
    for read, write in zip(reads, writes):
        read.wait()
        write.start()
    for copy in writes:
        copy.wait()


def solution(mesh):
    ep_size = mesh.shape["ep"]
    tok_spec = P(("dp", "ep"), None)
    id_spec = P(("dp", "ep"))

    def device_step(normed, residual, w_router, ws_gate, ws_up, ws_down, we_gate, we_up, we_down, first_id, alt_id):
        tok, d_model = normed.shape
        local_experts, _, ff_expert = we_gate.shape
        experts = local_experts * ep_size
        capacity = (5 * tok * ep_size + 4 * experts - 1) // (4 * experts)
        window = -(-(capacity + 7) // 16) * 16
        pack = -(-local_experts * capacity // 16) * 16
        pack_buf = max(pack, (local_experts - 1) * capacity // 8 * 8 + window)
        bounds = [0] + [int(pack * f) // 32 * 32 for f in (0.13, 0.255, 0.4, 0.6, 0.84)] + [pack]
        half = d_model // 2
        slots = local_experts * window
        n_half = half // WIDE
        r_rows = tok // ROW_BLOCKS
        sub_cols = half // SUBS
        dma = pltpu.SemaphoreType.DMA
        any_spec = pl.BlockSpec(memory_space=pl.ANY)
        vmem_spec = pl.BlockSpec(memory_space=pltpu.VMEM)
        per_ret = dma((SUBS, len(bounds) - 1))
        out = pl.pallas_call(
            functools.partial(moe_kernel, (experts, capacity, window, pack, bounds, local_experts, ep_size)),
            out_shape=jax.ShapeDtypeStruct((tok, d_model), BF16),
            in_specs=[any_spec] * 9 + [vmem_spec] * 2,
            out_specs=any_spec,
            scratch_shapes=[
                pltpu.VMEM((2, tok, d_model), BF16),
                pltpu.VMEM((2 * tok, d_model), BF16),
                pltpu.VMEM((tok, d_model), BF16),
                pltpu.VMEM((ep_size, 8, tok), jnp.int32),
                pltpu.VMEM((ep_size, 8, tok), F32),
                pltpu.VMEM((tok, LANES), F32),
                pltpu.VMEM((tok, LANES), F32),
                pltpu.VMEM((slots, d_model), BF16),
                pltpu.VMEM((n_half, tok, WIDE), F32),
                pltpu.VMEM((ROW_BLOCKS, n_half, r_rows, WIDE), F32),
                pltpu.VMEM((ROW_BLOCKS, n_half, r_rows, WIDE), F32),
                pltpu.VMEM((SUBS, pack_buf, sub_cols), F32),
                pltpu.VMEM((SUBS, pack_buf, sub_cols), F32),
                pltpu.VMEM((SUBS, pack, sub_cols), F32),
                pltpu.VMEM((SUBS, ep_size, pack, sub_cols), BF16),
                pltpu.VMEM((SUBS, tok, sub_cols), BF16),
                pltpu.VMEM((tok, half), BF16),
                pltpu.VMEM((experts, d_model), F32),
                dma((ROW_BLOCKS + 2,)), dma((3,)), dma((3,)), dma((1,)), dma((1,)), dma((X_CHUNKS,)), dma((X_CHUNKS,)), dma((X_CHUNKS,)), dma((X_CHUNKS,)),
                dma((ROW_BLOCKS, n_half)), dma((ROW_BLOCKS, n_half)), per_ret, per_ret, per_ret, per_ret, per_ret, per_ret, per_ret, per_ret,
                dma((SUBS,)), dma((SUBS,)), dma((SUBS,)),
            ],
            compiler_params=pltpu.CompilerParams(collective_id=0, has_side_effects=True, vmem_limit_bytes=67043328),
        )(normed, residual, w_router.T, ws_gate, ws_up, ws_down, jnp.swapaxes(we_gate, 1, 2), jnp.swapaxes(we_up, 1, 2), we_down,
          first_id.reshape(1, tok), alt_id.reshape(1, tok))
        return pl.pallas_call(
            copy_kernel,
            out_shape=jax.ShapeDtypeStruct((tok, d_model), BF16),
            in_specs=[any_spec],
            out_specs=any_spec,
            scratch_shapes=[pltpu.VMEM((tok, d_model), BF16), dma((COPY_CHUNKS,)), dma((COPY_CHUNKS,))],
        )(out)

    return jax.shard_map(device_step, mesh=mesh, in_specs=(tok_spec, tok_spec, P(None, None), P(None, 'tp'), P(None, 'tp'), P('tp', None), P('ep', None, 'tp'), P('ep', None, 'tp'), P('ep', 'tp', None), id_spec, id_spec), out_specs=tok_spec, check_vma=False)
```
